128 devices in a mesh: dp: 128 (over z, y, x, core).
Axes of the slice: x: 4, y: 4, z: 4, core: 2. Of those that a mesh axis runs over, the one named last changes fastest.
Arguments:
- q_hidden: bfloat16 [512, 48, 1024], P('dp')
- q_mask: int32 [512, 48], P('dp')
- p_hidden: bfloat16 [512, 2, 128, 1024], P('dp')
- p_mask: int32 [512, 2, 128], P('dp')
- w_qkv: bfloat16 [1024, 3, 16, 64], replicated
- b_qkv: float32 [3, 16, 64], replicated
- w_out: bfloat16 [16, 64, 1024], replicated
- b_out: float32 [1024], replicated
- ln1_gain: float32 [1024], replicated
- ln1_shift: float32 [1024], replicated
- w_up: bfloat16 [1024, 4096], replicated
- b_up: float32 [4096], replicated
- w_down: bfloat16 [4096, 1024], replicated
- b_down: float32 [1024], replicated
- ln2_gain: float32 [1024], replicated
- ln2_shift: float32 [1024], replicated
Outputs:
- output 1: float32 [], replicated
- output 2: bfloat16 [512, 48, 1024], P('dp')
- output 3: bfloat16 [512, 2, 128, 1024], P('dp')
- output 4: float32 [1024, 3, 16, 64], replicated
- output 5: float32 [3, 16, 64], replicated
- output 6: float32 [16, 64, 1024], replicated
- output 7: float32 [1024], replicated
- output 8: float32 [1024], replicated
- output 9: float32 [1024], replicated
- output 10: float32 [1024, 4096], replicated
- output 11: float32 [4096], replicated
- output 12: float32 [4096, 1024], replicated
- output 13: float32 [1024], replicated
- output 14: float32 [1024], replicated
- output 15: float32 [1024], replicated
All inputs are finite; a program needn't handle non-finite values.
Results may differ from the reference program's by a relative error of at most 0.0126557.
Values sent between devices are 32-bit elements.
A program may use at most 1 GiB of HBM per device.

```python
import jax
import jax.numpy as jnp
from jax import lax

D = 1024
HEADS = 16
HEAD = 64
FF = 4096
QUERIES = 512
BLOCK = 4
Q_LEN = 48
P_LEN = 128
TOPICS = 4

INV_TEMP = 100.0
LN_EPS = 1e-12
NEG_FILL = -1e9


def prefix_mask(mask_key, lead_shape, seq_len):
    lengths = jax.random.randint(mask_key, lead_shape, 1, seq_len + 1).reshape(-1)
    lengths = lengths.at[0].set(seq_len).reshape(lead_shape)
    positions = jnp.arange(seq_len)
    return (positions < lengths[..., None]).astype(jnp.int32)


def setup_inputs(seed: int = 0) -> dict:
    key_list = jax.random.split(jax.random.key(seed), 20)
    topic_vecs = jax.random.normal(key_list[0], (TOPICS, D), jnp.float32)
    topic_ids = jax.random.randint(key_list[1], (QUERIES,), 0, TOPICS)
    pair_vecs = jax.random.normal(key_list[2], (QUERIES, 2, D), jnp.float32)
    pair_scale = 0.04 * jnp.power(3.0, jax.random.uniform(key_list[19], (), jnp.float32))
    topic_part = 0.3 * topic_vecs[topic_ids]
    q_base = topic_part + pair_scale * pair_vecs[:, 0]
    p_base = topic_part[:, None, :] + pair_scale * pair_vecs
    q_noise = jax.random.normal(key_list[3], (QUERIES, Q_LEN, D), jnp.float32)
    p_noise = jax.random.normal(key_list[4], (QUERIES, 2, P_LEN, D), jnp.float32)
    q_hidden = (q_base[:, None, :] + q_noise).astype(jnp.bfloat16)
    p_hidden = (p_base[:, :, None, :] + p_noise).astype(jnp.bfloat16)
    q_mask = prefix_mask(key_list[5], (QUERIES,), Q_LEN)
    p_mask = prefix_mask(key_list[6], (QUERIES, 2), P_LEN)

    def dense_init(init_key, shape_in, fan_in):
        return (jax.random.normal(init_key, shape_in, jnp.float32) * fan_in ** -0.5).astype(jnp.bfloat16)

    def vec_init(init_key, shape_in, center, spread):
        return center + spread * jax.random.normal(init_key, shape_in, jnp.float32)

    return {
        'q_hidden': q_hidden,
        'q_mask': q_mask,
        'p_hidden': p_hidden,
        'p_mask': p_mask,
        'w_qkv': dense_init(key_list[7], (D, 3, HEADS, HEAD), D),
        'b_qkv': vec_init(key_list[8], (3, HEADS, HEAD), 0.0, 0.3),
        'w_out': dense_init(key_list[9], (HEADS, HEAD, D), D),
        'b_out': vec_init(key_list[10], (D,), 0.0, 0.3),
        'ln1_gain': vec_init(key_list[11], (D,), 1.0, 0.2),
        'ln1_shift': vec_init(key_list[12], (D,), 0.0, 0.2),
        'w_up': dense_init(key_list[13], (D, FF), D),
        'b_up': vec_init(key_list[14], (FF,), 0.0, 0.3),
        'w_down': dense_init(key_list[15], (FF, D), FF),
        'b_down': vec_init(key_list[16], (D,), 0.0, 0.3),
        'ln2_gain': vec_init(key_list[17], (D,), 1.0, 0.2),
        'ln2_shift': vec_init(key_list[18], (D,), 0.0, 0.2),
    }


def snap_bf16(value):
    return value.astype(jnp.bfloat16).astype(jnp.float32)


def layer_norm(resid_in, ln_gain, ln_shift):
    row_mean = jnp.mean(resid_in, axis=-1, keepdims=True)
    centered = resid_in - row_mean
    row_var = jnp.mean(centered * centered, axis=-1, keepdims=True)
    return centered * lax.rsqrt(row_var + LN_EPS) * ln_gain + ln_shift


def encode(hidden, tok_mask, params):
    w_qkv, b_qkv, w_out, b_out, ln1_gain, ln1_shift, w_up, b_up, w_down, b_down, ln2_gain, ln2_shift = params
    qkv_proj = snap_bf16(jnp.einsum('ntd,dshe->snthe', hidden, w_qkv) + b_qkv[:, None, None])
    scores = jnp.einsum('nqhe,nkhe->nhqk', qkv_proj[0], qkv_proj[1]) * (HEAD ** -0.5)
    key_keep = (tok_mask > 0)[:, None, None, :]
    attn_probs = snap_bf16(jax.nn.softmax(jnp.where(key_keep, scores, NEG_FILL), axis=-1))
    context = snap_bf16(jnp.einsum('nhqk,nkhe->nqhe', attn_probs, qkv_proj[2]))
    resid1 = hidden + jnp.einsum('nqhe,hed->nqd', context, w_out) + b_out
    normed1 = snap_bf16(layer_norm(resid1, ln1_gain, ln1_shift))
    ffn_act = snap_bf16(jax.nn.gelu(jnp.einsum('ntd,df->ntf', normed1, w_up) + b_up, approximate=False))
    resid2 = normed1 + jnp.einsum('ntf,fd->ntd', ffn_act, w_down) + b_down
    layer_out = layer_norm(resid2, ln2_gain, ln2_shift)
    mask_f = tok_mask.astype(jnp.float32)
    pooled = jnp.einsum('ntd,nt->nd', layer_out, mask_f) / jnp.sum(mask_f, axis=1, keepdims=True)
    return pooled * lax.rsqrt(jnp.sum(pooled * pooled, axis=-1, keepdims=True))


def info_nce(q_embed, p_embed):
    flat_pass = p_embed.reshape(-1, p_embed.shape[-1])
    logits = jnp.dot(q_embed, flat_pass.T) * INV_TEMP
    positive = jnp.sum(q_embed * p_embed[:, 0], axis=-1) * INV_TEMP
    return jnp.mean(jax.nn.logsumexp(logits, axis=-1) - positive)


def reference(q_hidden, q_mask, p_hidden, p_mask, w_qkv, b_qkv, w_out, b_out, ln1_gain, ln1_shift, w_up, b_up, w_down, b_down, ln2_gain, ln2_shift):
    params = [w_qkv.astype(jnp.float32), b_qkv, w_out.astype(jnp.float32), b_out, ln1_gain, ln1_shift,
              w_up.astype(jnp.float32), b_up, w_down.astype(jnp.float32), b_down, ln2_gain, ln2_shift]
    n_blocks = QUERIES // BLOCK
    q_blocks = q_hidden.reshape(n_blocks, BLOCK, Q_LEN, D)
    qm_blocks = q_mask.reshape(n_blocks, BLOCK, Q_LEN)
    p_blocks = p_hidden.reshape(n_blocks, 2 * BLOCK, P_LEN, D)
    pm_blocks = p_mask.reshape(n_blocks, 2 * BLOCK, P_LEN)

    def embed_block(block_in):
        q_blk, qm_blk, p_blk, pm_blk = block_in
        return (encode(q_blk.astype(jnp.float32), qm_blk, params),
                encode(p_blk.astype(jnp.float32), pm_blk, params))

    q_embed, p_embed = lax.map(embed_block, (q_blocks, qm_blocks, p_blocks, pm_blocks))
    q_embed = q_embed.reshape(QUERIES, D)
    p_embed = p_embed.reshape(QUERIES, 2, D)
    mean_loss, embed_grads = jax.value_and_grad(info_nce, argnums=(0, 1))(q_embed, p_embed)
    d_q_embed, d_p_embed = embed_grads

    def grad_block(grad_acc, block_in):
        q_blk, qm_blk, p_blk, pm_blk, dq_blk, dp_blk = block_in

        def pair_embed(q_in, p_in, param_list):
            return encode(q_in, qm_blk, param_list), encode(p_in, pm_blk, param_list)

        unused_out, pullback = jax.vjp(pair_embed, q_blk.astype(jnp.float32), p_blk.astype(jnp.float32), params)
        d_q_in, d_p_in, d_params = pullback((dq_blk, dp_blk))
        grad_acc = [total + part for total, part in zip(grad_acc, d_params)]
        return grad_acc, (d_q_in.astype(jnp.bfloat16), d_p_in.astype(jnp.bfloat16))

    zero_grads = [jnp.zeros_like(param) for param in params]
    grad_sums, hidden_grads = lax.scan(
        grad_block, zero_grads,
        (q_blocks, qm_blocks, p_blocks, pm_blocks,
         d_q_embed.reshape(n_blocks, BLOCK, D), d_p_embed.reshape(n_blocks, 2 * BLOCK, D)))
    d_q_hidden = hidden_grads[0].reshape(q_hidden.shape)
    d_p_hidden = hidden_grads[1].reshape(p_hidden.shape)
    return (mean_loss, d_q_hidden, d_p_hidden, grad_sums[0], grad_sums[1], grad_sums[2], grad_sums[3],
            grad_sums[4], grad_sums[5], grad_sums[6], grad_sums[7], grad_sums[8], grad_sums[9],
            grad_sums[10], grad_sums[11])
```

```python
import functools
import jax
import jax.numpy as jnp
from jax import lax
from jax.experimental import pallas as pl
from jax.experimental.pallas import tpu as pltpu
from jax.sharding import PartitionSpec as P

ZERO, ONE, ALL = 0, 1, ...

F32 = jnp.float32
BF16 = jnp.bfloat16
LOGICAL = pl.DeviceIdType.LOGICAL
RING = 4


def mesh_place(axis):
    me = lax.axis_index(axis)
    core = lax.rem(me, 2)
    chip = me // 2
    return (lax.rem(chip, RING), lax.rem(chip // RING, RING), chip // (RING * RING)), core


def device_at(coords, core):
    return ((coords[2] * RING + coords[ONE]) * RING + coords[ZERO]) * 2 + core


def moved(coords, dim, by):
    out = list(coords)
    out[dim] = lax.rem(coords[dim] + by + 2 * RING, RING)
    return tuple(out)


def wrap(i):
    return lax.rem(i + 4 * RING, RING)


def enter(peers):
    barrier = pltpu.get_barrier_semaphore()
    for peer in peers:
        pl.semaphore_signal(barrier, inc=ONE, device_id=peer, device_id_type=LOGICAL)
    pl.semaphore_wait(barrier, len(peers))


def sum_kernel(axis, piece, u0_ref, u1_ref, u2_ref, small_ref, o_ref, part_ref, small_out, acc, stage, land1, land2, land3,
               small_land, load_sem, swap_send, swap_recv, stage_sem, p1_send, p1_recv, p2_send, p2_recv,
               p3_send, p3_recv, a3_send, a3_recv, a2_send, a2_recv, a1_send, a1_recv, own_sem,
               push_send, push_recv, s_send, s_recv):
    u_refs = (u0_ref, u1_ref, u2_ref)
    sub, chunk, region = 4 * piece, 16 * piece, 64 * piece
    half = 6 * region
    coords, core = mesh_place(axis)
    partner = device_at(coords, ONE - core)
    base = core * half

    dims = [((k // 2) % 3, (k // 2 + ONE) % 3, (k // 2 + 2) % 3) for k in range(6)]
    sign = [ONE if k % 2 == ZERO else -ONE for k in range(6)]
    pos = [tuple(coords[d] for d in dims[k]) for k in range(6)]
    nxt = [tuple(device_at(moved(coords, d, sign[k]), core) for d in dims[k]) for k in range(6)]

    def rdma(src, dst, send, recv, to):
        pltpu.make_async_remote_copy(src_ref=src, dst_ref=dst, send_sem=send, recv_sem=recv,
                                     device_id=to, device_id_type=LOGICAL).start()

    def drain(ref, sem):
        pltpu.make_async_copy(ref, ref, sem).wait()

    def rows(at, n):
        return pl.ds(pl.multiple_of(at, 8), n)

    def c1(k, t):
        return wrap(pos[k][ZERO] - sign[k] * (ONE + t))

    def c2(k, i):
        return wrap(pos[k][ONE] - sign[k] * (ONE + i))

    def c3(k, i):
        return wrap(pos[k][2] - sign[k] * (ONE + i))

    def at2(k, j1, j2):
        return k * region + j1 * chunk + j2 * sub

    peers = [partner] + [device_at(moved(coords, d, by), core) for d in range(3) for by in (ONE, 2, 3)]
    enter(peers)

    def source(mine, k, r, n):
        return [u_refs[(c * 6 + k) // 4].at[rows((c * 6 + k) % 4 * region + r - k * region, n)] for c in ((ZERO, ONE) if mine else (ONE, ZERO))]

    def each_core(start):
        for c in range(2):
            pl.when(core == c)(functools.partial(start, c))

    def load(t):
        def start(c):
            for k in range(6):
                r = k * region + c1(k, t) * chunk
                pltpu.make_async_copy(source(True, k, r, chunk)[c], acc.at[rows(r, chunk)], load_sem.at[t]).start()
        each_core(start)

    def swap(n):
        t, i = divmod(n, 4)

        def start(c):
            for k in range(6):
                r = at2(k, c1(k, t), c2(k, i))
                rdma(source(False, k, r, sub)[c], part_ref.at[rows(r, sub)], swap_send.at[n], swap_recv.at[n], partner)
        each_core(start)

    def fetch(n):
        t, i = divmod(n, 4)
        drain(part_ref.at[pl.ds(ZERO, 6 * sub)], swap_recv.at[n])
        for k in range(6):
            r = at2(k, c1(k, t), c2(k, i))
            pltpu.make_async_copy(part_ref.at[rows(r, sub)], stage.at[n % 2, pl.ds(k * sub, sub)],
                                  stage_sem.at[n]).start()

    def add_rows(dst, terms, n):
        def step(r, _):
            at = pl.multiple_of(r * 8, 8)
            val = dst(at)[ALL]
            for term in terms:
                val = val + term(at)[ALL]
            dst(at)[ALL] = val
            return ZERO
        lax.fori_loop(ZERO, n // 8, step, ZERO, unroll=2)

    smalls = [(None, core, 2)] + [(d, coords[d], RING) for d in range(3)]

    def small_send(stage_no):
        d, place, size = smalls[stage_no]
        for by in range(ONE, size):
            to = partner if d is None else device_at(moved(coords, d, by), core)
            rdma(small_out, small_land.at[stage_no, by - ONE], s_send.at[stage_no], s_recv.at[stage_no], to)

    def small_add(stage_no):
        d, place, size = smalls[stage_no]
        drain(small_land.at[stage_no, pl.ds(ZERO, size - ONE)], s_recv.at[stage_no])
        drain(small_land.at[stage_no, pl.ds(ZERO, size - ONE)], s_send.at[stage_no])
        mine = small_out[ALL]
        total = None
        for p in range(size):
            val = mine
            for by in range(ONE, size):
                val = jnp.where(lax.rem(place - p + size, size) == by, small_land[stage_no, by - ONE], val)
            total = val if total is None else total + val
        small_out[ALL] = total

    small_out[ALL] = small_ref[ALL]
    for t in range(4):
        load(t)
    for n in range(4):
        swap(n)
    small_send(ZERO)
    fetch(ZERO)

    for n in range(16):
        t, i = divmod(n, 4)
        if n + 4 < 16:
            swap(n + 4)
        if n + ONE < 16:
            fetch(n + ONE)
        if i == ZERO:
            drain(acc.at[pl.ds(ZERO, 6 * chunk)], load_sem.at[t])
        drain(stage.at[n % 2], stage_sem.at[n])
        if t > ZERO:
            drain(land1.at[t - ONE, i], p1_recv.at[t - ONE, i])
        for k in range(6):
            r = at2(k, c1(k, t), c2(k, i))
            terms = [lambda at, k=k: stage.at[n % 2, pl.ds(k * sub + at, 8)]]
            if t > ZERO:
                terms.append(lambda at, k=k: land1.at[t - ONE, i, pl.ds(k * sub + at, 8)])
            add_rows(lambda at, r=r: acc.at[pl.ds(pl.multiple_of(r + at, 8), 8)], terms, sub)
        if t < 3:
            for k in range(6):
                r = at2(k, c1(k, t), c2(k, i))
                rdma(acc.at[rows(r, sub)], land1.at[t, i, pl.ds(k * sub, sub)], p1_send.at[t, i], p1_recv.at[t, i], nxt[k][ZERO])
        if n in (ONE, 3, 5, 7):
            small_add(n // 2)
            if n < 7:
                small_send(n // 2 + ONE)
        if t == 3:
            for g in range(4):
                if i > ZERO:
                    drain(land2.at[i - ONE, g], p2_recv.at[i - ONE, g])
                    for k in range(6):
                        r = at2(k, pos[k][ZERO], c2(k, i)) + c3(k, g) * piece
                        add_rows(lambda at, r=r: acc.at[pl.ds(pl.multiple_of(r + at, 8), 8)],
                                 [lambda at, k=k: land2.at[i - ONE, g, pl.ds(k * piece + at, 8)]], piece)
                if i < 3:
                    for k in range(6):
                        r = at2(k, pos[k][ZERO], c2(k, i)) + c3(k, g) * piece
                        rdma(acc.at[rows(r, piece)], land2.at[i, g, pl.ds(k * piece, piece)],
                             p2_send.at[i, g], p2_recv.at[i, g], nxt[k][ONE])
                else:
                    if g > ZERO:
                        drain(land3.at[g - ONE], p3_recv.at[g - ONE])
                        for k in range(6):
                            r = at2(k, pos[k][ZERO], pos[k][ONE]) + c3(k, g) * piece
                            add_rows(lambda at, r=r: acc.at[pl.ds(pl.multiple_of(r + at, 8), 8)],
                                     [lambda at, k=k: land3.at[g - ONE, pl.ds(k * piece + at, 8)]], piece)
                    if g < 3:
                        for k in range(6):
                            r = at2(k, pos[k][ZERO], pos[k][ONE]) + c3(k, g) * piece
                            rdma(acc.at[rows(r, piece)], land3.at[g, pl.ds(k * piece, piece)],
                                 p3_send.at[g], p3_recv.at[g], nxt[k][2])

    for k in range(6):
        r = at2(k, pos[k][ZERO], pos[k][ONE]) + pos[k][2] * piece
        pltpu.make_async_copy(acc.at[rows(r, piece)], o_ref.at[rows(base + r, piece)], own_sem.at[ZERO]).start()
        rdma(acc.at[rows(r, piece)], o_ref.at[rows(base + r, piece)], a3_send.at[ZERO], a3_recv.at[ZERO], nxt[k][2])
    for t in range(3):
        drain(acc.at[pl.ds(ZERO, 6 * piece)], a3_recv.at[t])
        if t < 2:
            for k in range(6):
                r = base + at2(k, pos[k][ZERO], pos[k][ONE]) + c3(k, t) * piece
                rdma(o_ref.at[rows(r, piece)], o_ref.at[rows(r, piece)], a3_send.at[t + ONE], a3_recv.at[t + ONE], nxt[k][2])
    drain(acc.at[pl.ds(ZERO, 6 * piece)], own_sem.at[ZERO])

    def spread(n, j1, j2):
        for k in range(6):
            r = base + at2(k, j1(k), j2(k))
            rdma(o_ref.at[rows(r, sub)], o_ref.at[rows(r, sub)], push_send.at[n], push_recv.at[n], partner)

    def hop2(t):
        for k in range(6):
            j2 = pos[k][ONE] if t == ZERO else c2(k, t - ONE)
            r = base + at2(k, pos[k][ZERO], j2)
            rdma(o_ref.at[rows(r, sub)], o_ref.at[rows(r, sub)], a2_send.at[t], a2_recv.at[t], nxt[k][ONE])

    def second(i):
        return lambda k: pos[k][ONE] if i == ZERO else c2(k, i - ONE)

    def first(t):
        return lambda k: pos[k][ZERO] if t == ZERO else c1(k, t - ONE)

    def hop1(t, i):
        for k in range(6):
            r = base + at2(k, first(t)(k), second(i)(k))
            rdma(o_ref.at[rows(r, sub)], o_ref.at[rows(r, sub)], a1_send.at[t, i], a1_recv.at[t, i], nxt[k][ZERO])

    for i in range(4):
        if i > ZERO:
            drain(acc.at[pl.ds(ZERO, 6 * sub)], a2_recv.at[i - ONE])
        if i < 3:
            hop2(i)
        hop1(ZERO, i)
        spread(i, first(ZERO), second(i))
    for t in range(3):
        for i in range(4):
            drain(acc.at[pl.ds(ZERO, 6 * sub)], a1_recv.at[t, i])
            if t < 2:
                hop1(t + ONE, i)
            spread(4 * (t + ONE) + i, first(t + ONE), second(i))

    for n in range(16):
        drain(acc.at[pl.ds(ZERO, 6 * sub)], swap_send.at[n])
    for t in range(3):
        for i in range(4):
            drain(acc.at[pl.ds(ZERO, 6 * sub)], p1_send.at[t, i])
            drain(acc.at[pl.ds(ZERO, 6 * piece)], p2_send.at[t, i])
            drain(acc.at[pl.ds(ZERO, 6 * sub)], a1_send.at[t, i])
        drain(acc.at[pl.ds(ZERO, 6 * piece)], p3_send.at[t])
        drain(acc.at[pl.ds(ZERO, 6 * piece)], a3_send.at[t])
        drain(acc.at[pl.ds(ZERO, 6 * sub)], a2_send.at[t])
    for n in range(16):
        drain(acc.at[pl.ds(ZERO, 6 * sub)], push_send.at[n])
        drain(acc.at[pl.ds(ZERO, 6 * sub)], push_recv.at[n])


def sum_over_devices(parts, small, axis, collective_id=ONE):
    width = parts[ZERO].shape[ONE]
    total = sum(p.shape[ZERO] for p in parts)
    piece = total // 768
    dma = pltpu.SemaphoreType.DMA
    sub = 4 * piece
    outs = pl.pallas_call(
        functools.partial(sum_kernel, axis, piece),
        out_shape=(jax.ShapeDtypeStruct((total, width), F32), jax.ShapeDtypeStruct((total // 2, width), F32),
                   jax.ShapeDtypeStruct(small.shape, F32)),
        in_specs=[pl.BlockSpec(memory_space=pl.ANY)] * 3 + [pl.BlockSpec(memory_space=pltpu.VMEM)],
        out_specs=(pl.BlockSpec(memory_space=pl.ANY), pl.BlockSpec(memory_space=pl.ANY),
                   pl.BlockSpec(memory_space=pltpu.VMEM)),
        scratch_shapes=[
            pltpu.VMEM((total // 2, width), F32),
            pltpu.VMEM((2, 6 * sub, width), F32),
            pltpu.VMEM((3, 4, 6 * sub, width), F32),
            pltpu.VMEM((3, 4, 6 * piece, width), F32),
            pltpu.VMEM((3, 6 * piece, width), F32),
            pltpu.VMEM((4, 3) + small.shape, F32),
            dma((4,)), dma((16,)), dma((16,)), dma((16,)),
            dma((3, 4)), dma((3, 4)), dma((3, 4)), dma((3, 4)), dma((3,)), dma((3,)),
            dma((3,)), dma((3,)), dma((3,)), dma((3,)), dma((3, 4)), dma((3, 4)), dma((ONE,)),
            dma((16,)), dma((16,)), dma((4,)), dma((4,)),
        ],
        compiler_params=pltpu.CompilerParams(collective_id=collective_id, has_side_effects=True,
                                             vmem_limit_bytes=64 * 1024 * 1024),
        name="sum_over_devices",
    )(*parts, small)
    return outs[ZERO], outs[2]


def gather_kernel(axis, e_ref, g_ref, mine, theirs, swap_sem, sems_send, sems_recv, push_send, push_recv):
    coords, core = mesh_place(axis)
    partner = device_at(coords, ONE - core)
    width = e_ref.shape[ONE]
    lanes = pl.ds(pl.multiple_of(core * (width // 2), 128), width // 2)
    x, y, z = coords
    peers = [partner] + [device_at(moved(coords, d, by), core) for d in range(3) for by in (ONE, 2, 3)]
    enter(peers)

    def rdma(src, dst, send, recv, to):
        pltpu.make_async_remote_copy(src_ref=src, dst_ref=dst, send_sem=send, recv_sem=recv,
                                     device_id=to, device_id_type=LOGICAL).start()

    def drain(ref, sem):
        pltpu.make_async_copy(ref, ref, sem).wait()

    rdma(e_ref, theirs, swap_sem.at[ZERO], swap_sem.at[ONE], partner)
    mine[ALL] = e_ref[ALL]
    drain(theirs, swap_sem.at[ONE])
    first = jnp.where(core == ZERO, mine[:, lanes], theirs[:, lanes])
    second = jnp.where(core == ZERO, theirs[:, lanes], mine[:, lanes])
    g_ref[z, y, x, ZERO:4, lanes] = first[ZERO:4]
    g_ref[z, y, x, 4:8, lanes] = second[ZERO:4]
    g_ref[z, y, x, 8:16, lanes] = first[8:16]
    g_ref[z, y, x, 16:24, lanes] = second[8:16]
    drain(e_ref, swap_sem.at[ZERO])

    def view(a, stage):
        idx = [z, y, x]
        for s in range(stage):
            idx[2 - (a + s) % 3] = slice(None)
        return g_ref.at[idx[ZERO], idx[ONE], idx[2], pl.ds(8 * a, 8), lanes]

    for stage in range(3):
        for by in (ONE, 3, 2):
            for a in range(3):
                to = device_at(moved(coords, (a + stage) % 3, by), core)
                rdma(view(a, stage), view(a, stage), sems_send.at[stage, by - ONE], sems_recv.at[stage, by - ONE], to)
        if stage == 2:
            for a in range(3):
                rdma(view(a, 2), view(a, 2), push_send.at[ZERO], push_recv.at[ZERO], partner)
        for by in (ONE, 3, 2):
            n = 4 ** stage
            shape_like = g_ref.at[ZERO, ZERO, ZERO, :, lanes] if stage == ZERO else (
                g_ref.at[ZERO, ZERO, :, :, lanes] if stage == ONE else g_ref.at[ZERO, :, :, :, lanes])
            drain(shape_like, sems_recv.at[stage, by - ONE])
            if stage == 2:
                for a in range(3):
                    far = moved(coords, (a + 2) % 3, RING - by)
                    idx = [far[2], far[ONE], far[ZERO]]
                    idx[2 - a] = slice(None)
                    idx[2 - (a + ONE) % 3] = slice(None)
                    v = g_ref.at[idx[ZERO], idx[ONE], idx[2], pl.ds(8 * a, 8), lanes]
                    rdma(v, v, push_send.at[by], push_recv.at[by], partner)
    for stage in range(3):
        shape_like = g_ref.at[ZERO, ZERO, ZERO, :, lanes] if stage == ZERO else (
            g_ref.at[ZERO, ZERO, :, :, lanes] if stage == ONE else g_ref.at[ZERO, :, :, :, lanes])
        for by in (ONE, 2, 3):
            drain(shape_like, sems_send.at[stage, by - ONE])
    for by in range(4):
        drain(g_ref.at[ZERO, :, :, :, lanes], push_send.at[by])
        drain(g_ref.at[ZERO, :, :, :, lanes], push_recv.at[by])


def gather_embeddings(e, axis, collective_id=2):
    dma = pltpu.SemaphoreType.DMA
    width = e.shape[ONE]
    g = pl.pallas_call(
        functools.partial(gather_kernel, axis),
        out_shape=jax.ShapeDtypeStruct((RING, RING, RING, 24, width), F32),
        in_specs=[pl.BlockSpec(memory_space=pltpu.VMEM)],
        out_specs=pl.BlockSpec(memory_space=pltpu.VMEM),
        scratch_shapes=[pltpu.VMEM(e.shape, F32), pltpu.VMEM(e.shape, F32), dma((2,)),
                        dma((3, 3)), dma((3, 3)), dma((4,)), dma((4,))],
        compiler_params=pltpu.CompilerParams(collective_id=collective_id, has_side_effects=True,
                                             vmem_limit_bytes=16 * 1024 * 1024),
        name="gather_embeddings",
    )(e)
    return g.reshape(RING ** 3, 24, width)


def loss_kernel(axis, n_query, g_ref, pooled_ref, loss_ref, d_ref, logit_ref, lse_ref):
    me = lax.axis_index(axis)
    core, chip = lax.rem(me, 2), me // 2
    width = pooled_ref.shape[ONE]
    chips = g_ref.shape[ZERO]
    gs = 100.0 / n_query
    hi = lax.Precision.HIGHEST
    nt = (((ONE,), (ONE,)), ((), ()))
    pall = g_ref[:, 8:24, :].reshape(chips * 16, width)
    block = 128
    per = block // 8

    def chunk(b, loss):
        qb = g_ref[pl.ds(b * per, per), ZERO:8, :].reshape(block, width)
        s = lax.dot_general(qb, pall, nt, precision=hi, preferred_element_type=F32) * 100.0
        logit_ref[pl.ds(pl.multiple_of(b * block, block), block), :] = s
        top = jnp.max(s, axis=ONE, keepdims=True)
        lse = jnp.log(jnp.sum(jnp.exp(s - top), axis=ONE, keepdims=True)) + top
        lse_ref[pl.ds(pl.multiple_of(b * block, block), block), :] = jnp.broadcast_to(lse, (block, 128))
        row = lax.broadcasted_iota(jnp.int32, s.shape, ZERO) + b * block
        col = lax.broadcasted_iota(jnp.int32, s.shape, ONE)
        pos = jnp.sum(jnp.where(col == 2 * row, s, 0.0), axis=ONE, keepdims=True)
        return loss + jnp.sum(lse - pos, axis=ZERO, keepdims=True)

    loss = lax.fori_loop(ZERO, chips // per, chunk, jnp.zeros((ONE, ONE), F32))
    loss_ref[ALL] = jnp.broadcast_to(loss * (1.0 / n_query), loss_ref.shape)

    at = pl.multiple_of(chip * 8, 8)
    s8 = logit_ref[pl.ds(at, 8), :]
    l8 = lse_ref[pl.ds(at, 8), ZERO:ONE]
    row = lax.broadcasted_iota(jnp.int32, s8.shape, ZERO) + chip * 8
    col = lax.broadcasted_iota(jnp.int32, s8.shape, ONE)
    w8 = jnp.exp(s8 - l8) * gs - jnp.where(col == 2 * row, gs, 0.0)
    dq8 = lax.dot_general(w8, pall, (((ONE,), (ZERO,)), ((), ())), precision=hi, preferred_element_type=F32)

    qall = g_ref[:, ZERO:8, :].reshape(chips * 8, width)
    p16 = g_ref[chip, 8:24, :]
    s16 = lax.dot_general(qall, p16, nt, precision=hi, preferred_element_type=F32) * 100.0
    row = lax.broadcasted_iota(jnp.int32, s16.shape, ZERO)
    col = lax.broadcasted_iota(jnp.int32, s16.shape, ONE) + chip * 16
    w16 = jnp.exp(s16 - lse_ref[:, ZERO:ONE]) * gs - jnp.where(col == 2 * row, gs, 0.0)
    dp16 = lax.dot_general(w16, qall, (((ZERO,), (ZERO,)), ((), ())), precision=hi, preferred_element_type=F32)

    dq = jnp.where(core == ZERO, dq8[ZERO:4], dq8[4:8])
    dp = jnp.where(core == ZERO, dp16[ZERO:8], dp16[8:16])
    pooled_q, pooled_p = pooled_ref[ZERO:4], pooled_ref[8:16]

    def back(d, pooled):
        inv = lax.rsqrt(jnp.sum(pooled * pooled, axis=ONE, keepdims=True))
        e = pooled * inv
        return (d - e * jnp.sum(e * d, axis=ONE, keepdims=True)) * inv

    d_ref[ALL] = jnp.zeros_like(d_ref)
    d_ref[ZERO:4, :] = back(dq, pooled_q)
    d_ref[8:16, :] = back(dp, pooled_p)


def loss_and_grad(g, pooled, axis, n_query):
    chips, _, width = g.shape
    loss, d = pl.pallas_call(
        functools.partial(loss_kernel, axis, n_query),
        out_shape=(jax.ShapeDtypeStruct((8, 128), F32), jax.ShapeDtypeStruct(pooled.shape, F32)),
        in_specs=[pl.BlockSpec(memory_space=pltpu.VMEM)] * 2,
        out_specs=(pl.BlockSpec(memory_space=pltpu.VMEM),) * 2,
        scratch_shapes=[pltpu.VMEM((chips * 8, chips * 16), F32), pltpu.VMEM((chips * 8, 128), F32)],
        compiler_params=pltpu.CompilerParams(vmem_limit_bytes=48 * 1024 * 1024),
        name="loss_and_grad",
    )(g, pooled)
    return loss[ZERO, ZERO], d


NN = (((ONE,), (ZERO,)), ((), ()))
NT = (((ONE,), (ONE,)), ((), ()))
TN = (((ZERO,), (ZERO,)), ((), ()))
LN_EPS = 1e-12
NEG_FILL = -1e9
TILE = 512


def mm(a, b, dims=NN):
    return lax.dot_general(a, b, dims, preferred_element_type=F32)


def vmem(mb=60):
    return pltpu.CompilerParams(vmem_limit_bytes=mb * 1024 * 1024)


def whole(shape):
    return pl.BlockSpec(shape, lambda j: (ZERO,) * len(shape), pipeline_mode=pl.Buffered(ONE))


def across(rows, tile):
    return pl.BlockSpec((rows, tile), lambda j: (ZERO, j))


def down(tile, cols):
    return pl.BlockSpec((tile, cols), lambda j: (j, ZERO))


def qkv_kernel(x_ref, w_ref, b_ref, oq_ref, op_ref):
    y = (mm(x_ref[ALL], w_ref[ALL], NT) + b_ref[ALL]).astype(BF16)
    tq = oq_ref.shape[ZERO]
    oq_ref[ALL] = y[:tq]
    op_ref[ALL] = y[tq:]


def qkv_project(x, w_t, b, tq, tile=TILE):
    t, d = x.shape
    tp = t - tq
    f = w_t.shape[ZERO]
    return pl.pallas_call(
        qkv_kernel, grid=(f // tile,),
        out_shape=(jax.ShapeDtypeStruct((tq, f), BF16), jax.ShapeDtypeStruct((tp, f), BF16)),
        in_specs=[whole((t, d)), down(tile, d), across(ONE, tile)],
        out_specs=(across(tq, tile), across(tp, tile)),
        compiler_params=vmem(), name="qkv_project",
    )(x, w_t, b)


def split_heads(pair, head):
    lane = lax.broadcasted_iota(jnp.int32, pair.shape, ONE)
    zero = jnp.zeros_like(pair)
    return jnp.concatenate([jnp.where(lane < head, pair, zero), jnp.where(lane >= head, pair, zero)], axis=ZERO)


def join_heads(stacked, head):
    t = stacked.shape[ZERO] // 2
    lane = lax.broadcasted_iota(jnp.int32, (t, stacked.shape[ONE]), ONE)
    return jnp.where(lane < head, stacked[:t], stacked[t:])


def attn_kernel(scale, head, qkv_ref, mask_ref, probs_ref, ctx_ref):
    d = ctx_ref.shape[ONE]
    pair = 2 * head
    keep = mask_ref[ZERO] > ZERO
    for g in range(d // pair):
        at = pl.ds(g * pair, pair)
        q = split_heads(qkv_ref[:, at], head)
        k = qkv_ref[:, pl.ds(d + g * pair, pair)]
        v = qkv_ref[:, pl.ds(2 * d + g * pair, pair)]
        s = jnp.where(keep, mm(q, k, NT) * scale, NEG_FILL)
        e = jnp.exp(s - jnp.max(s, axis=ONE, keepdims=True))
        p = (e / jnp.sum(e, axis=ONE, keepdims=True)).astype(BF16)
        probs_ref[ZERO, g] = p
        ctx_ref[:, at] = join_heads(mm(p, v), head).astype(BF16)


def attention(qkv, mask, seq, head):
    n = mask.shape[ZERO]
    d = qkv.shape[ONE] // 3
    pairs = d // (2 * head)
    return pl.pallas_call(
        functools.partial(attn_kernel, head ** -0.5, head), grid=(n,),
        out_shape=(jax.ShapeDtypeStruct((n, pairs, 2 * seq, seq), BF16), jax.ShapeDtypeStruct((n * seq, d), BF16)),
        in_specs=[down(seq, 3 * d), pl.BlockSpec((ONE, ONE, seq), lambda j: (j, ZERO, ZERO))],
        out_specs=(pl.BlockSpec((ONE, pairs, 2 * seq, seq), lambda j: (j, ZERO, ZERO, ZERO)), down(seq, d)),
        compiler_params=vmem(), name="attention",
    )(qkv, mask.reshape(n, ONE, seq))


def attn_bwd_kernel(scale, head, qkv_ref, probs_ref, dc_ref, d_ref):
    d = dc_ref.shape[ONE]
    pair = 2 * head
    for g in range(d // pair):
        at = pl.ds(g * pair, pair)
        q = split_heads(qkv_ref[:, at], head)
        k = qkv_ref[:, pl.ds(d + g * pair, pair)]
        v = qkv_ref[:, pl.ds(2 * d + g * pair, pair)]
        p = probs_ref[ZERO, g]
        dc = split_heads(dc_ref[:, at], head)
        dp = mm(dc, v, NT)
        pf = p.astype(F32)
        ds = (pf * (dp - jnp.sum(dp * pf, axis=ONE, keepdims=True)) * scale).astype(BF16)
        d_ref[:, at] = join_heads(mm(ds, k), head).astype(BF16)
        d_ref[:, pl.ds(d + g * pair, pair)] = mm(ds, q, TN).astype(BF16)
        d_ref[:, pl.ds(2 * d + g * pair, pair)] = mm(p, dc, TN).astype(BF16)


def attention_bwd(qkv, probs, d_ctx, seq, head):
    n, pairs = probs.shape[:2]
    d = d_ctx.shape[ONE]
    return pl.pallas_call(
        functools.partial(attn_bwd_kernel, head ** -0.5, head), grid=(n,),
        out_shape=jax.ShapeDtypeStruct((n * seq, 3 * d), BF16),
        in_specs=[down(seq, 3 * d),
                  pl.BlockSpec((ONE, pairs, 2 * seq, seq), lambda j: (j, ZERO, ZERO, ZERO)),
                  down(seq, d)],
        out_specs=down(seq, 3 * d),
        compiler_params=vmem(), name="attention_bwd",
    )(qkv, probs, d_ctx)


def norm_rows(x):
    c = x - jnp.mean(x, axis=ONE, keepdims=True)
    r = lax.rsqrt(jnp.mean(c * c, axis=ONE, keepdims=True) + LN_EPS)
    return c * r, r


def norm_back(g, hat, r):
    return r * (g - jnp.mean(g, axis=ONE, keepdims=True) - hat * jnp.mean(g * hat, axis=ONE, keepdims=True))


ERFC = (0.07122347, -0.27794802, 0.29668747, -0.02018065, 0.21581222, 0.21731356, 0.24887118, 0.24822095)


def gelu_parts(u):
    bell = jnp.exp(-0.5 * u * u)
    t = 1.0 / (1.0 + 0.311126984 * jnp.abs(u))
    poly = ERFC[ZERO]
    for c in ERFC[ONE:]:
        poly = poly * t + c
    tail = 0.5 * bell * (poly * t)
    return jnp.where(u >= 0.0, 1.0 - tail, tail), u * bell * 0.3989422804


ROWS = 304


def ffn_kernel(bounds, x_ref, cq_ref, cp_ref, wo_ref, vec_ref, wt_ref, wu_ref, bu_ref, wd_ref,
               h_ref, r1_ref, g_ref, gp_ref, r2_ref, pool_ref):
    j = pl.program_id(ZERO)
    t = x_ref.shape[ZERO]
    tq = cq_ref.shape[ZERO]
    b_out, g1, s1, b_down, g2, s2 = (vec_ref[i:i + ONE, :] for i in range(6))

    @pl.when(j == ZERO)
    def _():
        for ref, lo in ((cq_ref, ZERO), (cp_ref, tq)):
            n = ref.shape[ZERO]
            size = n if n < 256 else 256
            for a in range(ZERO, n, size):
                at = pl.ds(lo + a, size)
                r1 = x_ref[at, :].astype(F32) + mm(ref[pl.ds(a, size), :], wo_ref[ALL]) + b_out
                r1_ref[at, :] = r1
                h = (norm_rows(r1)[ZERO] * g1 + s1).astype(BF16)
                h_ref[at, :] = h
                r2_ref[at, :] = h.astype(F32) + b_down

    for a in range(ZERO, t, ROWS):
        at = pl.ds(a, ROWS)
        u = mm(h_ref[at, :], wu_ref[ALL]) + bu_ref[ALL]
        cdf, upd = gelu_parts(u)
        g = (u * cdf).astype(BF16)
        g_ref[at, :] = g
        gp_ref[at, :] = cdf + upd
        r2_ref[at, :] += mm(g, wd_ref[ALL])

    @pl.when(j == pl.num_programs(ZERO) - ONE)
    def _():
        pool_ref[ALL] = jnp.zeros_like(pool_ref)
        for row, lo, n in bounds:
            at = pl.ds(lo, n)
            y = norm_rows(r2_ref[at, :])[ZERO] * g2 + s2
            pool_ref[row:row + ONE, :] = jnp.sum(y * wt_ref[at, :], axis=ZERO, keepdims=True)


def ffn_forward(x, ctx_q, ctx_p, w_out, vecs, weights, w_up, b_up, w_down, bounds, tile=TILE):
    t, d = x.shape
    f = w_up.shape[ONE]
    sds = jax.ShapeDtypeStruct
    return pl.pallas_call(
        functools.partial(ffn_kernel, bounds), grid=(f // tile,),
        out_shape=(sds((t, d), BF16), sds((t, d), F32), sds((t, f), BF16), sds((t, f), F32), sds((t, d), F32), sds((16, d), F32)),
        in_specs=[whole((t, d)), whole(ctx_q.shape), whole(ctx_p.shape), whole((d, d)), whole(vecs.shape), whole((t, ONE)),
                  across(d, tile), across(ONE, tile),
                  down(tile, d)],
        out_specs=(whole((t, d)), whole((t, d)), across(t, tile),
                   across(t, tile), whole((t, d)), whole((16, d))),
        compiler_params=vmem(), name="ffn_forward",
    )(x, ctx_q, ctx_p, w_out, vecs, weights, w_up, b_up, w_down)


def ffn_bwd_kernel(bounds, dpool_ref, r2_ref, wt_ref, vec_ref, h_ref, g_ref, gp_ref, wd_ref, wu_ref, r1_ref, wo_ref,
                   dwd_ref, dwu_ref, dbu_ref, dr1_ref, dr1b_ref, dcq_ref, dcp_ref, dvec_ref, dr2_ref, ht_ref):
    j = pl.program_id(ZERO)
    t = h_ref.shape[ZERO]
    b_out, g1, s1, b_down, g2, s2 = (vec_ref[i:i + ONE, :] for i in range(6))

    @pl.when(j == ZERO)
    def _():
        dvec_ref[ALL] = jnp.zeros_like(dvec_ref)
        for row, lo, n in bounds:
            at = pl.ds(lo, n)
            hat, r = norm_rows(r2_ref[at, :])
            dy = wt_ref[at, :] * dpool_ref[row:row + ONE, :]
            dr2 = norm_back(dy * g2, hat, r)
            dr1_ref[at, :] = dr2
            dr2_ref[at, :] = dr2.astype(BF16)
            dvec_ref[3:4, :] += jnp.sum(dr2, axis=ZERO, keepdims=True)
            dvec_ref[4:5, :] += jnp.sum(dy * hat, axis=ZERO, keepdims=True)
            dvec_ref[5:6, :] += jnp.sum(dy, axis=ZERO, keepdims=True)
        ht_ref[ALL] = h_ref[ALL].T

    dg = mm(dr2_ref[ALL], wd_ref[ALL], NT).astype(BF16).astype(F32)
    dpre = dg * gp_ref[ALL]
    dbu_ref[ALL] = jnp.sum(dpre, axis=ZERO, keepdims=True)
    dpre = dpre.astype(BF16)
    dwu_ref[ZERO] = mm(ht_ref[ALL], dpre)
    dr1_ref[ALL] += mm(dpre, wu_ref[ALL], NT)
    dwd_ref[ALL] = mm(g_ref[ALL], dr2_ref[ALL], TN)

    @pl.when(j == pl.num_programs(ZERO) - ONE)
    def _():
        for a in range(ZERO, t, ROWS):
            at = pl.ds(a, ROWS)
            dy = dr1_ref[at, :].astype(BF16).astype(F32)
            hat, r = norm_rows(r1_ref[at, :])
            dr1 = norm_back(dy * g1, hat, r)
            dr1_ref[at, :] = dr1
            lo = dr1.astype(BF16)
            dr1b_ref[at, :] = lo
            dvec_ref[ZERO:ONE, :] += jnp.sum(dr1, axis=ZERO, keepdims=True)
            dvec_ref[ONE:2, :] += jnp.sum(dy * hat, axis=ZERO, keepdims=True)
            dvec_ref[2:3, :] += jnp.sum(dy, axis=ZERO, keepdims=True)
        tq = dcq_ref.shape[ZERO]
        dcq_ref[ALL] = mm(dr1b_ref[:tq, :], wo_ref[ALL], NT).astype(BF16)
        dcp_ref[ALL] = mm(dr1b_ref[tq:, :], wo_ref[ALL], NT).astype(BF16)


def ffn_backward(dpool, r2, weights, vecs, h, g, gp, w_down, w_up, r1, w_out, bounds, tq, tile=TILE):
    t, d = h.shape
    tp = t - tq
    f = w_up.shape[ONE]
    sds = jax.ShapeDtypeStruct
    per = d // tile
    return pl.pallas_call(
        functools.partial(ffn_bwd_kernel, bounds), grid=(f // tile,),
        out_shape=(sds((f, d), F32), sds((f // d, d, d), F32), sds((ONE, f), F32), sds((t, d), F32), sds((t, d), BF16),
                   sds((tq, d), BF16), sds((tp, d), BF16), sds((8, d), F32)),
        in_specs=[whole(dpool.shape), whole((t, d)), whole((t, ONE)), whole(vecs.shape), whole((t, d)),
                  across(t, tile), across(t, tile),
                  down(tile, d), across(d, tile),
                  whole((t, d)), whole((d, d))],
        out_specs=(down(tile, d), pl.BlockSpec((ONE, d, tile), lambda j: (lax.div(j, per), ZERO, lax.rem(j, per))),
                   across(ONE, tile), whole((t, d)), whole((t, d)), whole((tq, d)), whole((tp, d)), whole((8, d))),
        scratch_shapes=[pltpu.VMEM((t, d), BF16), pltpu.VMEM((d, t), BF16)],
        compiler_params=vmem(63), name="ffn_backward",
    )(dpool, r2, weights, vecs, h, g, gp, w_down, w_up, r1, w_out)


def qkv_bwd_kernel(steps, dq_ref, dp_ref, x_ref, w_ref, dr1_ref, cq_ref, cp_ref, dr1b_ref, dw_ref, db_ref, dh_ref, acc_ref):
    j = pl.program_id(ZERO)
    tq = dq_ref.shape[ZERO]

    @pl.when(j < steps)
    def _():
        dp = jnp.concatenate([dq_ref[ALL], dp_ref[ALL]], axis=ZERO)
        part = mm(dp, w_ref[ALL])

        @pl.when(j == ZERO)
        def _():
            acc_ref[ALL] = dr1_ref[ALL] + part

        @pl.when(j > ZERO)
        def _():
            acc_ref[ALL] += part
        dw_ref[ALL] = mm(dp, x_ref[ALL], TN)
        db_ref[ALL] = jnp.sum(dp.astype(F32), axis=ZERO, keepdims=True)

    @pl.when(j == steps - ONE)
    def _():
        dh_ref[ALL] = acc_ref[ALL].astype(BF16)

    @pl.when(j >= steps)
    def _():
        ctx = jnp.concatenate([cq_ref[ALL], cp_ref[ALL]], axis=ZERO)
        dw_ref[ALL] = mm(ctx, dr1b_ref[ALL], TN)


def qkv_backward(dq, dp, x, w_t, dr1, ctx_q, ctx_p, dr1b, tile=TILE):
    t, d = x.shape
    f = w_t.shape[ZERO]
    tq, tp = dq.shape[ZERO], dp.shape[ZERO]
    n, m = f // tile, d // tile
    sds = jax.ShapeDtypeStruct
    cut = lambda j: jnp.minimum(j, n - ONE)
    late = lambda j: jnp.maximum(j - n, ZERO)
    return pl.pallas_call(
        functools.partial(qkv_bwd_kernel, n), grid=(n + m,),
        out_shape=(sds((f + d, d), F32), sds((ONE, f), F32), sds((t, d), BF16)),
        in_specs=[pl.BlockSpec((tq, tile), lambda j: (ZERO, cut(j))), pl.BlockSpec((tp, tile), lambda j: (ZERO, cut(j))),
                  whole((t, d)), pl.BlockSpec((tile, d), lambda j: (cut(j), ZERO)), whole((t, d)),
                  pl.BlockSpec((tq, tile), lambda j: (ZERO, late(j))), pl.BlockSpec((tp, tile), lambda j: (ZERO, late(j))), whole((t, d))],
        out_specs=(down(tile, d), pl.BlockSpec((ONE, tile), lambda j: (ZERO, cut(j))), whole((t, d))),
        scratch_shapes=[pltpu.VMEM((t, d), F32)],
        compiler_params=vmem(), name="qkv_backward",
    )(dq, dp, x, w_t, dr1, ctx_q, ctx_p, dr1b)


def unpack_kernel(n1, n2, n3, s_ref, a_ref, b_ref, c_ref, d_ref):
    j = pl.program_id(ZERO)
    for ref, lo, hi in ((a_ref, ZERO, n1), (b_ref, n1, n2), (c_ref, n2, n3), (d_ref, n3, pl.num_programs(ZERO))):
        @pl.when((j >= lo) & (j < hi))
        def _():
            ref[ALL] = s_ref[ALL]


def unpack(total, sizes, d, tile=TILE):
    per = d // tile
    n1, n2, n3, n4 = (sum(sizes[:i + ONE]) // tile for i in range(len(sizes)))
    part = lambda lo, hi: (lambda j: (jnp.clip(j - lo, ZERO, hi - lo - ONE), ZERO))
    up = lambda j: (lax.rem(jnp.clip(j - n2, ZERO, n3 - n2 - ONE), per), lax.div(jnp.clip(j - n2, ZERO, n3 - n2 - ONE), per))
    rows = [jax.ShapeDtypeStruct((n, d), F32) for n in sizes]
    rows[2] = jax.ShapeDtypeStruct((d, sizes[2]), F32)
    maps = (part(ZERO, n1), part(n1, n2), up, part(n3, n4))
    return pl.pallas_call(
        functools.partial(unpack_kernel, n1, n2, n3), grid=(n4,), out_shape=rows,
        in_specs=[down(tile, d)], out_specs=[pl.BlockSpec((tile, d), m) for m in maps],
        compiler_params=vmem(), name="unpack",
    )(total)


def solution(mesh):
    axis = mesh.axis_names[ZERO]
    n_dev = mesh.shape[axis]

    def local_step(q_hidden, q_mask, p_hidden, p_mask, w_qkv, b_qkv, w_out, b_out, ln1_gain, ln1_shift,
                   w_up, b_up, w_down, b_down, ln2_gain, ln2_shift):
        nq, q_len, d = q_hidden.shape
        n_pass, p_len = nq * p_hidden.shape[ONE], p_hidden.shape[2]
        _, three, heads, head = w_qkv.shape
        ff = w_up.shape[ONE]
        tq = nq * q_len
        x = jnp.concatenate([q_hidden.reshape(-ONE, d), p_hidden.reshape(-ONE, d)], axis=ZERO)
        p_mask = p_mask.reshape(n_pass, p_len)
        wqkv_t = w_qkv.transpose(ONE, 2, 3, ZERO).reshape(-ONE, d)
        wo = w_out.reshape(-ONE, d)
        none = jnp.zeros_like(b_out)
        vecs = jnp.stack([b_out, ln1_gain, ln1_shift, b_down, ln2_gain, ln2_shift, none, none])

        def pool_weights(mask):
            m = mask.astype(F32)
            return (m / jnp.sum(m, axis=ONE, keepdims=True)).reshape(-ONE, ONE)

        weights = jnp.concatenate([pool_weights(q_mask), pool_weights(p_mask)], axis=ZERO)
        bounds = tuple((i, i * q_len, q_len) for i in range(nq)) + tuple(
            (2 * nq + i, tq + i * p_len, p_len) for i in range(n_pass))

        qkv_q, qkv_p = qkv_project(x, wqkv_t, b_qkv.reshape(ONE, -ONE), tq)
        probs_q, ctx_q = attention(qkv_q, q_mask, q_len, head)
        probs_p, ctx_p = attention(qkv_p, p_mask, p_len, head)
        h, r1, g, gp, r2, pooled = ffn_forward(x, ctx_q, ctx_p, wo, vecs, weights, w_up, b_up.reshape(ONE, -ONE), w_down, bounds)

        used = (jnp.arange(pooled.shape[ZERO]) < nq) | (jnp.arange(pooled.shape[ZERO]) >= 2 * nq)
        size = jnp.sum(pooled * pooled, axis=ONE, keepdims=True)
        embed = pooled * jnp.where(used[:, None], lax.rsqrt(size), 0.0)
        everyone = gather_embeddings(embed, axis)
        mean_loss, d_pooled = loss_and_grad(everyone, pooled, axis, nq * n_dev)

        dwd, dwu, dbu, dr1, dr1b, dc_q, dc_p, dvec = ffn_backward(
            d_pooled, r2, weights, vecs, h, g, gp, w_down, w_up, r1, wo, bounds, tq)
        dq = attention_bwd(qkv_q, probs_q, dc_q, q_len, head)
        dp = attention_bwd(qkv_p, probs_p, dc_p, p_len, head)
        dwa, dbq, dh = qkv_backward(dq, dp, x, wqkv_t, dr1, ctx_q, ctx_p, dr1b)

        small = jnp.concatenate([dvec, dbq.reshape(three, d), dbu.reshape(-ONE, d), jnp.zeros((ONE, d), F32)], axis=ZERO)
        total, small = sum_over_devices((dwa, dwu.reshape(-ONE, d), dwd), small, axis)
        d_qkv, d_out, d_up, d_down = unpack(total, (three * d, d, ff, ff), d)
        vec = [small[i] for i in range(6)]
        return (mean_loss, dh[:tq].reshape(q_hidden.shape), dh[tq:].reshape(p_hidden.shape),
                d_qkv.reshape(three, heads, head, d).transpose(3, ZERO, ONE, 2), small[8:8 + three].reshape(b_qkv.shape),
                d_out.reshape(w_out.shape), vec[ZERO], vec[ONE], vec[2], d_up, small[8 + three:-ONE].reshape(-ONE),
                d_down, vec[3], vec[4], vec[5])

    in_specs = (P(axis),) * 4 + (P(),) * 12
    out_specs = (P(), P(axis), P(axis)) + (P(),) * 12
    return jax.shard_map(local_step, mesh=mesh, in_specs=in_specs, out_specs=out_specs, check_vma=False)
```

```python
import functools
import types
import jax
import jax.numpy as jnp
from jax import lax
from jax.experimental import pallas as pl
from jax.experimental.pallas import tpu as pltpu
from jax.sharding import PartitionSpec as P

ZERO, ONE, ALL = 0, 1, ...

F32 = jnp.float32
BF16 = jnp.bfloat16
LOGICAL = pl.DeviceIdType.LOGICAL
RING = 4
WIDTH = 256
COLOURS = range(6)
AXES = range(3)
RINGS = range(RING)
TURNS = range(RING * RING)
ANY = pl.BlockSpec(memory_space=pl.ANY)


def mesh_place(axis):
    me = lax.axis_index(axis)
    core = lax.rem(me, 2)
    chip = lax.div(me, 2)
    row = lax.div(chip, RING)
    return (lax.rem(chip, RING), lax.rem(row, RING), lax.div(row, RING)), core


def device_at(coords, core):
    return ((coords[2] * RING + coords[ONE]) * RING + coords[ZERO]) * 2 + core


def moved(coords, dim, by):
    out = list(coords)
    out[dim] = lax.rem(coords[dim] + by + 2 * RING, RING)
    return tuple(out)


def wrap(i):
    return lax.rem(i + 4 * RING, RING)


def rdma(src, dst, send, recv, to):
    pltpu.make_async_remote_copy(src_ref=src, dst_ref=dst, send_sem=send, recv_sem=recv,
                                 device_id=to, device_id_type=LOGICAL).start()


def copy(src, dst, sem):
    pltpu.make_async_copy(src, dst, sem).start()


def drain(ref, sem):
    pltpu.make_async_copy(ref, ref, sem).wait()


def carve(sems, *counts):
    out, at = [], ZERO
    for n in counts:
        out.append(lambda i, at=at: sems.at[at + i])
        at += n
    return out


def ring_plan(axis, units):
    coords, core = mesh_place(axis)
    p = types.SimpleNamespace(coords=coords, core=core, partner=device_at(coords, ONE - core))
    p.dims = [tuple((k // 2 + s) % 3 for s in AXES) for k in COLOURS]
    p.sign = [ONE - 2 * (k % 2) for k in COLOURS]
    p.pos = [tuple(coords[d] for d in p.dims[k]) for k in COLOURS]
    p.nxt = [tuple(device_at(moved(coords, d, p.sign[k]), core) for d in p.dims[k]) for k in COLOURS]
    p.piece = [8 * u for u in units]
    p.lead = [sum(p.piece[:k]) for k in COLOURS]
    p.all = sum(p.piece)
    p.half = 64 * p.all
    p.base = core * p.half
    p.ring_peers = [p.partner] + [device_at(moved(coords, d, by), core) for d in AXES for by in (ONE, 3)]
    p.at = lambda k, j, step, s: wrap(p.pos[k][s] - p.sign[k] * (ONE + step))
    return p


def rows(at, n):
    return pl.ds(pl.multiple_of(at, 8), n)


def chunk_row(p, k, step):
    return 64 * p.lead[k] + wrap(p.pos[k][ZERO] - p.sign[k] * (ONE + step)) * (16 * p.piece[k])


def sub_row(p, k, row, step):
    return row + wrap(p.pos[k][ONE] - p.sign[k] * (ONE + step)) * (4 * p.piece[k])


def piece_row(p, k, row, step):
    return row + wrap(p.pos[k][2] - p.sign[k] * (ONE + step)) * p.piece[k]


def signal_peers(peers):
    barrier = pltpu.get_barrier_semaphore()
    for peer in peers:
        pl.semaphore_signal(barrier, inc=ONE, device_id=peer, device_id_type=LOGICAL)


def await_peers(peers):
    pl.semaphore_wait(pltpu.get_barrier_semaphore(), len(peers))


SCATTER_SEMS = 4 + 3 * 16 + 2 * 12 + 4 * 3


def scatter_scratch(units):
    n = 8 * sum(units)
    vm = lambda *s: pltpu.VMEM(s + (WIDTH,), F32)
    return [vm(64 * n), vm(2, 4 * n), vm(3, RING, 4 * n), vm(3, 4 * n), vm(3, n), pltpu.SemaphoreType.DMA((SCATTER_SEMS,))]


def scatter_rounds(p, src, part, out, acc, stage, land1, land2, land3, sems):
    load_sem, swap_send, swap_recv, stage_sem, p1_send, p1_recv, p2_send, p2_recv, p3_send, p3_recv = carve(
        sems, 4, 16, 16, 16, 12, 12, 3, 3, 3, 3)
    n_sub, n_chunk = 4 * p.all, 16 * p.all
    far = p.half - p.base

    def turn_row(k, n):
        return sub_row(p, k, chunk_row(p, k, n // RING), n % RING)

    def load(t):
        for k in COLOURS:
            r, m = chunk_row(p, k, t), 16 * p.piece[k]
            copy(src.at[rows(p.base + r, m)], acc.at[rows(r, m)], load_sem(t))

    def swap(n):
        for k in COLOURS:
            r, m = turn_row(k, n), 4 * p.piece[k]
            rdma(src.at[rows(far + r, m)], part.at[rows(r, m)], swap_send(n), swap_recv(n), p.partner)

    def fetch(n):
        drain(part.at[pl.ds(ZERO, n_sub)], swap_recv(n))
        for k in COLOURS:
            m = 4 * p.piece[k]
            copy(part.at[rows(turn_row(k, n), m)], stage.at[n % 2, pl.ds(4 * p.lead[k], m)], stage_sem(n))

    def begin():
        for t in RINGS:
            load(t)
        for n in range(6):
            swap(n)

    def turn(n):
        t, i = n // RING, n % RING
        if n == ZERO:
            fetch(n)
        if n + 6 < 16:
            swap(n + 6)
        if n + ONE < 16:
            fetch(n + ONE)
        if i == ZERO:
            drain(acc.at[pl.ds(ZERO, n_chunk)], load_sem(t))
        drain(stage.at[n % 2], stage_sem(n))
        if t > ZERO:
            drain(land1.at[t - ONE, i], p1_recv(n - 4))
        for k in COLOURS:
            at, m = rows(turn_row(k, n), 4 * p.piece[k]), pl.ds(4 * p.lead[k], 4 * p.piece[k])
            val = acc[at] + stage[n % 2, m]
            acc[at] = val + land1[t - ONE, i, m] if t > ZERO else val
        if t < 3:
            for k in COLOURS:
                at, m = rows(turn_row(k, n), 4 * p.piece[k]), pl.ds(4 * p.lead[k], 4 * p.piece[k])
                rdma(acc.at[at], land1.at[t, i, m], p1_send(n), p1_recv(n), p.nxt[k][ZERO])

    def second(i):
        if i > ZERO:
            drain(land2.at[i - ONE], p2_recv(i - ONE))
        for k in COLOURS:
            at, m = rows(turn_row(k, 12 + i), 4 * p.piece[k]), pl.ds(4 * p.lead[k], 4 * p.piece[k])
            if i > ZERO:
                acc[at] += land2[i - ONE, m]
        if i < 3:
            for k in COLOURS:
                at, m = rows(turn_row(k, 12 + i), 4 * p.piece[k]), pl.ds(4 * p.lead[k], 4 * p.piece[k])
                rdma(acc.at[at], land2.at[i, m], p2_send(i), p2_recv(i), p.nxt[k][ONE])

    def third(g):
        if g > ZERO:
            drain(land3.at[g - ONE], p3_recv(g - ONE))
        for k in COLOURS:
            at, m = rows(piece_row(p, k, turn_row(k, 15), g), p.piece[k]), pl.ds(p.lead[k], p.piece[k])
            if g > ZERO:
                acc[at] += land3[g - ONE, m]
            if g == 3:
                out[m] = acc[at]
        if g < 3:
            for k in COLOURS:
                at, m = rows(piece_row(p, k, turn_row(k, 15), g), p.piece[k]), pl.ds(p.lead[k], p.piece[k])
                rdma(acc.at[at], land3.at[g, m], p3_send(g), p3_recv(g), p.nxt[k][2])

    def finish():
        for n in TURNS:
            drain(acc.at[pl.ds(ZERO, n_sub)], swap_send(n))
        for n in range(12):
            drain(acc.at[pl.ds(ZERO, n_sub)], p1_send(n))
        for t in AXES:
            drain(acc.at[pl.ds(ZERO, n_sub)], p2_send(t))
            drain(acc.at[pl.ds(ZERO, p.all)], p3_send(t))

    act = functools.partial
    def both(*fs):
        def run():
            for f in fs:
                f()
        return run
    steps = [begin] + [act(turn, n) for n in range(12)]
    steps += [both(act(turn, 12), act(second, ZERO)), act(turn, 13), act(turn, 14), act(turn, 15), act(second, ONE), act(second, 2),
              both(act(second, 3), act(third, ZERO)), act(third, ONE), act(third, 2), act(third, 3), finish]
    return steps


GATHER_SEMS = ONE + 2 * (3 + 3 + 12 + 16)


def gather_rounds(p, piece, out, sems):
    own_sem, a3_send, a3_recv, a2_send, a2_recv, a1_send, a1_recv, push_send, push_recv = carve(
        sems, ONE, 3, 3, 3, 3, 12, 12, 16, 16)
    n_sub = 4 * p.all

    def many(n):
        return out.at[pl.ds(ZERO, n)]

    def mine(k, c, s, g):
        return p.base + piece_row(p, k, sub_row(p, k, chunk_row(p, k, c - ONE), s - ONE), g - ONE)

    def sub_at(k, c, s):
        return rows(p.base + sub_row(p, k, chunk_row(p, k, c - ONE), s - ONE), 4 * p.piece[k])

    def hop3(t):
        for k in COLOURS:
            at = rows(mine(k, ZERO, ZERO, t), p.piece[k])
            src = piece.at[pl.ds(p.lead[k], p.piece[k])] if t == ZERO else out.at[at]
            if t == ZERO:
                copy(src, out.at[at], own_sem(ZERO))
            rdma(src, out.at[at], a3_send(t), a3_recv(t), p.nxt[k][2])

    def third(t):
        if t > ZERO:
            drain(many(p.all), a3_recv(t - ONE))
        if t < 3:
            hop3(t)
        if t == 3:
            drain(many(p.all), own_sem(ZERO))

    def hop1(c, s):
        for k in COLOURS:
            if c < 3:
                rdma(out.at[sub_at(k, c, s)], out.at[sub_at(k, c, s)], a1_send(RING * c + s), a1_recv(RING * c + s), p.nxt[k][ZERO])
            rdma(out.at[sub_at(k, c, s)], out.at[sub_at(k, c, s)], push_send(RING * c + s), push_recv(RING * c + s), p.partner)

    def second(s):
        if s > ZERO:
            drain(many(n_sub), a2_recv(s - ONE))
        if s < 3:
            for k in COLOURS:
                rdma(out.at[sub_at(k, ZERO, s)], out.at[sub_at(k, ZERO, s)], a2_send(s), a2_recv(s), p.nxt[k][ONE])
        hop1(ZERO, s)

    def first(c, s):
        drain(many(n_sub), a1_recv(RING * (c - ONE) + s))
        hop1(c, s)

    def finish():
        for t in AXES:
            drain(many(p.all), a3_send(t))
            drain(many(n_sub), a2_send(t))
        for n in range(12):
            drain(many(n_sub), a1_send(n))
        for n in TURNS:
            drain(many(n_sub), push_send(n))
            drain(many(n_sub), push_recv(n))

    act = functools.partial
    return ([act(third, t) for t in RINGS] + [act(second, s) for s in RINGS]
            + [act(first, c, s) for c in (ONE, 2, 3) for s in RINGS] + [finish])


def small_scratch(shape):
    return [pltpu.VMEM((4, 3) + shape, F32), pltpu.SemaphoreType.DMA((8,))]


def small_rounds(p, src, out, land, sems):
    places = [(None, p.core, 2)] + [(d, p.coords[d], RING) for d in AXES]

    def send(n):
        d, _, size = places[n]
        for by in range(ONE, size):
            to = p.partner if d is None else device_at(moved(p.coords, d, by), p.core)
            rdma(out, land.at[n, by - ONE], sems.at[n], sems.at[4 + n], to)

    def step(n):
        if n == ZERO:
            out[ALL] = src[ALL]
        else:
            _, place, size = places[n - ONE]
            got = land.at[n - ONE, pl.ds(ZERO, size - ONE)]
            drain(got, sems.at[4 + n - ONE])
            drain(got, sems.at[n - ONE])
            mine, total = out[ALL], None
            for q in range(size):
                val = mine
                for by in range(ONE, size):
                    val = jnp.where(lax.rem(place - q + size, size) == by, land[n - ONE, by - ONE], val)
                total = val if total is None else total + val
            out[ALL] = total
        if n < 4:
            send(n)

    return [functools.partial(step, n) for n in range(5)]


def spread(steps, slots):
    plan = [[] for _ in range(slots)]
    for i, s in enumerate(steps):
        plan[i * slots // len(steps)].append(s)
    return plan


def run_slot(plan, j, per, point):
    for s in range(len(plan) // per):
        todo = plan[s * per + point]
        if todo:
            @pl.when(j == s)
            def _():
                for f in todo:
                    f()


def all_peers(p):
    return [p.partner] + [device_at(moved(p.coords, d, by), p.core) for d in AXES for by in (ONE, 2, 3)]


def finish_kernel(axis, units_b, units_c, pieceb_ref, c_ref, small_ref, b_out, c_out, small_out, part, piecec, *scratch):
    sc, (gather_sem, gather_sem2, small_land, small_sem) = scratch[:6], scratch[6:]
    pb, pc = ring_plan(axis, units_b), ring_plan(axis, units_c)
    peers = all_peers(pb)
    signal_peers(peers)
    await_peers(peers)
    reduce_c = scatter_rounds(pc, c_ref, part, piecec, *sc)
    gather_b = gather_rounds(pb, pieceb_ref, b_out, gather_sem)
    smalls = small_rounds(pb, small_ref, small_out, small_land, small_sem)
    reduce_c[ZERO]()
    n = len(reduce_c)
    fill = spread(gather_b[:-ONE], n - 2)
    for i in range(ONE, n - ONE):
        reduce_c[i]()
        if i % 3 == ONE and i // 3 < len(smalls):
            smalls[i // 3]()
        for f in fill[i - ONE]:
            f()
    for f in gather_rounds(pc, piecec, c_out, gather_sem2):
        f()
    reduce_c[-ONE]()
    gather_b[-ONE]()


def finish_sum(axis, units_b, units_c, piece_b, c, small, collective_id):
    sds = jax.ShapeDtypeStruct
    dma = pltpu.SemaphoreType.DMA
    vm = pl.BlockSpec(memory_space=pltpu.VMEM)
    n = c.shape[ZERO]
    outs = pl.pallas_call(
        functools.partial(finish_kernel, axis, units_b, units_c),
        out_shape=(sds(c.shape, F32), sds(c.shape, F32), sds(small.shape, F32), sds((n // 2, WIDTH), F32), sds((n // 128, WIDTH), F32)),
        in_specs=[vm, ANY, vm], out_specs=(ANY, ANY, vm, ANY, vm),
        scratch_shapes=scatter_scratch(units_c) + [dma((GATHER_SEMS,)), dma((GATHER_SEMS,))] + small_scratch(small.shape),
        compiler_params=pltpu.CompilerParams(collective_id=collective_id, has_side_effects=True, vmem_limit_bytes=48 * 1024 * 1024),
        name="finish_sum",
    )(piece_b, c, small)
    return outs[:3]


def gather_kernel(axis, e_ref, g_ref, mine, theirs, swap_sem, sems_send, sems_recv, push_send, push_recv):
    coords, core = mesh_place(axis)
    partner = device_at(coords, ONE - core)
    width = e_ref.shape[ONE]
    lanes = pl.ds(pl.multiple_of(core * (width // 2), 128), width // 2)
    x, y, z = coords
    peers = [partner] + [device_at(moved(coords, d, by), core) for d in AXES for by in (ONE, 2, 3)]
    signal_peers(peers)
    await_peers(peers)

    rdma(e_ref, theirs, swap_sem.at[ZERO], swap_sem.at[ONE], partner)
    mine[ALL] = e_ref[ALL]
    drain(theirs, swap_sem.at[ONE])
    first = jnp.where(core == ZERO, mine[:, lanes], theirs[:, lanes])
    second = jnp.where(core == ZERO, theirs[:, lanes], mine[:, lanes])
    g_ref[z, y, x, ZERO:4, lanes] = first[ZERO:4]
    g_ref[z, y, x, 4:8, lanes] = second[ZERO:4]
    g_ref[z, y, x, 8:16, lanes] = first[8:16]
    g_ref[z, y, x, 16:24, lanes] = second[8:16]
    drain(e_ref, swap_sem.at[ZERO])

    def view(a, stage):
        idx = [z, y, x]
        for s in range(stage):
            idx[2 - (a + s) % 3] = slice(None)
        return g_ref.at[idx[ZERO], idx[ONE], idx[2], pl.ds(8 * a, 8), lanes]

    for stage in range(3):
        for by in (ONE, 3, 2):
            for a in range(3):
                to = device_at(moved(coords, (a + stage) % 3, by), core)
                rdma(view(a, stage), view(a, stage), sems_send.at[stage, by - ONE], sems_recv.at[stage, by - ONE], to)
        if stage == 2:
            for a in range(3):
                rdma(view(a, 2), view(a, 2), push_send.at[ZERO], push_recv.at[ZERO], partner)
        for by in (ONE, 3, 2):
            n = 4 ** stage
            shape_like = g_ref.at[ZERO, ZERO, ZERO, :, lanes] if stage == ZERO else (
                g_ref.at[ZERO, ZERO, :, :, lanes] if stage == ONE else g_ref.at[ZERO, :, :, :, lanes])
            drain(shape_like, sems_recv.at[stage, by - ONE])
            if stage == 2:
                for a in range(3):
                    far = moved(coords, (a + 2) % 3, RING - by)
                    idx = [far[2], far[ONE], far[ZERO]]
                    idx[2 - a] = slice(None)
                    idx[2 - (a + ONE) % 3] = slice(None)
                    v = g_ref.at[idx[ZERO], idx[ONE], idx[2], pl.ds(8 * a, 8), lanes]
                    rdma(v, v, push_send.at[by], push_recv.at[by], partner)
    for stage in range(3):
        shape_like = g_ref.at[ZERO, ZERO, ZERO, :, lanes] if stage == ZERO else (
            g_ref.at[ZERO, ZERO, :, :, lanes] if stage == ONE else g_ref.at[ZERO, :, :, :, lanes])
        for by in (ONE, 2, 3):
            drain(shape_like, sems_send.at[stage, by - ONE])
    for by in range(4):
        drain(g_ref.at[ZERO, :, :, :, lanes], push_send.at[by])
        drain(g_ref.at[ZERO, :, :, :, lanes], push_recv.at[by])


def gather_embeddings(e, axis, collective_id=2):
    dma = pltpu.SemaphoreType.DMA
    width = e.shape[ONE]
    g = pl.pallas_call(
        functools.partial(gather_kernel, axis),
        out_shape=jax.ShapeDtypeStruct((RING, RING, RING, 24, width), F32),
        in_specs=[pl.BlockSpec(memory_space=pltpu.VMEM)],
        out_specs=pl.BlockSpec(memory_space=pltpu.VMEM),
        scratch_shapes=[pltpu.VMEM(e.shape, F32), pltpu.VMEM(e.shape, F32), dma((2,)),
                        dma((3, 3)), dma((3, 3)), dma((4,)), dma((4,))],
        compiler_params=pltpu.CompilerParams(collective_id=collective_id, has_side_effects=True,
                                             vmem_limit_bytes=16 * 1024 * 1024),
        name="gather_embeddings",
    )(e)
    return g.reshape(RING ** 3, 24, width)


def loss_kernel(axis, n_query, g_ref, pooled_ref, loss_ref, d_ref, logit_ref, lse_ref):
    me = lax.axis_index(axis)
    core, chip = lax.rem(me, 2), lax.div(me, 2)
    width = pooled_ref.shape[ONE]
    chips = g_ref.shape[ZERO]
    gs = 100.0 / n_query
    hi = lax.Precision.HIGHEST
    nt = (((ONE,), (ONE,)), ((), ()))
    pall = g_ref[:, 8:24, :].reshape(chips * 16, width)
    block = 128
    per = block // 8

    def chunk(b, loss):
        qb = g_ref[pl.ds(b * per, per), ZERO:8, :].reshape(block, width)
        s = lax.dot_general(qb, pall, nt, precision=hi, preferred_element_type=F32) * 100.0
        logit_ref[pl.ds(pl.multiple_of(b * block, block), block), :] = s
        top = jnp.max(s, axis=ONE, keepdims=True)
        lse = jnp.log(jnp.sum(jnp.exp(s - top), axis=ONE, keepdims=True)) + top
        lse_ref[pl.ds(pl.multiple_of(b * block, block), block), :] = jnp.broadcast_to(lse, (block, 128))
        row = lax.broadcasted_iota(jnp.int32, s.shape, ZERO) + b * block
        col = lax.broadcasted_iota(jnp.int32, s.shape, ONE)
        pos = jnp.sum(jnp.where(col == 2 * row, s, 0.0), axis=ONE, keepdims=True)
        return loss + jnp.sum(lse - pos, axis=ZERO, keepdims=True)

    loss = lax.fori_loop(ZERO, chips // per, chunk, jnp.zeros((ONE, ONE), F32))
    loss_ref[ALL] = jnp.broadcast_to(loss * (1.0 / n_query), loss_ref.shape)

    at = pl.multiple_of(chip * 8, 8)
    s8 = logit_ref[pl.ds(at, 8), :]
    l8 = lse_ref[pl.ds(at, 8), ZERO:ONE]
    row = lax.broadcasted_iota(jnp.int32, s8.shape, ZERO) + chip * 8
    col = lax.broadcasted_iota(jnp.int32, s8.shape, ONE)
    w8 = jnp.exp(s8 - l8) * gs - jnp.where(col == 2 * row, gs, 0.0)
    dq8 = lax.dot_general(w8, pall, (((ONE,), (ZERO,)), ((), ())), precision=hi, preferred_element_type=F32)

    qall = g_ref[:, ZERO:8, :].reshape(chips * 8, width)
    p16 = g_ref[chip, 8:24, :]
    s16 = lax.dot_general(qall, p16, nt, precision=hi, preferred_element_type=F32) * 100.0
    row = lax.broadcasted_iota(jnp.int32, s16.shape, ZERO)
    col = lax.broadcasted_iota(jnp.int32, s16.shape, ONE) + chip * 16
    w16 = jnp.exp(s16 - lse_ref[:, ZERO:ONE]) * gs - jnp.where(col == 2 * row, gs, 0.0)
    dp16 = lax.dot_general(w16, qall, (((ZERO,), (ZERO,)), ((), ())), precision=hi, preferred_element_type=F32)

    dq = jnp.where(core == ZERO, dq8[ZERO:4], dq8[4:8])
    dp = jnp.where(core == ZERO, dp16[ZERO:8], dp16[8:16])
    pooled_q, pooled_p = pooled_ref[ZERO:4], pooled_ref[8:16]

    def back(d, pooled):
        inv = lax.rsqrt(jnp.sum(pooled * pooled, axis=ONE, keepdims=True))
        e = pooled * inv
        return (d - e * jnp.sum(e * d, axis=ONE, keepdims=True)) * inv

    d_ref[ALL] = jnp.zeros_like(d_ref)
    d_ref[ZERO:4, :] = back(dq, pooled_q)
    d_ref[8:16, :] = back(dp, pooled_p)


def loss_and_grad(g, pooled, axis, n_query):
    chips, _, width = g.shape
    loss, d = pl.pallas_call(
        functools.partial(loss_kernel, axis, n_query),
        out_shape=(jax.ShapeDtypeStruct((8, 128), F32), jax.ShapeDtypeStruct(pooled.shape, F32)),
        in_specs=[pl.BlockSpec(memory_space=pltpu.VMEM)] * 2,
        out_specs=(pl.BlockSpec(memory_space=pltpu.VMEM),) * 2,
        scratch_shapes=[pltpu.VMEM((chips * 8, chips * 16), F32), pltpu.VMEM((chips * 8, 128), F32)],
        compiler_params=pltpu.CompilerParams(vmem_limit_bytes=48 * 1024 * 1024),
        name="loss_and_grad",
    )(g, pooled)
    return loss[ZERO, ZERO], d


NN = (((ONE,), (ZERO,)), ((), ()))
NT = (((ONE,), (ONE,)), ((), ()))
TN = (((ZERO,), (ZERO,)), ((), ()))
LN_EPS = 1e-12
NEG_FILL = -1e9
TILE = 512
UNITS_A, UNITS_B, UNITS_C = (3, 3, 3, 3, 2, 2), (3, 3, 2, 2, 3, 3), (2, 2, 3, 3, 3, 3)
sds = jax.ShapeDtypeStruct


def mm(a, b, dims=NN):
    return lax.dot_general(a, b, dims, preferred_element_type=F32)


def vmem(mb=60):
    return pltpu.CompilerParams(vmem_limit_bytes=mb * 1024 * 1024)


def whole(*shape):
    return pl.BlockSpec(shape, lambda j: (ZERO,) * len(shape), pipeline_mode=pl.Buffered(ONE))


def across(rows, tile):
    return pl.BlockSpec((rows, tile), lambda j: (ZERO, j))


def down(tile, cols):
    return pl.BlockSpec((tile, cols), lambda j: (j, ZERO))


def row_mean(x):
    return jnp.mean(x, axis=ONE, keepdims=True)


def row_sum(x):
    return jnp.sum(x, axis=ONE, keepdims=True)


def col_sum(x):
    return jnp.sum(x, axis=ZERO, keepdims=True)


def qkv_kernel(x_ref, w_ref, b_ref, oq_ref, op_ref):
    y = (mm(x_ref[ALL], w_ref[ALL], NT) + b_ref[ALL]).astype(BF16)
    tq = oq_ref.shape[ZERO]
    oq_ref[ALL] = y[:tq]
    op_ref[ALL] = y[tq:]


def qkv_project(x, w_t, b, tq, tile=TILE):
    t, d = x.shape
    f = w_t.shape[ZERO]
    return pl.pallas_call(
        qkv_kernel, grid=(f // tile,),
        out_shape=(sds((tq, f), BF16), sds((t - tq, f), BF16)),
        in_specs=[whole(t, d), down(tile, d), across(ONE, tile)],
        out_specs=(across(tq, tile), across(t - tq, tile)),
        compiler_params=vmem(), name="qkv_project",
    )(x, w_t, b)


def split_heads(pair, head):
    lane = lax.broadcasted_iota(jnp.int32, pair.shape, ONE)
    zero = jnp.zeros_like(pair)
    return jnp.concatenate([jnp.where(lane < head, pair, zero), jnp.where(lane >= head, pair, zero)], axis=ZERO)


def join_heads(stacked, head):
    t = stacked.shape[ZERO] // 2
    lane = lax.broadcasted_iota(jnp.int32, (t, stacked.shape[ONE]), ONE)
    return jnp.where(lane < head, stacked[:t], stacked[t:])


def attn_kernel(scale, head, qkv_ref, mask_ref, probs_ref, ctx_ref):
    d = ctx_ref.shape[ONE]
    pair = 2 * head
    keep = mask_ref[ZERO] > ZERO
    for g in range(d // pair):
        at = pl.ds(g * pair, pair)
        q = split_heads(qkv_ref[:, at], head)
        k = qkv_ref[:, pl.ds(d + g * pair, pair)]
        v = qkv_ref[:, pl.ds(2 * d + g * pair, pair)]
        s = jnp.where(keep, mm(q, k, NT) * scale, NEG_FILL)
        e = jnp.exp(s - jnp.max(s, axis=ONE, keepdims=True))
        p = (e / row_sum(e)).astype(BF16)
        probs_ref[ZERO, g] = p
        ctx_ref[:, at] = join_heads(mm(p, v), head).astype(BF16)


def attention(qkv, mask, head):
    n, seq = mask.shape
    d = qkv.shape[ONE] // 3
    pairs = d // (2 * head)
    return pl.pallas_call(
        functools.partial(attn_kernel, head ** -0.5, head), grid=(n,),
        out_shape=(sds((n, pairs, 2 * seq, seq), BF16), sds((n * seq, d), BF16)),
        in_specs=[down(seq, 3 * d), pl.BlockSpec((ONE, ONE, seq), lambda j: (j, ZERO, ZERO))],
        out_specs=(pl.BlockSpec((ONE, pairs, 2 * seq, seq), lambda j: (j, ZERO, ZERO, ZERO)), down(seq, d)),
        compiler_params=vmem(), name="attention",
    )(qkv, mask.reshape(n, ONE, seq))


def norm_rows(x):
    c = x - row_mean(x)
    r = lax.rsqrt(row_mean(c * c) + LN_EPS)
    return c * r, r


def norm_back(g, hat, r):
    return r * (g - row_mean(g) - hat * row_mean(g * hat))


ERFC = (0.07122347, -0.27794802, 0.29668747, -0.02018065, 0.21581222, 0.21731356, 0.24887118, 0.24822095)


def gelu_parts(u):
    bell = jnp.exp(-0.5 * u * u)
    t = 1.0 / (1.0 + 0.311126984 * jnp.abs(u))
    poly = ERFC[ZERO]
    for c in ERFC[ONE:]:
        poly = poly * t + c
    tail = 0.5 * bell * (poly * t)
    return jnp.where(u >= 0.0, 1.0 - tail, tail), u * bell * 0.3989422804


ROWS = 304


def ffn_kernel(bounds, x_ref, cq_ref, cp_ref, wo_ref, vec_ref, wt_ref, wu_ref, bu_ref, wd_ref,
               h_ref, r1q_ref, r1p_ref, g_ref, gp_ref, r2_ref, pool_ref):
    j = pl.program_id(ZERO)
    t = x_ref.shape[ZERO]
    tq = cq_ref.shape[ZERO]
    b_out, g1, s1, b_down, g2, s2 = (vec_ref[i:i + ONE, :] for i in range(6))

    @pl.when(j == ZERO)
    def _():
        for ref, r_ref, lo in ((cq_ref, r1q_ref, ZERO), (cp_ref, r1p_ref, tq)):
            n = ref.shape[ZERO]
            size = min(n, 256)
            for a in range(ZERO, n, size):
                at = pl.ds(lo + a, size)
                r1 = x_ref[at, :].astype(F32) + mm(ref[pl.ds(a, size), :], wo_ref[ALL]) + b_out
                r_ref[pl.ds(a, size), :] = r1
                h = (norm_rows(r1)[ZERO] * g1 + s1).astype(BF16)
                h_ref[at, :] = h
                r2_ref[at, :] = h.astype(F32) + b_down

    for a in range(ZERO, t, ROWS):
        at = pl.ds(a, ROWS)
        u = mm(h_ref[at, :], wu_ref[ALL]) + bu_ref[ALL]
        cdf, upd = gelu_parts(u)
        g = (u * cdf).astype(BF16)
        g_ref[at, :] = g
        gp_ref[at, :] = cdf + upd
        r2_ref[at, :] += mm(g, wd_ref[ALL])

    @pl.when(j == pl.num_programs(ZERO) - ONE)
    def _():
        pool_ref[ALL] = jnp.zeros_like(pool_ref)
        for row, lo, n in bounds:
            at = pl.ds(lo, n)
            y = norm_rows(r2_ref[at, :])[ZERO] * g2 + s2
            pool_ref[row:row + ONE, :] = col_sum(y * wt_ref[at, :])


def ffn_forward(x, ctx_q, ctx_p, w_out, vecs, weights, w_up, b_up, w_down, bounds, tile=TILE):
    t, d = x.shape
    tq, tp = ctx_q.shape[ZERO], ctx_p.shape[ZERO]
    f = w_up.shape[ONE]
    return pl.pallas_call(
        functools.partial(ffn_kernel, bounds), grid=(f // tile,),
        out_shape=(sds((t, d), BF16), sds((tq, d), F32), sds((tp, d), F32), sds((t, f), BF16), sds((t, f), F32),
                   sds((t, d), F32), sds((16, d), F32)),
        in_specs=[whole(t, d), whole(tq, d), whole(tp, d), whole(d, d), whole(*vecs.shape), whole(t, ONE),
                  across(d, tile), across(ONE, tile), down(tile, d)],
        out_specs=(whole(t, d), whole(tq, d), whole(tp, d), across(t, tile), across(t, tile), whole(t, d), whole(16, d)),
        compiler_params=vmem(), name="ffn_forward",
    )(x, ctx_q, ctx_p, w_out, vecs, weights, w_up, b_up, w_down)


def store_blocks(ref, val):
    for c in range(ref.shape[ZERO]):
        ref[c] = val[:, c * WIDTH:(c + ONE) * WIDTH]


def down_bwd_kernel(bounds, dpool_ref, r2_ref, wt_ref, vec_ref, g_ref, dwd_ref, dr2_ref, dr2b_ref, dvec_ref):
    g2 = vec_ref[4:5, :]

    @pl.when(pl.program_id(ZERO) == ZERO)
    def _():
        dvec_ref[ALL] = jnp.zeros_like(dvec_ref)
        for row, lo, n in bounds:
            at = pl.ds(lo, n)
            hat, r = norm_rows(r2_ref[at, :])
            dy = wt_ref[at, :] * dpool_ref[row:row + ONE, :]
            dr2 = norm_back(dy * g2, hat, r)
            dr2_ref[at, :] = dr2
            dr2b_ref[at, :] = dr2.astype(BF16)
            dvec_ref[ZERO:ONE, :] += col_sum(dr2)
            dvec_ref[ONE:2, :] += col_sum(dy * hat)
            dvec_ref[2:3, :] += col_sum(dy)

    store_blocks(dwd_ref, mm(g_ref[ALL], dr2b_ref[ALL], TN))


def down_backward(dpool, r2, weights, vecs, g, bounds, tile=TILE):
    t, d = r2.shape
    f = g.shape[ONE]
    n = d // WIDTH
    return pl.pallas_call(
        functools.partial(down_bwd_kernel, bounds), grid=(f // tile,),
        out_shape=(sds((n, f, WIDTH), F32), sds((t, d), F32), sds((t, d), BF16), sds((8, d), F32)),
        in_specs=[whole(*dpool.shape), whole(t, d), whole(t, ONE), whole(*vecs.shape), across(t, tile)],
        out_specs=(pl.BlockSpec((n, tile, WIDTH), lambda j: (ZERO, j, ZERO)), whole(t, d), whole(t, d), whole(8, d)),
        compiler_params=vmem(), name="down_backward",
    )(dpool, r2, weights, vecs, g)


def up_bwd_kernel(axis, dr2_ref, dr2b_ref, h_ref, gp_ref, wd_ref, wu_ref, a_ref,
                  dwu_ref, dbu_ref, dnq_ref, dnp_ref, piece_ref, part_ref, ht_ref, *scratch):
    j = pl.program_id(ZERO)
    tq = dnq_ref.shape[ZERO]
    p = ring_plan(axis, UNITS_A)
    peers = p.ring_peers
    points = 3
    steps = scatter_rounds(p, a_ref, part_ref, piece_ref, *scratch)
    plan = spread([functools.partial(signal_peers, peers), functools.partial(await_peers, peers)] + steps,
                  points * STEPS)

    @pl.when(j == ZERO)
    def _():
        ht_ref[ALL] = h_ref[ALL].T
        dnq_ref[ALL] = dr2_ref[:tq, :]
        dnp_ref[ALL] = dr2_ref[tq:, :]

    run_slot(plan, j, points, ZERO)
    dg = mm(dr2b_ref[ALL], wd_ref[ALL], NT).astype(BF16).astype(F32)
    dpre = dg * gp_ref[ALL]
    dbu_ref[ALL] = col_sum(dpre)
    dpre = dpre.astype(BF16)
    run_slot(plan, j, points, ONE)
    dwu = mm(ht_ref[ALL], dpre)
    for c in range(dwu_ref.shape[ZERO]):
        dwu_ref[c] = dwu[:, c * WIDTH:(c + ONE) * WIDTH]
    run_slot(plan, j, points, 2)
    dnq_ref[ALL] += mm(dpre[:tq], wu_ref[ALL], NT)
    dnp_ref[ALL] += mm(dpre[tq:], wu_ref[ALL], NT)


STEPS = 8


def up_backward(axis, dr2, dr2b, h, gp, w_down, w_up, part_a, tq, collective_id, tile=TILE):
    t, d = h.shape
    f = w_up.shape[ONE]
    n = tile // WIDTH
    total = part_a.shape[ZERO]
    return pl.pallas_call(
        functools.partial(up_bwd_kernel, axis), grid=(f // tile,),
        out_shape=(sds((f // WIDTH, d, WIDTH), F32), sds((ONE, f), F32), sds((tq, d), F32), sds((t - tq, d), F32),
                   sds((total // 128, WIDTH), F32), sds((total // 2, WIDTH), F32)),
        in_specs=[whole(t, d), whole(t, d), whole(t, d), across(t, tile), down(tile, d), across(d, tile), ANY],
        out_specs=(pl.BlockSpec((n, d, WIDTH), lambda j: (j, ZERO, ZERO)), across(ONE, tile), whole(tq, d), whole(t - tq, d),
                   whole(total // 128, WIDTH), ANY),
        scratch_shapes=[pltpu.VMEM((d, t), BF16)] + scatter_scratch(UNITS_A),
        compiler_params=pltpu.CompilerParams(collective_id=collective_id, has_side_effects=True, vmem_limit_bytes=63 * 1024 * 1024),
        name="up_backward",
    )(dr2, dr2b, h, gp, w_down, w_up, part_a)


def attn_bwd_body(scale, head, dn_ref, r1_ref, vec_ref, wo_ref, qkv_ref, probs_ref, d_ref, dr1_ref, dr1b_ref, dvec_ref, pause):
    d = dn_ref.shape[ONE]
    pair = 2 * head
    dy = dn_ref[ALL].astype(BF16).astype(F32)
    hat, r = norm_rows(r1_ref[ALL])
    dr1 = norm_back(dy * vec_ref[ONE:2, :], hat, r)
    dr1_ref[ALL] = dr1
    low = dr1.astype(BF16)
    dr1b_ref[ALL] = low

    @pl.when(pl.program_id(ZERO) == ZERO)
    def _():
        dvec_ref[ALL] = jnp.zeros_like(dvec_ref)
    dvec_ref[ZERO:ONE, :] += col_sum(dr1)
    dvec_ref[ONE:2, :] += col_sum(dy * hat)
    dvec_ref[2:3, :] += col_sum(dy)
    dctx = mm(low, wo_ref[ALL], NT).astype(BF16)
    pause(ZERO)
    for g in range(d // pair):
        if 2 * g == d // pair:
            pause(ONE)
        at = pl.ds(g * pair, pair)
        q = split_heads(qkv_ref[:, at], head)
        k = qkv_ref[:, pl.ds(d + g * pair, pair)]
        v = qkv_ref[:, pl.ds(2 * d + g * pair, pair)]
        p = probs_ref[ZERO, g]
        dc = split_heads(dctx[:, g * pair:(g + ONE) * pair], head)
        dp = mm(dc, v, NT)
        pf = p.astype(F32)
        ds = (pf * (dp - row_sum(dp * pf)) * scale).astype(BF16)
        d_ref[:, at] = join_heads(mm(ds, k), head).astype(BF16)
        d_ref[:, pl.ds(d + g * pair, pair)] = mm(ds, q, TN).astype(BF16)
        d_ref[:, pl.ds(2 * d + g * pair, pair)] = mm(p, dc, TN).astype(BF16)
    pause(2)


def attn_bwd_plain(scale, head, *refs):
    attn_bwd_body(scale, head, *refs, lambda point: None)


def attn_bwd_host(scale, head, axis, dn_ref, r1_ref, vec_ref, wo_ref, qkv_ref, probs_ref, b_ref,
                  d_ref, dr1_ref, dr1b_ref, dvec_ref, piece_ref, part_ref, *scratch):
    p = ring_plan(axis, UNITS_B)
    peers = p.ring_peers
    points = 3
    steps = scatter_rounds(p, b_ref, part_ref, piece_ref, *scratch)
    plan = spread([functools.partial(signal_peers, peers), functools.partial(await_peers, peers)] + steps,
                  points * STEPS)
    j = pl.program_id(ZERO)
    attn_bwd_body(scale, head, dn_ref, r1_ref, vec_ref, wo_ref, qkv_ref, probs_ref, d_ref, dr1_ref, dr1b_ref, dvec_ref,
                  functools.partial(run_slot, plan, j, points))


def attention_bwd(dn, r1, vecs, w_out, qkv, probs, head, axis=None, part_b=None, collective_id=None):
    n, pairs, _, seq = probs.shape
    d = dn.shape[ONE]
    scale = head ** -0.5
    in_specs = [down(seq, d), down(seq, d), whole(*vecs.shape), whole(d, d), down(seq, 3 * d),
                pl.BlockSpec((ONE, pairs, 2 * seq, seq), lambda j: (j, ZERO, ZERO, ZERO))]
    out_shape = [sds((n * seq, 3 * d), BF16), sds((n * seq, d), F32), sds((n * seq, d), BF16), sds((8, d), F32)]
    out_specs = [down(seq, 3 * d), down(seq, d), down(seq, d), whole(8, d)]
    args = (dn, r1, vecs, w_out, qkv, probs)
    if part_b is None:
        return pl.pallas_call(
            functools.partial(attn_bwd_plain, scale, head), grid=(n,), out_shape=out_shape, in_specs=in_specs, out_specs=out_specs,
            compiler_params=vmem(), name="attention_bwd")(*args)
    total = part_b.shape[ZERO]
    return pl.pallas_call(
        functools.partial(attn_bwd_host, scale, head, axis), grid=(n,),
        out_shape=out_shape + [sds((total // 128, WIDTH), F32), sds((total // 2, WIDTH), F32)],
        in_specs=in_specs + [ANY], out_specs=out_specs + [whole(total // 128, WIDTH), ANY],
        scratch_shapes=scatter_scratch(UNITS_B),
        compiler_params=pltpu.CompilerParams(collective_id=collective_id, has_side_effects=True, vmem_limit_bytes=60 * 1024 * 1024),
        name="attention_bwd_host")(*args, part_b)


def qkv_bwd_kernel(axis, steps, dq_ref, dp_ref, x_ref, w_ref, dr1q_ref, dr1p_ref, cq_ref, cp_ref, dr1bq_ref, dr1bp_ref, piece_ref,
                   dw_ref, db_ref, dhq_ref, dhp_ref, a_ref, accq_ref, accp_ref, sems):
    j = pl.program_id(ZERO)
    tq = dq_ref.shape[ZERO]
    p = ring_plan(axis, UNITS_A)
    peers = p.ring_peers
    points = 2
    plan = spread([functools.partial(signal_peers, peers), functools.partial(await_peers, peers)]
                  + gather_rounds(p, piece_ref, a_ref, sems), points * STEPS)
    run_slot(plan, j, points, ZERO)

    @pl.when(j == ZERO)
    def _():
        accq_ref[ALL] = dr1q_ref[ALL]
        accp_ref[ALL] = dr1p_ref[ALL]

    @pl.when(j < steps)
    def _():
        accq_ref[ALL] += mm(dq_ref[ALL], w_ref[ALL])
        accp_ref[ALL] += mm(dp_ref[ALL], w_ref[ALL])
        store_blocks(dw_ref, mm(dq_ref[ALL], x_ref[:tq, :], TN) + mm(dp_ref[ALL], x_ref[tq:, :], TN))
        db_ref[ALL] = col_sum(dq_ref[ALL].astype(F32)) + col_sum(dp_ref[ALL].astype(F32))

    @pl.when(j == steps - ONE)
    def _():
        dhq_ref[ALL] = accq_ref[ALL].astype(BF16)
        dhp_ref[ALL] = accp_ref[ALL].astype(BF16)

    @pl.when(j >= steps)
    def _():
        store_blocks(dw_ref, mm(cq_ref[ALL], dr1bq_ref[ALL], TN) + mm(cp_ref[ALL], dr1bp_ref[ALL], TN))
    run_slot(plan, j, points, ONE)


def qkv_backward(axis, dq, dp, x, w_t, dr1_q, dr1_p, ctx_q, ctx_p, dr1b_q, dr1b_p, piece, collective_id, tile=TILE):
    t, d = x.shape
    f = w_t.shape[ZERO]
    tq, tp = dq.shape[ZERO], dp.shape[ZERO]
    n, m = f // tile, d // tile
    cut = lambda j: (ZERO, jnp.minimum(j, n - ONE))
    late = lambda j: (ZERO, jnp.maximum(j - n, ZERO))
    cols = d // WIDTH
    return pl.pallas_call(
        functools.partial(qkv_bwd_kernel, axis, n), grid=(n + m,),
        out_shape=(sds((cols, f + d, WIDTH), F32), sds((ONE, f), F32), sds((tq, d), BF16), sds((tp, d), BF16),
                   sds((piece.shape[ZERO] * 128, WIDTH), F32)),
        in_specs=[pl.BlockSpec((tq, tile), cut), pl.BlockSpec((tp, tile), cut),
                  whole(t, d), pl.BlockSpec((tile, d), lambda j: (jnp.minimum(j, n - ONE), ZERO)), whole(tq, d), whole(tp, d),
                  pl.BlockSpec((tq, tile), late), pl.BlockSpec((tp, tile), late), whole(tq, d), whole(tp, d), whole(*piece.shape)],
        out_specs=(pl.BlockSpec((cols, tile, WIDTH), lambda j: (ZERO, j, ZERO)), pl.BlockSpec((ONE, tile), cut), whole(tq, d), whole(tp, d), ANY),
        scratch_shapes=[pltpu.VMEM((tq, d), F32), pltpu.VMEM((tp, d), F32), pltpu.SemaphoreType.DMA((GATHER_SEMS,))],
        compiler_params=pltpu.CompilerParams(collective_id=collective_id, has_side_effects=True, vmem_limit_bytes=60 * 1024 * 1024),
        name="qkv_backward",
    )(dq, dp, x, w_t, dr1_q, dr1_p, ctx_q, ctx_p, dr1b_q, dr1b_p, piece)


def unpack_kernel(n1, n2, n3, a_ref, b_ref, c_ref, qkv_ref, out_ref, up_ref, down_ref):
    j = pl.program_id(ZERO)

    def join(ref, src, lo, hi):
        @pl.when((j >= lo) & (j < hi))
        def _():
            for c in range(src.shape[ZERO]):
                ref[:, c * WIDTH:(c + ONE) * WIDTH] = src[c]
    join(down_ref, a_ref, ZERO, n1)
    join(up_ref, b_ref, n1, n2)
    join(qkv_ref, c_ref, n2, n3)
    join(out_ref, c_ref, n3, pl.num_programs(ZERO))


def unpack(a, b, c, three, d, tile=TILE):
    ff = a.shape[ONE]
    n1, n2, n3, n4 = ff // tile, 2 * ff // tile, (2 * ff + three * d) // tile, (2 * ff + (three + ONE) * d) // tile
    part = lambda lo, hi: (lambda j: jnp.clip(j - lo, ZERO, hi - lo - ONE))
    ja, jb, jc, jq, jo = part(ZERO, n1), part(n1, n2), part(n2, n4), part(n2, n3), part(n3, n4)
    return pl.pallas_call(
        functools.partial(unpack_kernel, n1, n2, n3), grid=(n4,),
        out_shape=(sds((three * d, d), F32), sds((d, d), F32), sds((d, ff), F32), sds((ff, d), F32)),
        in_specs=[pl.BlockSpec((d // WIDTH, tile, WIDTH), lambda j: (ZERO, ja(j), ZERO)),
                  pl.BlockSpec((tile // WIDTH, d, WIDTH), lambda j: (jb(j), ZERO, ZERO)),
                  pl.BlockSpec((d // WIDTH, tile, WIDTH), lambda j: (ZERO, jc(j), ZERO))],
        out_specs=(pl.BlockSpec((tile, d), lambda j: (jq(j), ZERO)), pl.BlockSpec((tile, d), lambda j: (jo(j), ZERO)),
                   pl.BlockSpec((d, tile), lambda j: (ZERO, jb(j))), pl.BlockSpec((tile, d), lambda j: (ja(j), ZERO))),
        compiler_params=vmem(), name="unpack",
    )(a, b, c)


def solution(mesh):
    axis = mesh.axis_names[ZERO]
    n_dev = mesh.shape[axis]

    def local_step(q_hidden, q_mask, p_hidden, p_mask, w_qkv, b_qkv, w_out, b_out, ln1_gain, ln1_shift,
                   w_up, b_up, w_down, b_down, ln2_gain, ln2_shift):
        nq, q_len, d = q_hidden.shape
        n_pass, p_len = nq * p_hidden.shape[ONE], p_hidden.shape[2]
        _, three, heads, head = w_qkv.shape
        tq = nq * q_len
        x = jnp.concatenate([q_hidden.reshape(-ONE, d), p_hidden.reshape(-ONE, d)], axis=ZERO)
        p_mask = p_mask.reshape(n_pass, p_len)
        wqkv_t = w_qkv.transpose(ONE, 2, 3, ZERO).reshape(-ONE, d)
        wo = w_out.reshape(-ONE, d)
        none = jnp.zeros_like(b_out)
        vecs = jnp.stack([b_out, ln1_gain, ln1_shift, b_down, ln2_gain, ln2_shift, none, none])

        def pool_weights(mask):
            m = mask.astype(F32)
            return (m / row_sum(m)).reshape(-ONE, ONE)

        weights = jnp.concatenate([pool_weights(q_mask), pool_weights(p_mask)], axis=ZERO)
        bounds = tuple((i, i * q_len, q_len) for i in range(nq)) + tuple(
            (2 * nq + i, tq + i * p_len, p_len) for i in range(n_pass))

        qkv_q, qkv_p = qkv_project(x, wqkv_t, b_qkv.reshape(ONE, -ONE), tq)
        probs_q, ctx_q = attention(qkv_q, q_mask, head)
        probs_p, ctx_p = attention(qkv_p, p_mask, head)
        h, r1_q, r1_p, g, gp, r2, pooled = ffn_forward(
            x, ctx_q, ctx_p, wo, vecs, weights, w_up, b_up.reshape(ONE, -ONE), w_down, bounds)

        used = (jnp.arange(pooled.shape[ZERO]) < nq) | (jnp.arange(pooled.shape[ZERO]) >= 2 * nq)
        embed = pooled * jnp.where(used[:, None], lax.rsqrt(row_sum(pooled * pooled)), 0.0)
        everyone = gather_embeddings(embed, axis, ONE)
        mean_loss, d_pooled = loss_and_grad(everyone, pooled, axis, nq * n_dev)

        dwd, dr2, dr2b, dvec2 = down_backward(d_pooled, r2, weights, vecs, g, bounds)
        dwu, dbu, dn_q, dn_p, piece_a, _ = up_backward(axis, dr2, dr2b, h, gp, w_down, w_up, dwd.reshape(-ONE, WIDTH), tq, 2)
        dq, dr1_q, dr1b_q, dvec_q = attention_bwd(dn_q, r1_q, vecs, wo, qkv_q, probs_q, head)
        dp, dr1_p, dr1b_p, dvec_p, piece_b, _ = attention_bwd(
            dn_p, r1_p, vecs, wo, qkv_p, probs_p, head, axis, dwu.reshape(-ONE, WIDTH), 3)
        dwa, dbq, dh_q, dh_p, a = qkv_backward(
            axis, dq, dp, x, wqkv_t, dr1_q, dr1_p, ctx_q, ctx_p, dr1b_q, dr1b_p, piece_a, 4)
        small = jnp.concatenate([(dvec_q + dvec_p)[:3], dvec2[:3], jnp.zeros((2, d), F32), dbq.reshape(three, d), dbu.reshape(-ONE, d),
                                 jnp.zeros((ONE, d), F32)], axis=ZERO)
        b, c, small = finish_sum(axis, UNITS_B, UNITS_C, piece_b, dwa.reshape(-ONE, WIDTH), small, 5)
        d_qkv, d_out, d_up, d_down = unpack(a.reshape(dwd.shape), b.reshape(dwu.shape), c.reshape(dwa.shape), three, d)
        vec = [small[i] for i in range(6)]
        return (mean_loss, dh_q.reshape(q_hidden.shape), dh_p.reshape(p_hidden.shape),
                d_qkv.reshape(three, heads, head, d).transpose(3, ZERO, ONE, 2), small[8:8 + three].reshape(b_qkv.shape),
                d_out.reshape(w_out.shape), vec[ZERO], vec[ONE], vec[2], d_up, small[8 + three:-ONE].reshape(-ONE),
                d_down, vec[3], vec[4], vec[5])

    in_specs = (P(axis),) * 4 + (P(),) * 12
    out_specs = (P(), P(axis), P(axis)) + (P(),) * 12
    return jax.shard_map(local_step, mesh=mesh, in_specs=in_specs, out_specs=out_specs, check_vma=False)
```

```python
import functools
import types
import jax
import jax.numpy as jnp
from jax import lax
from jax.experimental import pallas as pl
from jax.experimental.pallas import tpu as pltpu
from jax.sharding import PartitionSpec as P

ZERO, ONE, TWO, THREE, ALL = 0, 1, 2, 3, ...

F32 = jnp.float32
BF16 = jnp.bfloat16
LOGICAL = pl.DeviceIdType.LOGICAL
RING = 4
WIDTH = 256
COLOURS = range(6)
AXES = range(THREE)
RINGS = range(RING)
TURNS = range(RING * RING)
ANY = pl.BlockSpec(memory_space=pl.ANY)


def mesh_place(axis):
    me = lax.axis_index(axis)
    core = lax.rem(me, TWO)
    chip = lax.div(me, TWO)
    row = lax.div(chip, RING)
    return (lax.rem(chip, RING), lax.rem(row, RING), lax.div(row, RING)), core


def device_at(coords, core):
    return ((coords[TWO] * RING + coords[ONE]) * RING + coords[ZERO]) * TWO + core


def moved(coords, dim, by):
    out = list(coords)
    out[dim] = lax.rem(coords[dim] + by + TWO * RING, RING)
    return tuple(out)


def wrap(i):
    return lax.rem(i + 4 * RING, RING)


def rdma(src, dst, send, recv, to):
    pltpu.make_async_remote_copy(src_ref=src, dst_ref=dst, send_sem=send, recv_sem=recv,
                                 device_id=to, device_id_type=LOGICAL).start()


def copy(src, dst, sem):
    pltpu.make_async_copy(src, dst, sem).start()


def drain(ref, sem):
    pltpu.make_async_copy(ref, ref, sem).wait()


def carve(sems, *counts):
    out, at = [], ZERO
    for n in counts:
        out.append(lambda i, at=at: sems.at[at + i])
        at += n
    return out


def ring_plan(axis, units):
    coords, core = mesh_place(axis)
    p = types.SimpleNamespace(coords=coords, core=core, partner=device_at(coords, ONE - core))
    p.dims = [tuple((k // TWO + s) % THREE for s in AXES) for k in COLOURS]
    p.sign = [ONE - TWO * (k % TWO) for k in COLOURS]
    p.pos = [tuple(coords[d] for d in p.dims[k]) for k in COLOURS]
    p.nxt = [tuple(device_at(moved(coords, d, p.sign[k]), core) for d in p.dims[k]) for k in COLOURS]
    p.piece = [8 * u for u in units]
    p.lead = [sum(p.piece[:k]) for k in COLOURS]
    p.all = sum(p.piece)
    p.half = 64 * p.all
    p.base = core * p.half
    p.peers = [p.partner] + [device_at(moved(coords, d, by), core) for d in AXES for by in (ONE, TWO, THREE)]
    p.to = lambda k, s, step: device_at(moved(coords, p.dims[k][s], -p.sign[k] * (ONE + step)), core)
    return p


def rows(at, n):
    return pl.ds(pl.multiple_of(at, 8), n)


def chunk_row(p, k, step):
    return 64 * p.lead[k] + wrap(p.pos[k][ZERO] - p.sign[k] * (ONE + step)) * (16 * p.piece[k])


def sub_row(p, k, row, step):
    return row + wrap(p.pos[k][ONE] - p.sign[k] * (ONE + step)) * (4 * p.piece[k])


def piece_row(p, k, row, step):
    return row + wrap(p.pos[k][TWO] - p.sign[k] * (ONE + step)) * p.piece[k]


def signal_peers(peers):
    barrier = pltpu.get_barrier_semaphore()
    for peer in peers:
        pl.semaphore_signal(barrier, inc=ONE, device_id=peer, device_id_type=LOGICAL)


def await_peers(peers):
    pl.semaphore_wait(pltpu.get_barrier_semaphore(), len(peers))


SCATTER_SEMS = 4 + THREE * 16 + TWO * 12 + 4 * THREE


def scatter_scratch(units):
    n = 8 * sum(units)
    vm = lambda *s: pltpu.VMEM(s + (WIDTH,), F32)
    return [vm(64 * n), vm(TWO, 4 * n), vm(THREE, RING, 4 * n), vm(THREE, 4 * n), vm(THREE, n), pltpu.SemaphoreType.DMA((SCATTER_SEMS,))]


def scatter_rounds(p, src, part, out, acc, stage, land1, land2, land3, sems):
    load_sem, swap_send, swap_recv, stage_sem, p1_send, p1_recv, p2_send, p2_recv, p3_send, p3_recv = carve(
        sems, 4, 16, 16, 16, 12, 12, THREE, THREE, THREE, THREE)
    n_sub, n_chunk = 4 * p.all, 16 * p.all
    far = p.half - p.base

    def turn_row(k, n):
        return sub_row(p, k, chunk_row(p, k, n // RING), n % RING)

    def load(t):
        for k in COLOURS:
            r, m = chunk_row(p, k, t), 16 * p.piece[k]
            copy(src.at[rows(p.base + r, m)], acc.at[rows(r, m)], load_sem(t))

    def swap(n):
        for k in COLOURS:
            r, m = turn_row(k, n), 4 * p.piece[k]
            rdma(src.at[rows(far + r, m)], part.at[rows(r, m)], swap_send(n), swap_recv(n), p.partner)

    def fetch(n):
        drain(part.at[pl.ds(ZERO, n_sub)], swap_recv(n))
        for k in COLOURS:
            m = 4 * p.piece[k]
            copy(part.at[rows(turn_row(k, n), m)], stage.at[n % TWO, pl.ds(4 * p.lead[k], m)], stage_sem(n))

    def begin():
        for t in RINGS:
            load(t)
        for n in range(6):
            swap(n)

    def turn(n):
        t, i = n // RING, n % RING
        if n == ZERO:
            fetch(n)
        if n + 6 < 16:
            swap(n + 6)
        if n + ONE < 16:
            fetch(n + ONE)
        if i == ZERO:
            drain(acc.at[pl.ds(ZERO, n_chunk)], load_sem(t))
        drain(stage.at[n % TWO], stage_sem(n))
        if t > ZERO:
            drain(land1.at[t - ONE, i], p1_recv(n - 4))
        for k in COLOURS:
            at, m = rows(turn_row(k, n), 4 * p.piece[k]), pl.ds(4 * p.lead[k], 4 * p.piece[k])
            val = acc[at] + stage[n % TWO, m]
            acc[at] = val + land1[t - ONE, i, m] if t > ZERO else val
        if t < THREE:
            for k in COLOURS:
                at, m = rows(turn_row(k, n), 4 * p.piece[k]), pl.ds(4 * p.lead[k], 4 * p.piece[k])
                rdma(acc.at[at], land1.at[t, i, m], p1_send(n), p1_recv(n), p.nxt[k][ZERO])

    def second(i):
        for k in COLOURS:
            at, m = rows(turn_row(k, 12 + i), 4 * p.piece[k]), pl.ds(4 * p.lead[k], 4 * p.piece[k])
            rdma(acc.at[at], land2.at[i, m], p2_send(i), p2_recv(i), p.to(k, ONE, i))

    def third():
        for i in AXES:
            drain(land2.at[i], p2_recv(i))
        for k in COLOURS:
            at, m = rows(turn_row(k, 15), 4 * p.piece[k]), pl.ds(4 * p.lead[k], 4 * p.piece[k])
            acc[at] += land2[ZERO, m] + land2[ONE, m] + land2[TWO, m]
        for g in AXES:
            for k in COLOURS:
                at, m = rows(piece_row(p, k, turn_row(k, 15), g), p.piece[k]), pl.ds(p.lead[k], p.piece[k])
                rdma(acc.at[at], land3.at[g, m], p3_send(g), p3_recv(g), p.to(k, TWO, g))

    def last():
        for g in AXES:
            drain(land3.at[g], p3_recv(g))
        for k in COLOURS:
            at, m = rows(piece_row(p, k, turn_row(k, 15), THREE), p.piece[k]), pl.ds(p.lead[k], p.piece[k])
            out[m] = acc[at] + (land3[ZERO, m] + land3[ONE, m] + land3[TWO, m])

    def finish():
        for n in TURNS:
            drain(acc.at[pl.ds(ZERO, n_sub)], swap_send(n))
        for n in range(12):
            drain(acc.at[pl.ds(ZERO, n_sub)], p1_send(n))
        for t in AXES:
            drain(acc.at[pl.ds(ZERO, n_sub)], p2_send(t))
            drain(acc.at[pl.ds(ZERO, p.all)], p3_send(t))

    act = functools.partial
    def both(*fs):
        def run():
            for f in fs:
                f()
        return run
    steps = [begin] + [act(turn, n) for n in range(12)]
    steps += [both(act(turn, 12 + i), act(second, i)) for i in AXES] + [act(turn, 15), third, last, finish]
    return steps


GATHER_SEMS = ONE + TWO * (THREE + THREE + 12 + 16)


def gather_rounds(p, piece, out, sems):
    own_sem, a3_send, a3_recv, a2_send, a2_recv, a1_send, a1_recv, push_send, push_recv = carve(
        sems, ONE, THREE, THREE, THREE, THREE, 12, 12, 16, 16)
    n_sub = 4 * p.all

    def many(n):
        return out.at[pl.ds(ZERO, n)]

    def mine(k, c, s, g):
        return p.base + piece_row(p, k, sub_row(p, k, chunk_row(p, k, c - ONE), s - ONE), g - ONE)

    def sub_at(k, c, s):
        return rows(p.base + sub_row(p, k, chunk_row(p, k, c - ONE), s - ONE), 4 * p.piece[k])

    def third():
        for k in COLOURS:
            src, at = piece.at[pl.ds(p.lead[k], p.piece[k])], out.at[rows(mine(k, ZERO, ZERO, ZERO), p.piece[k])]
            copy(src, at, own_sem(ZERO))
            for t in AXES:
                rdma(src, at, a3_send(t), a3_recv(t), p.to(k, TWO, t))

    def hop1(c, s):
        for k in COLOURS:
            if c < THREE:
                rdma(out.at[sub_at(k, c, s)], out.at[sub_at(k, c, s)], a1_send(RING * c + s), a1_recv(RING * c + s), p.nxt[k][ZERO])
            rdma(out.at[sub_at(k, c, s)], out.at[sub_at(k, c, s)], push_send(RING * c + s), push_recv(RING * c + s), p.partner)

    def second(s):
        if s == ZERO:
            drain(many(p.all), own_sem(ZERO))
            for t in AXES:
                drain(many(p.all), a3_recv(t))
            for t in AXES:
                for k in COLOURS:
                    rdma(out.at[sub_at(k, ZERO, ZERO)], out.at[sub_at(k, ZERO, ZERO)], a2_send(t), a2_recv(t), p.to(k, ONE, t))
        else:
            drain(many(n_sub), a2_recv(THREE - s))
        hop1(ZERO, s)

    def first(c, s):
        drain(many(n_sub), a1_recv(RING * (c - ONE) + s))
        hop1(c, s)

    def finish():
        for t in AXES:
            drain(many(p.all), a3_send(t))
            drain(many(n_sub), a2_send(t))
        for n in range(12):
            drain(many(n_sub), a1_send(n))
        for n in TURNS:
            drain(many(n_sub), push_send(n))
            drain(many(n_sub), push_recv(n))

    act = functools.partial
    return ([third] + [act(second, s) for s in RINGS]
            + [act(first, c, s) for c in (ONE, TWO, THREE) for s in RINGS] + [finish])


def small_scratch(shape):
    return [pltpu.VMEM((4, THREE) + shape, F32), pltpu.SemaphoreType.DMA((8,))]


def small_rounds(p, src, out, land, sems):
    places = [(None, p.core, TWO)] + [(d, p.coords[d], RING) for d in AXES]

    def send(n):
        d, _, size = places[n]
        for by in range(ONE, size):
            to = p.partner if d is None else device_at(moved(p.coords, d, by), p.core)
            rdma(out, land.at[n, by - ONE], sems.at[n], sems.at[4 + n], to)

    def step(n):
        if n == ZERO:
            out[ALL] = src[ALL]
        else:
            _, place, size = places[n - ONE]
            got = land.at[n - ONE, pl.ds(ZERO, size - ONE)]
            drain(got, sems.at[4 + n - ONE])
            drain(got, sems.at[n - ONE])
            mine, total = out[ALL], None
            for q in range(size):
                val = mine
                for by in range(ONE, size):
                    val = jnp.where(lax.rem(place - q + size, size) == by, land[n - ONE, by - ONE], val)
                total = val if total is None else total + val
            out[ALL] = total
        if n < 4:
            send(n)

    return [functools.partial(step, n) for n in range(5)]


def spread(steps, slots):
    plan = [[] for _ in range(slots)]
    for i, s in enumerate(steps):
        plan[i * slots // len(steps)].append(s)
    return plan


def finish_kernel(axis, units_b, units_c, pieceb_ref, c_ref, vec1_ref, vec2_ref, bq_ref, bu_ref, bc_out, small_out, part,
                  small_ref, piecec, *scratch):
    sc, (gather_sem, gather_sem2, small_land, small_sem) = scratch[:6], scratch[6:]
    pb, pc = ring_plan(axis, units_b), ring_plan(axis, units_c)
    n_b, n_c = TWO * pb.half, TWO * pc.half
    b_out, c_out = bc_out.at[pl.ds(ZERO, n_b)], bc_out.at[pl.ds(n_b, n_c)]
    signal_peers(pb.peers)
    width = small_ref.shape[ONE]
    small_ref[ALL] = jnp.zeros_like(small_ref)
    small_ref[ZERO:THREE, :] = vec1_ref[ZERO:THREE, :]
    small_ref[THREE:6, :] = vec2_ref[ZERO:THREE, :]
    at = 8
    for ref in (bq_ref, bu_ref):
        for i in range(ref.shape[ONE] // width):
            small_ref[at:at + ONE, :] = ref[:, i * width:(i + ONE) * width]
            at += ONE
    await_peers(pb.peers)
    reduce_c = scatter_rounds(pc, c_ref, part, piecec, *sc)
    gather_b = gather_rounds(pb, pieceb_ref, b_out, gather_sem)
    gather_c = gather_rounds(pc, piecec, c_out, gather_sem2)
    smalls = small_rounds(pb, small_ref, small_out, small_land, small_sem)
    main = reduce_c[:-ONE] + gather_c[:-ONE]
    fill = spread(gather_b[:-ONE], len(main) - 4)
    for i, f in enumerate(main):
        f()
        if i % THREE == ONE and i // THREE < len(smalls):
            smalls[i // THREE]()
        for f in fill[i] if i < len(fill) else ():
            f()
    for rounds in (reduce_c, gather_b, gather_c):
        rounds[-ONE]()


def finish_sum(axis, units_b, units_c, piece_b, c, vec1, vec2, bq, bu, collective_id):
    sds = jax.ShapeDtypeStruct
    dma = pltpu.SemaphoreType.DMA
    vm = pl.BlockSpec(memory_space=pltpu.VMEM)
    n = c.shape[ZERO]
    small = (16, vec1.shape[ONE])
    outs = pl.pallas_call(
        functools.partial(finish_kernel, axis, units_b, units_c),
        out_shape=(pltpu.VMEM((piece_b.shape[ZERO] * 128 + n, WIDTH), F32), sds(small, F32), sds((n // TWO, WIDTH), F32)),
        in_specs=[vm, ANY, vm, vm, vm, vm], out_specs=(vm, vm, ANY),
        scratch_shapes=[pltpu.VMEM(small, F32), pltpu.VMEM((n // 128, WIDTH), F32)] + scatter_scratch(units_c)
        + [dma((GATHER_SEMS,)), dma((GATHER_SEMS,))] + small_scratch(small),
        compiler_params=pltpu.CompilerParams(collective_id=collective_id, has_side_effects=True, vmem_limit_bytes=22 * 1024 * 1024),
        name="finish_sum",
    )(piece_b, c, vec1, vec2, bq, bu)
    return outs[:TWO]


def gather_kernel(axis, pooled_ref, g_ref, e_ref, mine, theirs, swap_sem, sems_send, sems_recv, push_send, push_recv):
    coords, core = mesh_place(axis)
    partner = device_at(coords, ONE - core)
    width = e_ref.shape[ONE]
    lanes = pl.ds(pl.multiple_of(core * (width // TWO), 128), width // TWO)
    x, y, z = coords
    peers = [partner] + [device_at(moved(coords, d, by), core) for d in AXES for by in (ONE, TWO, THREE)]
    signal_peers(peers)
    size = row_sum(pooled_ref[ALL] * pooled_ref[ALL])
    e_ref[ALL] = pooled_ref[ALL] * jnp.where(size > 0.0, lax.rsqrt(size), 0.0)
    mine[ALL] = e_ref[ALL]
    await_peers(peers)

    rdma(e_ref, theirs, swap_sem.at[ZERO], swap_sem.at[ONE], partner)
    drain(theirs, swap_sem.at[ONE])
    first = jnp.where(core == ZERO, mine[:, lanes], theirs[:, lanes])
    second = jnp.where(core == ZERO, theirs[:, lanes], mine[:, lanes])
    g_ref[z, y, x, ZERO:4, lanes] = first[ZERO:4]
    g_ref[z, y, x, 4:8, lanes] = second[ZERO:4]
    g_ref[z, y, x, 8:16, lanes] = first[8:16]
    g_ref[z, y, x, 16:24, lanes] = second[8:16]
    drain(e_ref, swap_sem.at[ZERO])

    def view(a, stage):
        idx = [z, y, x]
        for s in range(stage):
            idx[TWO - (a + s) % THREE] = slice(None)
        return g_ref.at[idx[ZERO], idx[ONE], idx[TWO], pl.ds(8 * a, 8), lanes]

    for stage in range(THREE):
        for by in (ONE, THREE, TWO):
            for a in range(THREE):
                to = device_at(moved(coords, (a + stage) % THREE, by), core)
                rdma(view(a, stage), view(a, stage), sems_send.at[stage, by - ONE], sems_recv.at[stage, by - ONE], to)
        if stage == TWO:
            for a in range(THREE):
                rdma(view(a, TWO), view(a, TWO), push_send.at[ZERO], push_recv.at[ZERO], partner)
        for by in (ONE, THREE, TWO):
            n = 4 ** stage
            shape_like = g_ref.at[ZERO, ZERO, ZERO, :, lanes] if stage == ZERO else (
                g_ref.at[ZERO, ZERO, :, :, lanes] if stage == ONE else g_ref.at[ZERO, :, :, :, lanes])
            drain(shape_like, sems_recv.at[stage, by - ONE])
            if stage == TWO:
                for a in range(THREE):
                    far = moved(coords, (a + TWO) % THREE, RING - by)
                    idx = [far[TWO], far[ONE], far[ZERO]]
                    idx[TWO - a] = slice(None)
                    idx[TWO - (a + ONE) % THREE] = slice(None)
                    v = g_ref.at[idx[ZERO], idx[ONE], idx[TWO], pl.ds(8 * a, 8), lanes]
                    rdma(v, v, push_send.at[by], push_recv.at[by], partner)
    for stage in range(THREE):
        shape_like = g_ref.at[ZERO, ZERO, ZERO, :, lanes] if stage == ZERO else (
            g_ref.at[ZERO, ZERO, :, :, lanes] if stage == ONE else g_ref.at[ZERO, :, :, :, lanes])
        for by in (ONE, TWO, THREE):
            drain(shape_like, sems_send.at[stage, by - ONE])
    for by in range(4):
        drain(g_ref.at[ZERO, :, :, :, lanes], push_send.at[by])
        drain(g_ref.at[ZERO, :, :, :, lanes], push_recv.at[by])


def gather_embeddings(e, axis, collective_id):
    dma = pltpu.SemaphoreType.DMA
    width = e.shape[ONE]
    g = pl.pallas_call(
        functools.partial(gather_kernel, axis),
        out_shape=jax.ShapeDtypeStruct((RING, RING, RING, 24, width), F32),
        in_specs=[pl.BlockSpec(memory_space=pltpu.VMEM)],
        out_specs=pl.BlockSpec(memory_space=pltpu.VMEM),
        scratch_shapes=[pltpu.VMEM(e.shape, F32)] * THREE + [dma((TWO,)),
                        dma((THREE, THREE)), dma((THREE, THREE)), dma((4,)), dma((4,))],
        compiler_params=pltpu.CompilerParams(collective_id=collective_id, has_side_effects=True,
                                             vmem_limit_bytes=16 * 1024 * 1024),
        name="gather_embeddings",
    )(e)
    return g.reshape(RING ** THREE, 24, width)


def split3(x):
    hi = x.astype(BF16)
    rest = x - hi.astype(F32)
    mid = rest.astype(BF16)
    return hi, mid, (rest - mid.astype(F32)).astype(BF16)


def dot6(a, b, dims):
    low = mm(a[TWO], b[ZERO], dims) + mm(a[ZERO], b[TWO], dims) + mm(a[ONE], b[ONE], dims)
    return mm(a[ZERO], b[ZERO], dims) + (mm(a[ZERO], b[ONE], dims) + mm(a[ONE], b[ZERO], dims) + low)


def loss_kernel(axis, n_query, g_ref, pooled_ref, loss_ref, d_ref, logit_ref, lse_ref, q_ref, p_ref, dp_ref):
    me = lax.axis_index(axis)
    core, chip = lax.rem(me, TWO), lax.div(me, TWO)
    chips, _, width = g_ref.shape
    nq = chips * 8
    lanes = 128
    gs = 100.0 / n_query
    for i, part in enumerate(split3(g_ref[:, ZERO:8, :].reshape(nq, width))):
        q_ref[i] = part
    block = TWO * lanes

    def logits(b, _):
        at = pl.multiple_of(b * block, block)
        p = split3(g_ref[pl.ds(b * (block // 16), block // 16), 8:24, :].reshape(block, width))
        for i, part in enumerate(p):
            p_ref[i, pl.ds(at, block), :] = part
        logit_ref[:, pl.ds(at, block)] = dot6((q_ref[ZERO], q_ref[ONE], q_ref[TWO]), p, NT) * 100.0
        return ZERO

    lax.fori_loop(ZERO, chips * 16 // block, logits, ZERO)

    def rows_of(b, loss):
        at = pl.ds(pl.multiple_of(b * lanes, lanes), lanes)
        s = logit_ref[at, :]
        top = jnp.max(s, axis=ONE, keepdims=True)
        lse = jnp.log(row_sum(jnp.exp(s - top))) + top
        lse_ref[at, :] = jnp.broadcast_to(lse, (lanes, lanes))
        row = lax.broadcasted_iota(jnp.int32, s.shape, ZERO) + b * lanes
        col = lax.broadcasted_iota(jnp.int32, s.shape, ONE)
        return loss + col_sum(lse - row_sum(jnp.where(col == TWO * row, s, 0.0)))

    loss = lax.fori_loop(ZERO, nq // lanes, rows_of, jnp.zeros((ONE, ONE), F32))
    loss_ref[ALL] = jnp.broadcast_to(loss * (1.0 / n_query), loss_ref.shape)

    def weights(s, lse, row, col):
        row = lax.broadcasted_iota(jnp.int32, s.shape, ZERO) + row
        col = lax.broadcasted_iota(jnp.int32, s.shape, ONE) + col
        return jnp.exp(s - lse) * gs - jnp.where(col == TWO * row, gs, 0.0)

    at = pl.ds(pl.multiple_of(chip * 8, 8), 8)
    w = jnp.concatenate([x.astype(F32) for x in split3(weights(logit_ref[at, :], lse_ref[at, ZERO:ONE], chip * 8, ZERO))], axis=ZERO).astype(BF16)
    by_hi, by_mid, by_low = (mm(w, p_ref[i]) for i in range(THREE))
    dq = by_hi[ZERO:8] + (by_hi[8:16] + by_mid[ZERO:8] + (by_hi[16:24] + by_mid[8:16] + by_low[ZERO:8]))

    first = pl.multiple_of(lax.div(chip, 8) * lanes, lanes)
    w = weights(logit_ref[:, pl.ds(first, lanes)], lse_ref[ALL], ZERO, first)
    dp_ref[ALL] = dot6(split3(w.T), (q_ref[ZERO], q_ref[ONE], q_ref[TWO]), NN)
    dp = dp_ref[pl.ds(pl.multiple_of(lax.rem(chip, 8) * 16 + core * 8, 8), 8), :]

    def back(d, pooled):
        inv = lax.rsqrt(row_sum(pooled * pooled))
        e = pooled * inv
        return (d - e * row_sum(e * d)) * inv

    d_ref[ALL] = jnp.zeros_like(d_ref)
    d_ref[ZERO:4, :] = back(jnp.where(core == ZERO, dq[ZERO:4], dq[4:8]), pooled_ref[ZERO:4])
    d_ref[8:16, :] = back(dp, pooled_ref[8:16])


def loss_and_grad(g, pooled, axis, n_query):
    chips, _, width = g.shape
    nq, n_pass, lanes = chips * 8, chips * 16, 128
    vm = pl.BlockSpec(memory_space=pltpu.VMEM)
    loss, d = pl.pallas_call(
        functools.partial(loss_kernel, axis, n_query),
        out_shape=(jax.ShapeDtypeStruct((8, lanes), F32), jax.ShapeDtypeStruct(pooled.shape, F32)),
        in_specs=[vm] * TWO, out_specs=(vm,) * TWO,
        scratch_shapes=[pltpu.VMEM((nq, n_pass), F32), pltpu.VMEM((nq, lanes), F32), pltpu.VMEM((THREE, nq, width), BF16),
                        pltpu.VMEM((THREE, n_pass, width), BF16), pltpu.VMEM((lanes, width), F32)],
        compiler_params=vmem(28), name="loss_and_grad",
    )(g, pooled)
    return loss[ZERO, ZERO], d


NN = (((ONE,), (ZERO,)), ((), ()))
NT = (((ONE,), (ONE,)), ((), ()))
TN = (((ZERO,), (ZERO,)), ((), ()))
LN_EPS = 1e-12
NEG_FILL = -1e9
TILE = 512
UNITS_A, UNITS_B, UNITS_C = (THREE, THREE, THREE, THREE, TWO, TWO), (THREE, THREE, THREE, THREE, 4, 4), (TWO,) * 6
sds = jax.ShapeDtypeStruct


def mm(a, b, dims=NN):
    return lax.dot_general(a, b, dims, preferred_element_type=F32)


def vmem(mb=60):
    return pltpu.CompilerParams(vmem_limit_bytes=mb * 1024 * 1024)


def whole(*shape):
    return pl.BlockSpec(shape, lambda j: (ZERO,) * len(shape), pipeline_mode=pl.Buffered(ONE))


def across(rows, tile):
    return pl.BlockSpec((rows, tile), lambda j: (ZERO, j))


def down(tile, cols):
    return pl.BlockSpec((tile, cols), lambda j: (j, ZERO))


def row_mean(x):
    return jnp.mean(x, axis=ONE, keepdims=True)


def row_sum(x):
    return jnp.sum(x, axis=ONE, keepdims=True)


def col_sum(x):
    return jnp.sum(x, axis=ZERO, keepdims=True)


def qkv_kernel(xq_ref, xp_ref, w_ref, b_ref, oq_ref, op_ref):
    for x_ref, o_ref in ((xq_ref, oq_ref), (xp_ref, op_ref)):
        o_ref[ALL] = (mm(x_ref[ALL], w_ref[ALL], NT) + b_ref[ALL]).astype(BF16)


def qkv_project(xq, xp, w_t, b, tile=TILE):
    tq, d = xq.shape
    tp, f = xp.shape[ZERO], w_t.shape[ZERO]
    return pl.pallas_call(
        qkv_kernel, grid=(f // tile,),
        out_shape=(sds((tq, f), BF16), sds((tp, f), BF16)),
        in_specs=[whole(tq, d), whole(tp, d), down(tile, d), across(ONE, tile)],
        out_specs=(across(tq, tile), across(tp, tile)),
        compiler_params=vmem(), name="qkv_project",
    )(xq, xp, w_t, b)


def split_heads(pair, head):
    lane = lax.broadcasted_iota(jnp.int32, pair.shape, ONE)
    zero = jnp.zeros_like(pair)
    return jnp.concatenate([jnp.where(lane < head, pair, zero), jnp.where(lane >= head, pair, zero)], axis=ZERO)


def join_heads(stacked, head):
    t = stacked.shape[ZERO] // TWO
    lane = lax.broadcasted_iota(jnp.int32, (t, stacked.shape[ONE]), ONE)
    return jnp.where(lane < head, stacked[:t], stacked[t:])


def attn_kernel(scale, head, qkv_ref, mask_ref, probs_ref, ctx_ref):
    d = ctx_ref.shape[ONE]
    pair = TWO * head
    keep = mask_ref[ZERO] > ZERO
    for g in range(d // pair):
        at = pl.ds(g * pair, pair)
        q = split_heads(qkv_ref[:, at], head)
        k = qkv_ref[:, pl.ds(d + g * pair, pair)]
        v = qkv_ref[:, pl.ds(TWO * d + g * pair, pair)]
        s = jnp.where(keep, mm(q, k, NT) * scale, NEG_FILL)
        e = jnp.exp(s - jnp.max(s, axis=ONE, keepdims=True))
        p = (e / row_sum(e)).astype(BF16)
        probs_ref[ZERO, g] = p
        ctx_ref[:, at] = join_heads(mm(p, v), head).astype(BF16)


def attention(qkv, mask, head):
    n, seq = mask.shape
    d = qkv.shape[ONE] // THREE
    pairs = d // (TWO * head)
    return pl.pallas_call(
        functools.partial(attn_kernel, head ** -0.5, head), grid=(n,),
        out_shape=(sds((n, pairs, TWO * seq, seq), BF16), sds((n * seq, d), BF16)),
        in_specs=[down(seq, THREE * d), pl.BlockSpec((ONE, ONE, seq), lambda j: (j, ZERO, ZERO))],
        out_specs=(pl.BlockSpec((ONE, pairs, TWO * seq, seq), lambda j: (j, ZERO, ZERO, ZERO)), down(seq, d)),
        compiler_params=vmem(), name="attention",
    )(qkv, mask.reshape(n, ONE, seq))


def norm_rows(x):
    c = x - row_mean(x)
    r = lax.rsqrt(row_mean(c * c) + LN_EPS)
    return c * r, r


def norm_back(g, hat, r):
    return r * (g - row_mean(g) - hat * row_mean(g * hat))


ERFC = (0.07122347, -0.27794802, 0.29668747, -0.02018065, 0.21581222, 0.21731356, 0.24887118, 0.24822095)


def gelu_parts(u):
    bell = jnp.exp2(u * u * -0.7213475204)
    t = 1.0 / (1.0 + 0.311126984 * jnp.abs(u))
    poly = 0.5 * ERFC[ZERO]
    for c in ERFC[ONE:]:
        poly = poly * t + 0.5 * c
    tail = bell * (poly * t)
    return jnp.where(u >= 0.0, 1.0 - tail, tail), u * bell * 0.3989422804


def sequences(mq_ref, mp_ref):
    lo, out = ZERO, []
    for first, ref in ((ZERO, mq_ref), (8, mp_ref)):
        n, seq = ref.shape
        for i in range(n):
            size = row_sum(ref[i:i + ONE, :].astype(F32))
            token = lax.broadcasted_iota(jnp.int32, (seq, ONE), ZERO).astype(F32)
            out.append((first + i, pl.ds(lo, seq), jnp.where(token < size, 1.0 / size, 0.0)))
            lo += seq
    return out


def row_blocks(n, size=256):
    size = min(n, size)
    return [pl.ds(a, size) for a in range(ZERO, n, size)]


ROWS = 304


def ffn_kernel(xq_ref, xp_ref, cq_ref, cp_ref, wo_ref, vec_ref, mq_ref, mp_ref, wu_ref, bu_ref, wd_ref,
               h_ref, r1q_ref, r1p_ref, g_ref, gp_ref, r2_ref, pool_ref):
    j = pl.program_id(ZERO)
    t, tq = h_ref.shape[ZERO], cq_ref.shape[ZERO]
    b_out, g1, s1, b_down, g2, s2 = (vec_ref[i:i + ONE, :] for i in range(6))

    @pl.when(j == ZERO)
    def _():
        for x_ref, c_ref, r_ref, lo in ((xq_ref, cq_ref, r1q_ref, ZERO), (xp_ref, cp_ref, r1p_ref, tq)):
            for at in row_blocks(c_ref.shape[ZERO]):
                r1 = x_ref[at, :].astype(F32) + mm(c_ref[at, :], wo_ref[ALL]) + b_out
                r_ref[at, :] = r1
                h = (norm_rows(r1)[ZERO] * g1 + s1).astype(BF16)
                to = pl.ds(lo + at.start, at.size)
                h_ref[to, :] = h
                r2_ref[to, :] = h.astype(F32) + b_down

    for a in range(ZERO, t, ROWS):
        at = pl.ds(a, ROWS)
        u = mm(h_ref[at, :], wu_ref[ALL]) + bu_ref[ALL]
        cdf, upd = gelu_parts(u)
        g = (u * cdf).astype(BF16)
        g_ref[at, :] = g
        gp_ref[at, :] = cdf + upd
        r2_ref[at, :] += mm(g, wd_ref[ALL])

    @pl.when(j == pl.num_programs(ZERO) - ONE)
    def _():
        pool_ref[ALL] = jnp.zeros_like(pool_ref)
        for row, at, weight in sequences(mq_ref, mp_ref):
            y = norm_rows(r2_ref[at, :])[ZERO] * g2 + s2
            pool_ref[row:row + ONE, :] = col_sum(y * weight)


def ffn_forward(xq, xp, ctx_q, ctx_p, w_out, vecs, mask_q, mask_p, w_up, b_up, w_down, tile=TILE):
    tq, d = xq.shape
    tp, f = xp.shape[ZERO], w_up.shape[ONE]
    t = tq + tp
    return pl.pallas_call(
        ffn_kernel, grid=(f // tile,),
        out_shape=(sds((t, d), BF16), sds((tq, d), F32), sds((tp, d), F32), sds((t, f), BF16), sds((t, f), F32),
                   sds((t, d), F32), sds((16, d), F32)),
        in_specs=[whole(tq, d), whole(tp, d), whole(tq, d), whole(tp, d), whole(d, d), whole(*vecs.shape),
                  whole(*mask_q.shape), whole(*mask_p.shape), across(d, tile), across(ONE, tile), down(tile, d)],
        out_specs=(whole(t, d), whole(tq, d), whole(tp, d), across(t, tile), across(t, tile), whole(t, d), whole(16, d)),
        compiler_params=vmem(), name="ffn_forward",
    )(xq, xp, ctx_q, ctx_p, w_out, vecs, mask_q, mask_p, w_up, b_up, w_down)


def store_blocks(ref, val):
    for c in range(ref.shape[ZERO]):
        ref[c] = val[:, c * WIDTH:(c + ONE) * WIDTH]


def down_bwd_kernel(dpool_ref, r2_ref, mq_ref, mp_ref, vec_ref, g_ref, dwd_ref, dr2_ref, dr2b_ref, dvec_ref):
    @pl.when(pl.program_id(ZERO) == ZERO)
    def _():
        dvec_ref[ALL] = jnp.zeros_like(dvec_ref)
        for row, at, weight in sequences(mq_ref, mp_ref):
            hat, r = norm_rows(r2_ref[at, :])
            dy = weight * dpool_ref[row:row + ONE, :]
            dr2 = norm_back(dy * vec_ref[4:5, :], hat, r)
            dr2_ref[at, :] = dr2
            dr2b_ref[at, :] = dr2.astype(BF16)
            dvec_ref[ZERO:ONE, :] += col_sum(dr2)
            dvec_ref[ONE:TWO, :] += col_sum(dy * hat)
            dvec_ref[TWO:THREE, :] += col_sum(dy)

    store_blocks(dwd_ref, mm(g_ref[ALL], dr2b_ref[ALL], TN))


def down_backward(dpool, r2, mask_q, mask_p, vecs, g, tile=TILE):
    t, d = r2.shape
    f = g.shape[ONE]
    n = d // WIDTH
    return pl.pallas_call(
        down_bwd_kernel, grid=(f // tile,),
        out_shape=(sds((n, f, WIDTH), F32), sds((t, d), F32), sds((t, d), BF16), sds((8, d), F32)),
        in_specs=[whole(*dpool.shape), whole(t, d), whole(*mask_q.shape), whole(*mask_p.shape), whole(*vecs.shape), across(t, tile)],
        out_specs=(pl.BlockSpec((n, tile, WIDTH), lambda j: (ZERO, j, ZERO)), whole(t, d), whole(t, d), whole(8, d)),
        compiler_params=vmem(), name="down_backward",
    )(dpool, r2, mask_q, mask_p, vecs, g)


PACE_UP = (5.5, 2.3, 14.0, 6.0)
PACE_B = (5.5, 2.8, 9.0, 5.0)
PACE_A = (8.0, 3.3, 0.0, 0.0)
def place(timed, slot_times):
    plan = [[] for _ in slot_times]
    for t, f in sorted(timed, key=lambda x: x[ZERO]):
        plan[min([i for i, at in enumerate(slot_times) if at >= t], default=-ONE)].append(f)
    return plan


def timeline(steps, start, pace, before_third, before_last):
    n = len(steps)
    times = [0.0] + [start + pace * i for i in range(n - TWO)] + [1e3]
    if before_last:
        times[-THREE] = times[-4] + before_third
        times[-TWO] = times[-THREE] + before_last
    return list(zip(times, steps))


def run_slot(plan, j, per, point):
    for s in range(len(plan) // per):
        todo = plan[s * per + point]
        if todo:
            @pl.when(j == s)
            def _():
                for f in todo:
                    f()


def host(collective_id, mb):
    return pltpu.CompilerParams(collective_id=collective_id, has_side_effects=True, vmem_limit_bytes=mb * 1024 * 1024)


def up_bwd_kernel(axis, steps, dr2_hbm, dr2b_ref, h_ref, gp_ref, wd_ref, wu_ref, r1q_ref, r1p_ref, vec_ref, cq_ref, cp_ref, a_ref,
                  dw_ref, dbu_ref, dr1q_ref, dr1p_ref, lowq_ref, lowp_ref, dvec_ref, piece_ref, part_ref, ht_ref, sem, *scratch):
    j = pl.program_id(ZERO)
    tq = dr1q_ref.shape[ZERO]
    tp = dr1p_ref.shape[ZERO]
    p = ring_plan(axis, UNITS_A)
    pace = 5.6
    timed = timeline(scatter_rounds(p, a_ref, part_ref, piece_ref, *scratch), *PACE_UP)
    points = THREE
    plan = place(timed, [pace * (s // points) + pace * (s % points) / points for s in range(points * (steps + TWO))])
    parts = ((dr1q_ref, dr2_hbm.at[pl.ds(ZERO, tq)]), (dr1p_ref, dr2_hbm.at[pl.ds(tq, tp)]))

    @pl.when(j == ZERO)
    def _():
        signal_peers(p.peers)
        for ref, src in parts:
            copy(src, ref, sem.at[ZERO])
        ht_ref[ALL] = h_ref[ALL].T
        for ref, src in parts:
            drain(ref, sem.at[ZERO])
        await_peers(p.peers)

    run_slot(plan, j, points, ZERO)

    @pl.when(j < steps)
    def _():
        dg = mm(dr2b_ref[ALL], wd_ref[ALL], NT).astype(BF16).astype(F32)
        dpre = dg * gp_ref[ALL]
        dbu_ref[ALL] = col_sum(dpre)
        dpre = dpre.astype(BF16)
        run_slot(plan, j, points, ONE)
        store_blocks(dw_ref, mm(ht_ref[ALL], dpre))
        run_slot(plan, j, points, TWO)
        dr1q_ref[ALL] += mm(dpre[:tq], wu_ref[ALL], NT)
        dr1p_ref[ALL] += mm(dpre[tq:], wu_ref[ALL], NT)

    @pl.when(j == steps)
    def _():
        dvec_ref[ALL] = jnp.zeros_like(dvec_ref)
        for d_ref, r_ref, low_ref in ((dr1q_ref, r1q_ref, lowq_ref), (dr1p_ref, r1p_ref, lowp_ref)):
            for at in row_blocks(d_ref.shape[ZERO]):
                dy = d_ref[at, :].astype(BF16).astype(F32)
                hat, r = norm_rows(r_ref[at, :])
                dr1 = norm_back(dy * vec_ref[ONE:TWO, :], hat, r)
                d_ref[at, :] = dr1
                low_ref[at, :] = dr1.astype(BF16)
                dvec_ref[ZERO:ONE, :] += col_sum(dr1)
                dvec_ref[ONE:TWO, :] += col_sum(dy * hat)
                dvec_ref[TWO:THREE, :] += col_sum(dy)

    @pl.when(j >= steps)
    def _():
        half = dr1q_ref.shape[ONE] // TWO
        at = pl.ds(pl.multiple_of(jnp.maximum(j - steps, ZERO) * half, half), half)
        run_slot(plan, j, points, ONE)
        store_blocks(dw_ref, mm(cq_ref[ALL], lowq_ref[:, at], TN) + mm(cp_ref[ALL], lowp_ref[:, at], TN))
        run_slot(plan, j, points, TWO)


def up_backward(axis, dr2, dr2b, h, gp, w_down, w_up, r1_q, r1_p, vecs, ctx_q, ctx_p, part_a, collective_id, tile=TILE):
    t, d = h.shape
    f = w_up.shape[ONE]
    tq, tp = r1_q.shape[ZERO], r1_p.shape[ZERO]
    n, total, steps = tile // WIDTH, part_a.shape[ZERO], f // tile
    cut = lambda j: jnp.minimum(j, steps - ONE)
    wide = lambda rows: pl.BlockSpec((rows, tile), lambda j: (ZERO, cut(j)))
    return pl.pallas_call(
        functools.partial(up_bwd_kernel, axis, steps), grid=(steps + TWO,),
        out_shape=(sds(((f + d) // WIDTH, d, WIDTH), F32), sds((ONE, f), F32), sds((tq, d), F32), sds((tp, d), F32),
                   sds((tq, d), BF16), sds((tp, d), BF16), sds((8, d), F32),
                   sds((total // 128, WIDTH), F32), sds((total // TWO, WIDTH), F32)),
        in_specs=[ANY, whole(t, d), whole(t, d), wide(t), pl.BlockSpec((tile, d), lambda j: (cut(j), ZERO)), wide(d),
                  whole(tq, d), whole(tp, d), whole(*vecs.shape), whole(tq, d), whole(tp, d), ANY],
        out_specs=(pl.BlockSpec((n, d, WIDTH), lambda j: (j, ZERO, ZERO)), wide(ONE), whole(tq, d), whole(tp, d), whole(tq, d), whole(tp, d),
                   whole(8, d), whole(total // 128, WIDTH), ANY),
        scratch_shapes=[pltpu.VMEM((d, t), BF16), pltpu.SemaphoreType.DMA((ONE,))] + scatter_scratch(UNITS_A),
        compiler_params=host(collective_id, 63), name="up_backward",
    )(dr2, dr2b, h, gp, w_down, w_up, r1_q, r1_p, vecs, ctx_q, ctx_p, part_a)


def attn_bwd_body(scale, head, low_ref, wo_ref, qkv_ref, probs_ref, out_ref, pause):
    d = low_ref.shape[ONE]
    pair = TWO * head
    dctx = mm(low_ref[ALL], wo_ref[ALL], NT).astype(BF16)
    for g in range(d // pair):
        if g == d // (TWO * pair):
            pause(ONE)
        at = pl.ds(g * pair, pair)
        q = split_heads(qkv_ref[:, at], head)
        k = qkv_ref[:, pl.ds(d + g * pair, pair)]
        v = qkv_ref[:, pl.ds(TWO * d + g * pair, pair)]
        p = probs_ref[ZERO, g]
        dc = split_heads(dctx[:, g * pair:(g + ONE) * pair], head)
        dp = mm(dc, v, NT)
        pf = p.astype(F32)
        ds = (pf * (dp - row_sum(dp * pf)) * scale).astype(BF16)
        out_ref[:, at] = join_heads(mm(ds, k), head).astype(BF16)
        out_ref[:, pl.ds(d + g * pair, pair)] = mm(ds, q, TN).astype(BF16)
        out_ref[:, pl.ds(TWO * d + g * pair, pair)] = mm(p, dc, TN).astype(BF16)


def attn_qkv_kernel(axis, scale, head, nq, n_pass, lowq_ref, lowp_ref, wo_ref, qkvq_ref, qkvp_ref, probq_ref, probp_ref,
                    xq_ref, xp_ref, w_ref, dr1q_hbm, dr1p_hbm, b_ref, piecea_ref,
                    dw_ref, db_ref, dhq_ref, dhp_ref, pieceb_ref, part_ref, a_ref, dq_ref, dp_ref, accq_ref, accp_ref, sem, gsem, *scratch):
    j = pl.program_id(ZERO)
    first, last = nq + n_pass, pl.num_programs(ZERO) - ONE
    tile = w_ref.shape[ZERO]
    per = dq_ref.shape[TWO] // tile
    pa, pb = ring_plan(axis, UNITS_A), ring_plan(axis, UNITS_B)
    points = TWO
    steps = [3.2] * nq + [3.3] * n_pass + [4.3] * per
    slots = [sum(steps[:i]) + steps[i] * h / points for i in range(len(steps)) for h in range(points)]
    timed = timeline(scatter_rounds(pb, b_ref, part_ref, pieceb_ref, *scratch), *PACE_B)
    timed += timeline(gather_rounds(pa, piecea_ref, a_ref, gsem), *PACE_A)
    plan = place(timed, slots)
    pause = functools.partial(run_slot, plan, j, points)
    loads = ((dr1q_hbm, accq_ref), (dr1p_hbm, accp_ref))

    @pl.when(j == ZERO)
    def _():
        signal_peers(pa.peers)
        for src, dst in loads:
            copy(src, dst, sem.at[ZERO])
        await_peers(pa.peers)
    pause(ZERO)

    @pl.when(j < nq)
    def _():
        attn_bwd_body(scale, head, lowq_ref, wo_ref, qkvq_ref, probq_ref, dq_ref.at[jnp.minimum(j, nq - ONE)], pause)

    @pl.when((j >= nq) & (j < first))
    def _():
        attn_bwd_body(scale, head, lowp_ref, wo_ref, qkvp_ref, probp_ref, dp_ref.at[jnp.clip(j - nq, ZERO, n_pass - ONE)], pause)

    @pl.when(j == first - ONE)
    def _():
        for src, dst in loads:
            drain(dst, sem.at[ZERO])

    @pl.when(j >= first)
    def _():
        at = pl.ds(pl.multiple_of(jnp.maximum(j - first, ZERO) * tile, tile), tile)
        dq = dq_ref[:, :, at].reshape(-ONE, tile)
        dp = dp_ref[:, :, at].reshape(-ONE, tile)
        store_blocks(dw_ref, mm(dq, xq_ref[ALL], TN) + mm(dp, xp_ref[ALL], TN))
        db_ref[ALL] = col_sum(dq.astype(F32)) + col_sum(dp.astype(F32))
        pause(ONE)
        accq_ref[ALL] += mm(dq, w_ref[ALL])
        accp_ref[ALL] += mm(dp, w_ref[ALL])

    @pl.when(j == last)
    def _():
        dhq_ref[ALL] = accq_ref[ALL].astype(BF16)
        dhp_ref[ALL] = accp_ref[ALL].astype(BF16)


def attn_qkv_backward(axis, low_q, low_p, w_out, qkv_q, qkv_p, probs_q, probs_p, xq, xp, w_t, dr1_q, dr1_p, part_b, piece_a, head,
                      collective_id, tile=TILE):
    f, d = w_t.shape
    nq, pairs, _, lq = probs_q.shape
    n_pass, _, _, lp = probs_p.shape
    tq, tp = nq * lq, n_pass * lp
    per, cols, total = f // tile, d // WIDTH, part_b.shape[ZERO]
    jq = lambda j: jnp.minimum(j, nq - ONE)
    jp = lambda j: jnp.clip(j - nq, ZERO, n_pass - ONE)
    jt = lambda j: jnp.clip(j - nq - n_pass, ZERO, per - ONE)
    rows_of = lambda n, c, at: pl.BlockSpec((n, c), lambda j: (at(j), ZERO))
    probs_of = lambda n, at: pl.BlockSpec((ONE, pairs, TWO * n, n), lambda j: (at(j), ZERO, ZERO, ZERO))
    return pl.pallas_call(
        functools.partial(attn_qkv_kernel, axis, head ** -0.5, head, nq, n_pass), grid=(nq + n_pass + per,),
        out_shape=(sds((cols, f, WIDTH), F32), sds((ONE, f), F32), sds((tq, d), BF16), sds((tp, d), BF16),
                   sds((total // 128, WIDTH), F32), sds((total // TWO, WIDTH), F32), sds((piece_a.shape[ZERO] * 128, WIDTH), F32)),
        in_specs=[rows_of(lq, d, jq), rows_of(lp, d, jp), whole(d, d), rows_of(lq, f, jq), rows_of(lp, f, jp),
                  probs_of(lq, jq), probs_of(lp, jp), whole(tq, d), whole(tp, d), rows_of(tile, d, jt), ANY, ANY, ANY, whole(*piece_a.shape)],
        out_specs=(pl.BlockSpec((cols, tile, WIDTH), lambda j: (ZERO, jt(j), ZERO)), pl.BlockSpec((ONE, tile), lambda j: (ZERO, jt(j))),
                   whole(tq, d), whole(tp, d), whole(total // 128, WIDTH), ANY, ANY),
        scratch_shapes=[pltpu.VMEM((nq, lq, f), BF16), pltpu.VMEM((n_pass, lp, f), BF16), pltpu.VMEM((tq, d), F32),
                        pltpu.VMEM((tp, d), F32), pltpu.SemaphoreType.DMA((ONE,)), pltpu.SemaphoreType.DMA((GATHER_SEMS,))]
        + scatter_scratch(UNITS_B),
        compiler_params=host(collective_id, 63), name="attn_qkv_backward",
    )(low_q, low_p, w_out, qkv_q, qkv_p, probs_q, probs_p, xq, xp, w_t, dr1_q, dr1_p, part_b, piece_a)


def unpack_kernel(a_hbm, bc_ref, down_ref, up_ref, out_ref, qkv_ref, stage, sems, in_sem, out_sem):
    n_up = up_ref.shape[ONE] // WIDTH
    slots, _, rows_each, _ = stage.shape

    def cols(i):
        return pl.ds(i * WIDTH, WIDTH)

    def load(i):
        copy(a_hbm.at[:, pl.ds(i * rows_each, rows_each)], stage.at[i % slots], in_sem.at[i % slots])

    total = down_ref.shape[ZERO] // rows_each
    for i in range(slots):
        load(i)
    n, m, k = up_ref.shape[ZERO], qkv_ref.shape[ZERO], n_up + out_ref.shape[ONE] // WIDTH
    for i in range(k):
        copy(bc_ref.at[pl.ds(i * n, n)], up_ref.at[:, cols(i)] if i < n_up else out_ref.at[:, cols(i - n_up)], sems.at[ZERO])
    for i in range(qkv_ref.shape[ONE] // WIDTH):
        copy(bc_ref.at[pl.ds(k * n + i * m, m)], qkv_ref.at[:, cols(i)], sems.at[ZERO])
    for i in range(total):
        slot = i % slots
        drain(stage.at[slot], in_sem.at[slot])
        for k in range(stage.shape[ONE]):
            copy(stage.at[slot, k], down_ref.at[pl.ds(i * rows_each, rows_each), cols(k)], out_sem.at[slot])
        if i >= ONE and i - ONE + slots < total:
            drain(stage.at[(i - ONE) % slots], out_sem.at[(i - ONE) % slots])
            load(i - ONE + slots)
    for i in range(max(total - slots, ZERO), total):
        drain(stage.at[i % slots], out_sem.at[i % slots])
    drain(bc_ref, sems.at[ZERO])


def unpack(a, bc, d, f):
    ff = a.shape[ONE]
    vm = pl.BlockSpec(memory_space=pltpu.VMEM)
    slots = 4
    dma = pltpu.SemaphoreType.DMA
    return pl.pallas_call(
        unpack_kernel, out_shape=(sds((ff, d), F32), sds((d, ff), F32), sds((d, d), F32), sds((f, d), F32)),
        in_specs=[ANY, vm], out_specs=(ANY,) * 4,
        scratch_shapes=[pltpu.VMEM((slots, d // WIDTH, TILE, WIDTH), F32), dma((ONE,)), dma((slots,)), dma((slots,))],
        compiler_params=vmem(12), name="unpack",
    )(a, pltpu.with_memory_space_constraint(bc, pltpu.VMEM))


def solution(mesh):
    axis = mesh.axis_names[ZERO]
    n_dev = mesh.shape[axis]

    def local_step(q_hidden, q_mask, p_hidden, p_mask, w_qkv, b_qkv, w_out, b_out, ln1_gain, ln1_shift,
                   w_up, b_up, w_down, b_down, ln2_gain, ln2_shift):
        nq, _, d = q_hidden.shape
        n_pass, p_len = nq * p_hidden.shape[ONE], p_hidden.shape[TWO]
        _, three, heads, head = w_qkv.shape
        xq, xp = q_hidden.reshape(-ONE, d), p_hidden.reshape(-ONE, d)
        p_mask = p_mask.reshape(n_pass, p_len)
        wqkv_t = w_qkv.transpose(ONE, TWO, THREE, ZERO).reshape(-ONE, d)
        wo = w_out.reshape(-ONE, d)
        none = jnp.zeros_like(b_out)
        vecs = jnp.stack([b_out, ln1_gain, ln1_shift, b_down, ln2_gain, ln2_shift, none, none])

        qkv_q, qkv_p = qkv_project(xq, xp, wqkv_t, b_qkv.reshape(ONE, -ONE))
        probs_q, ctx_q = attention(qkv_q, q_mask, head)
        probs_p, ctx_p = attention(qkv_p, p_mask, head)
        h, r1_q, r1_p, g, gp, r2, pooled = ffn_forward(
            xq, xp, ctx_q, ctx_p, wo, vecs, q_mask, p_mask, w_up, b_up.reshape(ONE, -ONE), w_down)
        everyone = gather_embeddings(pooled, axis, ONE)
        mean_loss, d_pooled = loss_and_grad(everyone, pooled, axis, nq * n_dev)
        dwd, dr2, dr2b, dvec2 = down_backward(d_pooled, r2, q_mask, p_mask, vecs, g)
        dwb, dbu, dr1_q, dr1_p, low_q, low_p, dvec1, piece_a, _ = up_backward(
            axis, dr2, dr2b, h, gp, w_down, w_up, r1_q, r1_p, vecs, ctx_q, ctx_p, dwd.reshape(-ONE, WIDTH), TWO)
        dwq, dbq, dh_q, dh_p, piece_b, _, a = attn_qkv_backward(
            axis, low_q, low_p, wo, qkv_q, qkv_p, probs_q, probs_p, xq, xp, wqkv_t, dr1_q, dr1_p, dwb.reshape(-ONE, WIDTH), piece_a, head, THREE)
        bc, small = finish_sum(axis, UNITS_B, UNITS_C, piece_b, dwq.reshape(-ONE, WIDTH), dvec1, dvec2, dbq, dbu, 4)
        d_down, d_up, d_out, d_qkv = unpack(a.reshape(dwd.shape), bc, d, three * d)
        vec = [small[i] for i in range(6)]
        return (mean_loss, dh_q.reshape(q_hidden.shape), dh_p.reshape(p_hidden.shape),
                d_qkv.reshape(three, heads, head, d).transpose(THREE, ZERO, ONE, TWO), small[8:8 + three].reshape(b_qkv.shape),
                d_out.reshape(w_out.shape), vec[ZERO], vec[ONE], vec[TWO], d_up, small[8 + three:-ONE].reshape(-ONE),
                d_down, vec[THREE], vec[4], vec[5])

    in_specs = (P(axis),) * 4 + (P(),) * 12
    out_specs = (P(), P(axis), P(axis)) + (P(),) * 12
    return jax.shard_map(local_step, mesh=mesh, in_specs=in_specs, out_specs=out_specs, check_vma=False)
```

```python
import functools
import types
import jax
import jax.numpy as jnp
from jax import lax
from jax.experimental import pallas as pl
from jax.experimental.pallas import tpu as pltpu
from jax.sharding import PartitionSpec as P

ZERO, ONE, TWO, THREE, ALL = 0, 1, 2, 3, ...

F32 = jnp.float32
BF16 = jnp.bfloat16
LOGICAL = pl.DeviceIdType.LOGICAL
RING = 4
WIDTH = 256
COLOURS = range(6)
AXES = range(THREE)
RINGS = range(RING)
TURNS = range(RING * RING)
ANY = pl.BlockSpec(memory_space=pl.ANY)


def mesh_place(axis):
    me = lax.axis_index(axis)
    core = lax.rem(me, TWO)
    chip = lax.div(me, TWO)
    row = lax.div(chip, RING)
    return (lax.rem(chip, RING), lax.rem(row, RING), lax.div(row, RING)), core


def device_at(coords, core):
    return ((coords[TWO] * RING + coords[ONE]) * RING + coords[ZERO]) * TWO + core


def moved(coords, dim, by):
    out = list(coords)
    out[dim] = lax.rem(coords[dim] + by + TWO * RING, RING)
    return tuple(out)


def wrap(i):
    return lax.rem(i + 4 * RING, RING)


def rdma(src, dst, send, recv, to):
    pltpu.make_async_remote_copy(src_ref=src, dst_ref=dst, send_sem=send, recv_sem=recv,
                                 device_id=to, device_id_type=LOGICAL).start()


def copy(src, dst, sem):
    pltpu.make_async_copy(src, dst, sem).start()


def drain(ref, sem):
    pltpu.make_async_copy(ref, ref, sem).wait()


def carve(sems, *counts):
    out, at = [], ZERO
    for n in counts:
        out.append(lambda i, at=at: sems.at[at + i])
        at += n
    return out


def ring_plan(axis, units):
    coords, core = mesh_place(axis)
    p = types.SimpleNamespace(coords=coords, core=core, partner=device_at(coords, ONE - core))
    p.dims = [tuple((k // TWO + s) % THREE for s in AXES) for k in COLOURS]
    p.sign = [ONE - TWO * (k % TWO) for k in COLOURS]
    p.pos = [tuple(coords[d] for d in p.dims[k]) for k in COLOURS]
    p.nxt = [tuple(device_at(moved(coords, d, p.sign[k]), core) for d in p.dims[k]) for k in COLOURS]
    p.piece = [8 * u for u in units]
    p.lead = [sum(p.piece[:k]) for k in COLOURS]
    p.all = sum(p.piece)
    p.half = 64 * p.all
    p.base = core * p.half
    p.peers = [p.partner] + [device_at(moved(coords, d, by), core) for d in AXES for by in (ONE, THREE)]
    p.across = [device_at(moved(coords, d, TWO), core) for d in AXES]
    p.prv = [tuple(device_at(moved(coords, d, -p.sign[k]), core) for d in p.dims[k]) for k in COLOURS]
    return p


def rows(at, n):
    return pl.ds(pl.multiple_of(at, 8), n)


def place_of(p, k, ring, back):
    return wrap(p.pos[k][ring] - p.sign[k] * back)


def chunk_row(p, k, back):
    return 64 * p.lead[k] + place_of(p, k, ZERO, back) * (16 * p.piece[k])


def sub_row(p, k, row, back):
    return row + place_of(p, k, ONE, back) * (4 * p.piece[k])


def piece_row(p, k, row, back):
    return row + place_of(p, k, TWO, back) * p.piece[k]


GIVE = (TWO, ONE, THREE, ZERO)
TAKE = (ZERO, ONE, THREE, TWO)


def signal_peers(peers):
    barrier = pltpu.get_barrier_semaphore()
    for peer in peers:
        pl.semaphore_signal(barrier, inc=ONE, device_id=peer, device_id_type=LOGICAL)


def await_peers(peers):
    pl.semaphore_wait(pltpu.get_barrier_semaphore(), len(peers))


SCATTER_SEMS = 4 + THREE * 16 + TWO * 12 + 4 * THREE


def scatter_scratch(units):
    n = 8 * sum(units)
    vm = lambda *s: pltpu.VMEM(s + (WIDTH,), F32)
    return [vm(64 * n), vm(TWO, 4 * n), vm(THREE, RING, 4 * n), vm(THREE, 4 * n), vm(THREE, n), pltpu.SemaphoreType.DMA((SCATTER_SEMS,))]


def scatter_rounds(p, src, part, out, acc, stage, land1, land2, land3, sems):
    load_sem, swap_send, swap_recv, stage_sem, p1_send, p1_recv, p2_send, p2_recv, p3_send, p3_recv = carve(
        sems, 4, 16, 16, 16, 12, 12, THREE, THREE, THREE, THREE)
    n_sub, n_chunk = 4 * p.all, 16 * p.all
    far = p.half - p.base

    def turn_row(k, n):
        return sub_row(p, k, chunk_row(p, k, n // RING + ONE), GIVE[n % RING])

    def load(t):
        for k in COLOURS:
            r, m = chunk_row(p, k, t + ONE), 16 * p.piece[k]
            copy(src.at[rows(p.base + r, m)], acc.at[rows(r, m)], load_sem(t))

    def swap(n):
        for k in COLOURS:
            r, m = turn_row(k, n), 4 * p.piece[k]
            rdma(src.at[rows(far + r, m)], part.at[rows(r, m)], swap_send(n), swap_recv(n), p.partner)

    def fetch(n):
        drain(part.at[pl.ds(ZERO, n_sub)], swap_recv(n))
        for k in COLOURS:
            m = 4 * p.piece[k]
            copy(part.at[rows(turn_row(k, n), m)], stage.at[n % TWO, pl.ds(4 * p.lead[k], m)], stage_sem(n))

    def begin():
        for t in RINGS:
            load(t)
        for n in range(6):
            swap(n)

    def turn(n):
        t, i = n // RING, n % RING
        if n == ZERO:
            fetch(n)
        if n + 6 < 16:
            swap(n + 6)
        if n + ONE < 16:
            fetch(n + ONE)
        if i == ZERO:
            drain(acc.at[pl.ds(ZERO, n_chunk)], load_sem(t))
        drain(stage.at[n % TWO], stage_sem(n))
        if t > ZERO:
            drain(land1.at[t - ONE, i], p1_recv(n - 4))
        for k in COLOURS:
            at, m = rows(turn_row(k, n), 4 * p.piece[k]), pl.ds(4 * p.lead[k], 4 * p.piece[k])
            val = acc[at] + stage[n % TWO, m]
            acc[at] = val + land1[t - ONE, i, m] if t > ZERO else val
        if t < THREE:
            for k in COLOURS:
                at, m = rows(turn_row(k, n), 4 * p.piece[k]), pl.ds(4 * p.lead[k], 4 * p.piece[k])
                rdma(acc.at[at], land1.at[t, i, m], p1_send(n), p1_recv(n), p.nxt[k][ZERO])

    def pass_on(i, where, land, send, recv, ring):
        if i == TWO:
            drain(land.at[ZERO], recv(ZERO))
        for k in COLOURS:
            at, m = where(k, i)
            if i == TWO:
                acc[at] += land[ZERO, m]
        for k in COLOURS:
            at, m = where(k, i)
            rdma(acc.at[at], land.at[i, m], send(i), recv(i), (p.prv if i == ONE else p.nxt)[k][ring])

    def sub_at(k, i):
        return rows(turn_row(k, 12 + i), 4 * p.piece[k]), pl.ds(4 * p.lead[k], 4 * p.piece[k])

    def piece_at(k, i):
        return rows(piece_row(p, k, turn_row(k, 15), GIVE[i]), p.piece[k]), pl.ds(p.lead[k], p.piece[k])

    def second(i):
        pass_on(i, sub_at, land2, p2_send, p2_recv, ONE)

    def third():
        for i in (ONE, TWO):
            drain(land2.at[i], p2_recv(i))
        for k in COLOURS:
            at, m = sub_at(k, THREE)
            acc[at] += land2[ONE, m] + land2[TWO, m]
        for i in (ZERO, ONE):
            pass_on(i, piece_at, land3, p3_send, p3_recv, TWO)

    def fourth():
        pass_on(TWO, piece_at, land3, p3_send, p3_recv, TWO)

    def last():
        for i in (ONE, TWO):
            drain(land3.at[i], p3_recv(i))
        for k in COLOURS:
            at, m = piece_at(k, THREE)
            out[m] = acc[at] + (land3[ONE, m] + land3[TWO, m])

    def finish():
        for n in TURNS:
            drain(acc.at[pl.ds(ZERO, n_sub)], swap_send(n))
        for n in range(12):
            drain(acc.at[pl.ds(ZERO, n_sub)], p1_send(n))
        for t in AXES:
            drain(acc.at[pl.ds(ZERO, n_sub)], p2_send(t))
            drain(acc.at[pl.ds(ZERO, p.all)], p3_send(t))

    act = functools.partial
    def both(*fs):
        def run():
            for f in fs:
                f()
        return run
    steps = [begin] + [act(turn, n) for n in range(12)]
    steps += [both(act(turn, 12 + i), act(second, i)) for i in AXES] + [act(turn, 15), third, fourth, last, finish]
    return steps


GATHER_SEMS = ONE + TWO * (THREE + THREE + 12 + 16)


def gather_rounds(p, piece, out, sems):
    own_sem, a3_send, a3_recv, a2_send, a2_recv, a1_send, a1_recv, push_send, push_recv = carve(
        sems, ONE, THREE, THREE, THREE, THREE, 12, 12, 16, 16)
    n_sub = 4 * p.all

    def many(n):
        return out.at[pl.ds(ZERO, n)]

    def sub_at(k, c, s):
        return rows(p.base + sub_row(p, k, chunk_row(p, k, c), TAKE[s]), 4 * p.piece[k])

    def piece_at(k, g):
        return rows(p.base + piece_row(p, k, sub_row(p, k, chunk_row(p, k, ZERO), ZERO), TAKE[g]), p.piece[k])

    def both_ways(at, send, recv, ring, srcs=out):
        for k in COLOURS:
            src = out.at[at(k)] if srcs is out else srcs.at[pl.ds(p.lead[k], p.piece[k])]
            rdma(src, out.at[at(k)], send(ZERO), recv(ZERO), p.nxt[k][ring])
            rdma(src, out.at[at(k)], send(ONE), recv(ONE), p.prv[k][ring])

    def forward(at, send, recv, ring):
        for k in COLOURS:
            rdma(out.at[at(k)], out.at[at(k)], send(TWO), recv(TWO), p.nxt[k][ring])

    def third():
        for k in COLOURS:
            copy(piece.at[pl.ds(p.lead[k], p.piece[k])], out.at[piece_at(k, ZERO)], own_sem(ZERO))
        both_ways(lambda k: piece_at(k, ZERO), a3_send, a3_recv, TWO, piece)

    def fourth():
        drain(many(p.all), a3_recv(ZERO))
        forward(lambda k: piece_at(k, ONE), a3_send, a3_recv, TWO)

    def hop1(c, s):
        for k in COLOURS:
            if c < THREE:
                rdma(out.at[sub_at(k, c, s)], out.at[sub_at(k, c, s)], a1_send(RING * c + s), a1_recv(RING * c + s), p.nxt[k][ZERO])
            rdma(out.at[sub_at(k, c, s)], out.at[sub_at(k, c, s)], push_send(RING * c + s), push_recv(RING * c + s), p.partner)

    def second(s):
        if s == ZERO:
            for sem in (own_sem(ZERO), a3_recv(ONE), a3_recv(TWO)):
                drain(many(p.all), sem)
            both_ways(lambda k: sub_at(k, ZERO, ZERO), a2_send, a2_recv, ONE)
        else:
            drain(many(n_sub), a2_recv(s - ONE))
        if s == ONE:
            forward(lambda k: sub_at(k, ZERO, ONE), a2_send, a2_recv, ONE)
        hop1(ZERO, s)

    def first(c, s):
        drain(many(n_sub), a1_recv(RING * (c - ONE) + s))
        hop1(c, s)

    def finish():
        for t in AXES:
            drain(many(p.all), a3_send(t))
            drain(many(n_sub), a2_send(t))
        for n in range(12):
            drain(many(n_sub), a1_send(n))
        for n in TURNS:
            drain(many(n_sub), push_send(n))
            drain(many(n_sub), push_recv(n))

    act = functools.partial
    return ([third, fourth] + [act(second, s) for s in RINGS]
            + [act(first, c, s) for c in (ONE, TWO, THREE) for s in RINGS] + [finish])


def small_scratch(shape):
    return [pltpu.VMEM((4, THREE) + shape, F32), pltpu.SemaphoreType.DMA((8,))]


def small_rounds(p, src, out, land, sems):
    places = [(None, p.core, TWO)] + [(d, p.coords[d], RING) for d in AXES]

    def send(n):
        d, _, size = places[n]
        for by in range(ONE, size):
            to = p.partner if d is None else device_at(moved(p.coords, d, by), p.core)
            rdma(out, land.at[n, by - ONE], sems.at[n], sems.at[4 + n], to)

    def step(n):
        if n == ZERO:
            out[ALL] = src[ALL]
        else:
            _, place, size = places[n - ONE]
            got = land.at[n - ONE, pl.ds(ZERO, size - ONE)]
            drain(got, sems.at[4 + n - ONE])
            drain(got, sems.at[n - ONE])
            mine, total = out[ALL], None
            for q in range(size):
                val = mine
                for by in range(ONE, size):
                    val = jnp.where(lax.rem(place - q + size, size) == by, land[n - ONE, by - ONE], val)
                total = val if total is None else total + val
            out[ALL] = total
        if n < 4:
            send(n)

    return [functools.partial(step, n) for n in range(5)]


def spread(steps, slots):
    plan = [[] for _ in range(slots)]
    for i, s in enumerate(steps):
        plan[i * slots // len(steps)].append(s)
    return plan


def finish_kernel(axis, units_b, units_c, pieceb_ref, c_ref, vec1_ref, vec2_ref, bq_ref, bu_ref, bc_out, small_out, part,
                  small_ref, piecec, *scratch):
    sc, (gather_sem, gather_sem2, small_land, small_sem) = scratch[:6], scratch[6:]
    pb, pc = ring_plan(axis, units_b), ring_plan(axis, units_c)
    n_b, n_c = TWO * pb.half, TWO * pc.half
    b_out, c_out = bc_out.at[pl.ds(ZERO, n_b)], bc_out.at[pl.ds(n_b, n_c)]
    peers = pb.peers + pb.across
    signal_peers(peers)
    width = small_ref.shape[ONE]
    small_ref[ALL] = jnp.zeros_like(small_ref)
    small_ref[ZERO:THREE, :] = vec1_ref[ZERO:THREE, :]
    small_ref[THREE:6, :] = vec2_ref[ZERO:THREE, :]
    at = 8
    for ref in (bq_ref, bu_ref):
        for i in range(ref.shape[ONE] // width):
            small_ref[at:at + ONE, :] = ref[:, i * width:(i + ONE) * width]
            at += ONE
    await_peers(peers)
    reduce_c = scatter_rounds(pc, c_ref, part, piecec, *sc)
    gather_b = gather_rounds(pb, pieceb_ref, b_out, gather_sem)
    gather_c = gather_rounds(pc, piecec, c_out, gather_sem2)
    smalls = small_rounds(pb, small_ref, small_out, small_land, small_sem)
    main = reduce_c[:-ONE] + gather_c[:-ONE]
    fill = spread(gather_b[:-ONE], len(main) - 4)
    for i, f in enumerate(main):
        f()
        if i % THREE == ONE and i // THREE < len(smalls):
            smalls[i // THREE]()
        for f in fill[i] if i < len(fill) else ():
            f()
    for rounds in (reduce_c, gather_b, gather_c):
        rounds[-ONE]()


def finish_sum(axis, units_b, units_c, piece_b, c, vec1, vec2, bq, bu, collective_id):
    sds = jax.ShapeDtypeStruct
    dma = pltpu.SemaphoreType.DMA
    vm = pl.BlockSpec(memory_space=pltpu.VMEM)
    n = c.shape[ZERO]
    small = (16, vec1.shape[ONE])
    outs = pl.pallas_call(
        functools.partial(finish_kernel, axis, units_b, units_c),
        out_shape=(pltpu.VMEM((piece_b.shape[ZERO] * 128 + n, WIDTH), F32), sds(small, F32), sds((n // TWO, WIDTH), F32)),
        in_specs=[vm, ANY, vm, vm, vm, vm], out_specs=(vm, vm, ANY),
        scratch_shapes=[pltpu.VMEM(small, F32), pltpu.VMEM((n // 128, WIDTH), F32)] + scatter_scratch(units_c)
        + [dma((GATHER_SEMS,)), dma((GATHER_SEMS,))] + small_scratch(small),
        compiler_params=pltpu.CompilerParams(collective_id=collective_id, has_side_effects=True, vmem_limit_bytes=22 * 1024 * 1024),
        name="finish_sum",
    )(piece_b, c, vec1, vec2, bq, bu)
    return outs[:TWO]


def gather_kernel(axis, pooled_ref, g_ref, e_ref, mine, theirs, swap_sem, sems_send, sems_recv, push_send, push_recv):
    coords, core = mesh_place(axis)
    partner = device_at(coords, ONE - core)
    width = e_ref.shape[ONE]
    lanes = pl.ds(pl.multiple_of(core * (width // TWO), 128), width // TWO)
    x, y, z = coords
    peers = [partner] + [device_at(moved(coords, d, by), core) for d in AXES for by in (ONE, TWO, THREE)]
    signal_peers(peers)
    size = row_sum(pooled_ref[ALL] * pooled_ref[ALL])
    e_ref[ALL] = pooled_ref[ALL] * jnp.where(size > 0.0, lax.rsqrt(size), 0.0)
    mine[ALL] = e_ref[ALL]
    await_peers(peers)

    rdma(e_ref, theirs, swap_sem.at[ZERO], swap_sem.at[ONE], partner)
    drain(theirs, swap_sem.at[ONE])
    first = jnp.where(core == ZERO, mine[:, lanes], theirs[:, lanes])
    second = jnp.where(core == ZERO, theirs[:, lanes], mine[:, lanes])
    g_ref[z, y, x, ZERO:4, lanes] = first[ZERO:4]
    g_ref[z, y, x, 4:8, lanes] = second[ZERO:4]
    g_ref[z, y, x, 8:16, lanes] = first[8:16]
    g_ref[z, y, x, 16:24, lanes] = second[8:16]
    drain(e_ref, swap_sem.at[ZERO])

    def view(a, stage):
        idx = [z, y, x]
        for s in range(stage):
            idx[TWO - (a + s) % THREE] = slice(None)
        return g_ref.at[idx[ZERO], idx[ONE], idx[TWO], pl.ds(8 * a, 8), lanes]

    for stage in range(THREE):
        for by in (ONE, THREE, TWO):
            for a in range(THREE):
                to = device_at(moved(coords, (a + stage) % THREE, by), core)
                rdma(view(a, stage), view(a, stage), sems_send.at[stage, by - ONE], sems_recv.at[stage, by - ONE], to)
        if stage == TWO:
            for a in range(THREE):
                rdma(view(a, TWO), view(a, TWO), push_send.at[ZERO], push_recv.at[ZERO], partner)
        for by in (ONE, THREE, TWO):
            n = 4 ** stage
            shape_like = g_ref.at[ZERO, ZERO, ZERO, :, lanes] if stage == ZERO else (
                g_ref.at[ZERO, ZERO, :, :, lanes] if stage == ONE else g_ref.at[ZERO, :, :, :, lanes])
            drain(shape_like, sems_recv.at[stage, by - ONE])
            if stage == TWO:
                for a in range(THREE):
                    far = moved(coords, (a + TWO) % THREE, RING - by)
                    idx = [far[TWO], far[ONE], far[ZERO]]
                    idx[TWO - a] = slice(None)
                    idx[TWO - (a + ONE) % THREE] = slice(None)
                    v = g_ref.at[idx[ZERO], idx[ONE], idx[TWO], pl.ds(8 * a, 8), lanes]
                    rdma(v, v, push_send.at[by], push_recv.at[by], partner)
    for stage in range(THREE):
        shape_like = g_ref.at[ZERO, ZERO, ZERO, :, lanes] if stage == ZERO else (
            g_ref.at[ZERO, ZERO, :, :, lanes] if stage == ONE else g_ref.at[ZERO, :, :, :, lanes])
        for by in (ONE, TWO, THREE):
            drain(shape_like, sems_send.at[stage, by - ONE])
    for by in range(4):
        drain(g_ref.at[ZERO, :, :, :, lanes], push_send.at[by])
        drain(g_ref.at[ZERO, :, :, :, lanes], push_recv.at[by])


def gather_embeddings(e, axis, collective_id):
    dma = pltpu.SemaphoreType.DMA
    width = e.shape[ONE]
    g = pl.pallas_call(
        functools.partial(gather_kernel, axis),
        out_shape=jax.ShapeDtypeStruct((RING, RING, RING, 24, width), F32),
        in_specs=[pl.BlockSpec(memory_space=pltpu.VMEM)],
        out_specs=pl.BlockSpec(memory_space=pltpu.VMEM),
        scratch_shapes=[pltpu.VMEM(e.shape, F32)] * THREE + [dma((TWO,)),
                        dma((THREE, THREE)), dma((THREE, THREE)), dma((4,)), dma((4,))],
        compiler_params=pltpu.CompilerParams(collective_id=collective_id, has_side_effects=True,
                                             vmem_limit_bytes=16 * 1024 * 1024),
        name="gather_embeddings",
    )(e)
    return g.reshape(RING ** THREE, 24, width)


def split3(x):
    hi = x.astype(BF16)
    rest = x - hi.astype(F32)
    mid = rest.astype(BF16)
    return hi, mid, (rest - mid.astype(F32)).astype(BF16)


def dot6(a, b, dims):
    low = mm(a[TWO], b[ZERO], dims) + mm(a[ZERO], b[TWO], dims) + mm(a[ONE], b[ONE], dims)
    return mm(a[ZERO], b[ZERO], dims) + (mm(a[ZERO], b[ONE], dims) + mm(a[ONE], b[ZERO], dims) + low)


def loss_kernel(axis, n_query, g_ref, pooled_ref, loss_ref, d_ref, logit_ref, lse_ref, q_ref, p_ref, dp_ref):
    me = lax.axis_index(axis)
    core, chip = lax.rem(me, TWO), lax.div(me, TWO)
    chips, _, width = g_ref.shape
    nq = chips * 8
    lanes = 128
    gs = 100.0 / n_query
    for i, part in enumerate(split3(g_ref[:, ZERO:8, :].reshape(nq, width))):
        q_ref[i] = part
    block = TWO * lanes

    def logits(b, _):
        at = pl.multiple_of(b * block, block)
        p = split3(g_ref[pl.ds(b * (block // 16), block // 16), 8:24, :].reshape(block, width))
        for i, part in enumerate(p):
            p_ref[i, pl.ds(at, block), :] = part
        logit_ref[:, pl.ds(at, block)] = dot6((q_ref[ZERO], q_ref[ONE], q_ref[TWO]), p, NT) * 100.0
        return ZERO

    lax.fori_loop(ZERO, chips * 16 // block, logits, ZERO)

    def rows_of(b, loss):
        at = pl.ds(pl.multiple_of(b * lanes, lanes), lanes)
        s = logit_ref[at, :]
        top = jnp.max(s, axis=ONE, keepdims=True)
        lse = jnp.log(row_sum(jnp.exp(s - top))) + top
        lse_ref[at, :] = jnp.broadcast_to(lse, (lanes, lanes))
        row = lax.broadcasted_iota(jnp.int32, s.shape, ZERO) + b * lanes
        col = lax.broadcasted_iota(jnp.int32, s.shape, ONE)
        return loss + col_sum(lse - row_sum(jnp.where(col == TWO * row, s, 0.0)))

    loss = lax.fori_loop(ZERO, nq // lanes, rows_of, jnp.zeros((ONE, ONE), F32))
    loss_ref[ALL] = jnp.broadcast_to(loss * (1.0 / n_query), loss_ref.shape)

    def weights(s, lse, row, col):
        row = lax.broadcasted_iota(jnp.int32, s.shape, ZERO) + row
        col = lax.broadcasted_iota(jnp.int32, s.shape, ONE) + col
        return jnp.exp(s - lse) * gs - jnp.where(col == TWO * row, gs, 0.0)

    at = pl.ds(pl.multiple_of(chip * 8, 8), 8)
    w = jnp.concatenate([x.astype(F32) for x in split3(weights(logit_ref[at, :], lse_ref[at, ZERO:ONE], chip * 8, ZERO))], axis=ZERO).astype(BF16)
    by_hi, by_mid, by_low = (mm(w, p_ref[i]) for i in range(THREE))
    dq = by_hi[ZERO:8] + (by_hi[8:16] + by_mid[ZERO:8] + (by_hi[16:24] + by_mid[8:16] + by_low[ZERO:8]))

    first = pl.multiple_of(lax.div(chip, 8) * lanes, lanes)
    w = weights(logit_ref[:, pl.ds(first, lanes)], lse_ref[ALL], ZERO, first)
    dp_ref[ALL] = dot6(split3(w.T), (q_ref[ZERO], q_ref[ONE], q_ref[TWO]), NN)
    dp = dp_ref[pl.ds(pl.multiple_of(lax.rem(chip, 8) * 16 + core * 8, 8), 8), :]

    def back(d, pooled):
        inv = lax.rsqrt(row_sum(pooled * pooled))
        e = pooled * inv
        return (d - e * row_sum(e * d)) * inv

    d_ref[ALL] = jnp.zeros_like(d_ref)
    d_ref[ZERO:4, :] = back(jnp.where(core == ZERO, dq[ZERO:4], dq[4:8]), pooled_ref[ZERO:4])
    d_ref[8:16, :] = back(dp, pooled_ref[8:16])


def loss_and_grad(g, pooled, axis, n_query):
    chips, _, width = g.shape
    nq, n_pass, lanes = chips * 8, chips * 16, 128
    vm = pl.BlockSpec(memory_space=pltpu.VMEM)
    loss, d = pl.pallas_call(
        functools.partial(loss_kernel, axis, n_query),
        out_shape=(jax.ShapeDtypeStruct((8, lanes), F32), jax.ShapeDtypeStruct(pooled.shape, F32)),
        in_specs=[vm] * TWO, out_specs=(vm,) * TWO,
        scratch_shapes=[pltpu.VMEM((nq, n_pass), F32), pltpu.VMEM((nq, lanes), F32), pltpu.VMEM((THREE, nq, width), BF16),
                        pltpu.VMEM((THREE, n_pass, width), BF16), pltpu.VMEM((lanes, width), F32)],
        compiler_params=vmem(28), name="loss_and_grad",
    )(g, pooled)
    return loss[ZERO, ZERO], d


NN = (((ONE,), (ZERO,)), ((), ()))
NT = (((ONE,), (ONE,)), ((), ()))
TN = (((ZERO,), (ZERO,)), ((), ()))
LN_EPS = 1e-12
NEG_FILL = -1e9
TILE = 512
UNITS_A, UNITS_B, UNITS_C = (THREE, THREE, THREE, THREE, TWO, TWO), (THREE, THREE, THREE, THREE, 4, 4), (TWO,) * 6
sds = jax.ShapeDtypeStruct


def mm(a, b, dims=NN):
    return lax.dot_general(a, b, dims, preferred_element_type=F32)


def vmem(mb=60):
    return pltpu.CompilerParams(vmem_limit_bytes=mb * 1024 * 1024)


def whole(*shape):
    return pl.BlockSpec(shape, lambda j: (ZERO,) * len(shape), pipeline_mode=pl.Buffered(ONE))


def across(rows, tile):
    return pl.BlockSpec((rows, tile), lambda j: (ZERO, j))


def down(tile, cols):
    return pl.BlockSpec((tile, cols), lambda j: (j, ZERO))


def row_mean(x):
    return jnp.mean(x, axis=ONE, keepdims=True)


def row_sum(x):
    return jnp.sum(x, axis=ONE, keepdims=True)


def col_sum(x):
    return jnp.sum(x, axis=ZERO, keepdims=True)


def qkv_kernel(xq_ref, xp_ref, w_ref, b_ref, oq_ref, op_ref, x_ref):
    tq = xq_ref.shape[ZERO]

    @pl.when(pl.program_id(ZERO) == ZERO)
    def _():
        x_ref[:tq, :] = xq_ref[ALL]
        x_ref[tq:, :] = xp_ref[ALL]
    y = (mm(x_ref[ALL], w_ref[ALL], NT) + b_ref[ALL]).astype(BF16)
    oq_ref[ALL] = y[:tq]
    op_ref[ALL] = y[tq:]


def qkv_project(xq, xp, w_t, b, tile=TILE):
    tq, d = xq.shape
    tp, f = xp.shape[ZERO], w_t.shape[ZERO]
    return pl.pallas_call(
        qkv_kernel, grid=(f // tile,),
        out_shape=(sds((tq, f), BF16), sds((tp, f), BF16)),
        in_specs=[whole(tq, d), whole(tp, d), down(tile, d), across(ONE, tile)],
        out_specs=(across(tq, tile), across(tp, tile)),
        scratch_shapes=[pltpu.VMEM((tq + tp, d), BF16)],
        compiler_params=vmem(), name="qkv_project",
    )(xq, xp, w_t, b)


def split_heads(pair, head):
    lane = lax.broadcasted_iota(jnp.int32, pair.shape, ONE)
    zero = jnp.zeros_like(pair)
    return jnp.concatenate([jnp.where(lane < head, pair, zero), jnp.where(lane >= head, pair, zero)], axis=ZERO)


def join_heads(stacked, head):
    t = stacked.shape[ZERO] // TWO
    lane = lax.broadcasted_iota(jnp.int32, (t, stacked.shape[ONE]), ONE)
    return jnp.where(lane < head, stacked[:t], stacked[t:])


def attn_kernel(scale, head, qkv_ref, mask_ref, probs_ref, ctx_ref):
    d = ctx_ref.shape[ONE]
    pair = TWO * head
    keep = mask_ref[ZERO] > ZERO
    for g in range(d // pair):
        at = pl.ds(g * pair, pair)
        q = split_heads(qkv_ref[:, at], head)
        k = qkv_ref[:, pl.ds(d + g * pair, pair)]
        v = qkv_ref[:, pl.ds(TWO * d + g * pair, pair)]
        s = jnp.where(keep, mm(q, k, NT) * scale, NEG_FILL)
        e = jnp.exp(s - jnp.max(s, axis=ONE, keepdims=True))
        p = (e / row_sum(e)).astype(BF16)
        probs_ref[ZERO, g] = p
        ctx_ref[:, at] = join_heads(mm(p, v), head).astype(BF16)


def attention(qkv, mask, head):
    n, seq = mask.shape
    d = qkv.shape[ONE] // THREE
    pairs = d // (TWO * head)
    return pl.pallas_call(
        functools.partial(attn_kernel, head ** -0.5, head), grid=(n,),
        out_shape=(sds((n, pairs, TWO * seq, seq), BF16), sds((n * seq, d), BF16)),
        in_specs=[down(seq, THREE * d), pl.BlockSpec((ONE, ONE, seq), lambda j: (j, ZERO, ZERO))],
        out_specs=(pl.BlockSpec((ONE, pairs, TWO * seq, seq), lambda j: (j, ZERO, ZERO, ZERO)), down(seq, d)),
        compiler_params=vmem(), name="attention",
    )(qkv, mask.reshape(n, ONE, seq))


def norm_rows(x):
    c = x - row_mean(x)
    r = lax.rsqrt(row_mean(c * c) + LN_EPS)
    return c * r, r


def norm_back(g, hat, r):
    return r * (g - row_mean(g) - hat * row_mean(g * hat))


ERFC = (0.07122347, -0.27794802, 0.29668747, -0.02018065, 0.21581222, 0.21731356, 0.24887118, 0.24822095)


def gelu_parts(u):
    bell = jnp.exp2(u * u * -0.7213475204)
    t = 1.0 / (1.0 + 0.311126984 * jnp.abs(u))
    poly = 0.5 * ERFC[ZERO]
    for c in ERFC[ONE:]:
        poly = poly * t + 0.5 * c
    tail = bell * (poly * t)
    return jnp.where(u >= 0.0, 1.0 - tail, tail), u * bell * 0.3989422804


def each_sequence(mq_ref, mp_ref, act):
    for first, lo, ref in ((ZERO, ZERO, mq_ref), (8, mq_ref.shape[ZERO] * mq_ref.shape[ONE], mp_ref)):
        n, seq = ref.shape

        def one(i, _):
            size = row_sum(ref[pl.ds(i, ONE), :].astype(F32))
            token = lax.broadcasted_iota(jnp.int32, (seq, ONE), ZERO).astype(F32)
            act(first + i, pl.ds(pl.multiple_of(lo + i * seq, 16), seq), jnp.where(token < size, 1.0 / size, 0.0))
            return ZERO
        lax.fori_loop(ZERO, n, one, ZERO)


def each_block(lo, hi, act, size=304):
    def one(i, _):
        act(pl.ds(pl.multiple_of(lo + i * size, 16), size))
        return ZERO
    lax.fori_loop(ZERO, (hi - lo) // size, one, ZERO)


def ffn_kernel(xq_ref, xp_ref, cq_ref, cp_ref, wo_ref, bo_ref, g1_ref, s1_ref, bd_ref, g2_ref, s2_ref, mq_ref, mp_ref,
               wu_ref, bu_ref, wd_ref, h_hbm, r1_hbm, g_ref, gp_ref, r2_hbm, pool_ref, h_ref, r1_ref, r2_ref, sems):
    j = pl.program_id(ZERO)
    t, tq = h_ref.shape[ZERO], cq_ref.shape[ZERO]
    saved = ((h_ref, h_hbm), (r1_ref, r1_hbm), (r2_ref, r2_hbm))

    @pl.when(j == ZERO)
    def _():
        for x_ref, c_ref, lo, size in ((xq_ref, cq_ref, ZERO, tq), (xp_ref, cp_ref, tq, 256)):
            def block(at):
                to = pl.ds(pl.multiple_of(lo + at.start, 16), size)
                r1 = x_ref[at, :].astype(F32) + mm(c_ref[at, :], wo_ref[ALL]) + bo_ref[ALL]
                r1_ref[to, :] = r1
                h = (norm_rows(r1)[ZERO] * g1_ref[ALL] + s1_ref[ALL]).astype(BF16)
                h_ref[to, :] = h
                r2_ref[to, :] = h.astype(F32) + bd_ref[ALL]
            each_block(ZERO, c_ref.shape[ZERO], block, size)
        for i in range(TWO):
            copy(*saved[i], sems.at[i])

    def block(at):
        u = mm(h_ref[at, :], wu_ref[ALL]) + bu_ref[ALL]
        cdf, upd = gelu_parts(u)
        g = (u * cdf).astype(BF16)
        g_ref[at, :] = g
        gp_ref[at, :] = cdf + upd
        r2_ref[at, :] += mm(g, wd_ref[ALL])
    each_block(ZERO, t, block, 608)

    @pl.when(j == pl.num_programs(ZERO) - ONE)
    def _():
        copy(*saved[TWO], sems.at[TWO])
        pool_ref[ALL] = jnp.zeros_like(pool_ref)

        def pool(row, at, weight):
            y = norm_rows(r2_ref[at, :])[ZERO] * g2_ref[ALL] + s2_ref[ALL]
            pool_ref[pl.ds(row, ONE), :] = col_sum(y * weight)
        each_sequence(mq_ref, mp_ref, pool)
        for i in range(THREE):
            drain(saved[i][ZERO], sems.at[i])


def ffn_forward(xq, xp, ctx_q, ctx_p, w_out, vecs, mask_q, mask_p, w_up, b_up, w_down, tile=TILE):
    tq, d = xq.shape
    tp, f = xp.shape[ZERO], w_up.shape[ONE]
    t = tq + tp
    return pl.pallas_call(
        ffn_kernel, grid=(f // tile,),
        out_shape=(sds((t, d), BF16), sds((t, d), F32), sds((t, f), BF16), sds((t, f), F32), sds((t, d), F32), sds((16, d), F32)),
        in_specs=[whole(tq, d), whole(tp, d), whole(tq, d), whole(tp, d), whole(d, d), *(whole(ONE, d) for _ in vecs),
                  whole(*mask_q.shape), whole(*mask_p.shape), across(d, tile), across(ONE, tile), down(tile, d)],
        out_specs=(ANY, ANY, across(t, tile), across(t, tile), ANY, whole(16, d)),
        scratch_shapes=[pltpu.VMEM((t, d), BF16), pltpu.VMEM((t, d), F32), pltpu.VMEM((t, d), F32), pltpu.SemaphoreType.DMA((THREE,))],
        compiler_params=vmem(), name="ffn_forward",
    )(xq, xp, ctx_q, ctx_p, w_out, *vecs, mask_q, mask_p, w_up, b_up, w_down)


def store_blocks(ref, val):
    for c in range(ref.shape[ZERO]):
        ref[c] = val[:, c * WIDTH:(c + ONE) * WIDTH]


def down_bwd_kernel(dpool_ref, r2_ref, mq_ref, mp_ref, g2_ref, g_ref, dwd_ref, dr2_hbm, dr2b_hbm, dvec_ref, dr2_ref, dr2b_ref, sems):
    j = pl.program_id(ZERO)
    saved = ((dr2_ref, dr2_hbm), (dr2b_ref, dr2b_hbm))

    @pl.when(j == ZERO)
    def _():
        dvec_ref[ALL] = jnp.zeros_like(dvec_ref)

        def one(row, at, weight):
            hat, r = norm_rows(r2_ref[at, :])
            dy = weight * dpool_ref[pl.ds(row, ONE), :]
            dr2 = norm_back(dy * g2_ref[ALL], hat, r)
            dr2_ref[at, :] = dr2
            dr2b_ref[at, :] = dr2.astype(BF16)
            dvec_ref[ZERO:ONE, :] += col_sum(dr2)
            dvec_ref[ONE:TWO, :] += col_sum(dy * hat)
            dvec_ref[TWO:THREE, :] += col_sum(dy)
        each_sequence(mq_ref, mp_ref, one)
        for i in range(TWO):
            copy(*saved[i], sems.at[i])

    store_blocks(dwd_ref, mm(g_ref[ALL], dr2b_ref[ALL], TN))

    @pl.when(j == pl.num_programs(ZERO) - ONE)
    def _():
        for i in range(TWO):
            drain(saved[i][ZERO], sems.at[i])


def down_backward(dpool, r2, mask_q, mask_p, gain, g, tile=TILE):
    t, d = r2.shape
    f = g.shape[ONE]
    n = d // WIDTH
    return pl.pallas_call(
        down_bwd_kernel, grid=(f // tile,),
        out_shape=(sds((n, f, WIDTH), F32), sds((t, d), F32), sds((t, d), BF16), sds((8, d), F32)),
        in_specs=[whole(*dpool.shape), whole(t, d), whole(*mask_q.shape), whole(*mask_p.shape), whole(ONE, d), across(t, tile)],
        out_specs=(pl.BlockSpec((n, tile, WIDTH), lambda j: (ZERO, j, ZERO)), ANY, ANY, whole(8, d)),
        scratch_shapes=[pltpu.VMEM((t, d), F32), pltpu.VMEM((t, d), BF16), pltpu.SemaphoreType.DMA((TWO,))],
        compiler_params=vmem(), name="down_backward",
    )(dpool, r2, mask_q, mask_p, gain, g)


PACE_UP = (3.0, 2.5, 6.0, 4.0)
PACE_B = (4.5, 2.6, 6.5, 4.5)
PACE_A = (12.0, 3.0, 0.0, 0.0)
def place(timed, slot_times):
    plan = [[] for _ in slot_times]
    for t, f in sorted(timed, key=lambda x: x[ZERO]):
        plan[min([i for i, at in enumerate(slot_times) if at >= t], default=-ONE)].append(f)
    return plan


def timeline(steps, start, pace, before_third, before_last):
    n = len(steps)
    times = [0.0] + [start + pace * i for i in range(n - TWO)] + [1e3]
    if before_last:
        times[-4] = times[-5] + before_third
        times[-THREE] = times[-4] + before_last
        times[-TWO] = times[-THREE] + before_last
    return list(zip(times, steps))


def run_slot(plan, j, per, steps, point):
    for s in range(*steps):
        todo = plan[s * per + point]
        if todo:
            @pl.when(j == s)
            def _():
                for f in todo:
                    f()


def host(collective_id, mb):
    return pltpu.CompilerParams(collective_id=collective_id, has_side_effects=True, vmem_limit_bytes=mb * 1024 * 1024)


def up_bwd_kernel(axis, steps, dr2_hbm, dr2b_ref, h_ref, gp_ref, wd_ref, wu_ref, r1_hbm, g1_ref, cq_hbm, cp_hbm, a_ref,
                  dw_ref, dbu_ref, dr1q_hbm, dr1p_hbm, lowq_hbm, lowp_hbm, dvec_ref, piece_ref, part_ref,
                  dr1_ref, low_ref, r1_ref, ctx_ref, ht_ref, in_sem, out_sem, *scratch):
    j = pl.program_id(ZERO)
    t, tq, tp = dr1_ref.shape[ZERO], dr1q_hbm.shape[ZERO], dr1p_hbm.shape[ZERO]
    p = ring_plan(axis, UNITS_A)
    pace = 5.6
    timed = timeline(scatter_rounds(p, a_ref, part_ref, piece_ref, *scratch), *PACE_UP)
    points = THREE
    plan = place(timed, [pace * (s // points) + pace * (s % points) / points for s in range(points * (steps + TWO))])
    pause = functools.partial(run_slot, plan, j, points)
    q_rows, p_rows = pl.ds(ZERO, tq), pl.ds(tq, tp)
    late = ((r1_hbm, r1_ref), (cq_hbm, ctx_ref.at[q_rows]), (cp_hbm, ctx_ref.at[p_rows]))
    results = ((dr1_ref.at[q_rows], dr1q_hbm), (dr1_ref.at[p_rows], dr1p_hbm), (low_ref.at[q_rows], lowq_hbm), (low_ref.at[p_rows], lowp_hbm))

    @pl.when(j == ZERO)
    def _():
        signal_peers(p.peers)
        copy(dr2_hbm, dr1_ref, in_sem.at[ZERO])
        ht_ref[ALL] = h_ref[ALL].T
        drain(dr1_ref, in_sem.at[ZERO])
        for i in range(THREE):
            copy(*late[i], in_sem.at[ONE + i])

    @pl.when(j < steps)
    def _():
        dg = mm(dr2b_ref[ALL], wd_ref[ALL], NT).astype(BF16).astype(F32)
        dpre = dg * gp_ref[ALL]
        dbu_ref[ALL] = col_sum(dpre)
        dpre = dpre.astype(BF16)

        @pl.when(j == ZERO)
        def _():
            await_peers(p.peers)
        pause((ZERO, steps), ZERO)
        store_blocks(dw_ref, mm(ht_ref[ALL], dpre))
        pause((ZERO, steps), ONE)
        dr1_ref[ALL] += mm(dpre, wu_ref[ALL], NT)
        pause((ZERO, steps), TWO)

    def norm_backward(at):
        dy = dr1_ref[at, :].astype(BF16).astype(F32)
        hat, r = norm_rows(r1_ref[at, :])
        dr1 = norm_back(dy * g1_ref[ALL], hat, r)
        dr1_ref[at, :] = dr1
        low_ref[at, :] = dr1.astype(BF16)
        dvec_ref[ZERO:ONE, :] += col_sum(dr1)
        dvec_ref[ONE:TWO, :] += col_sum(dy * hat)
        dvec_ref[TWO:THREE, :] += col_sum(dy)

    @pl.when(j == steps)
    def _():
        dvec_ref[ALL] = jnp.zeros_like(dvec_ref)
        for i in range(THREE):
            drain(late[i][ONE], in_sem.at[ONE + i])
        each_block(ZERO, t, norm_backward)
        pause((steps, steps + ONE), ZERO)
        for i in range(4):
            copy(*results[i], out_sem.at[i])

    @pl.when(j >= steps)
    def _():
        half = dr1_ref.shape[ONE] // TWO
        at = pl.ds(pl.multiple_of(jnp.maximum(j - steps, ZERO) * half, half), half)
        pause((steps + ONE, steps + TWO), ZERO)
        pause((steps, steps + TWO), ONE)
        store_blocks(dw_ref, mm(ctx_ref[ALL], low_ref[:, at], TN))
        pause((steps, steps + TWO), TWO)

    @pl.when(j == steps + ONE)
    def _():
        for i in range(4):
            drain(results[i][ZERO], out_sem.at[i])


def up_backward(axis, dr2, dr2b, h, gp, w_down, w_up, r1, gain, ctx_q, ctx_p, part_a, collective_id, tile=TILE):
    t, d = h.shape
    f = w_up.shape[ONE]
    tq, tp = ctx_q.shape[ZERO], ctx_p.shape[ZERO]
    n, total, steps = tile // WIDTH, part_a.shape[ZERO], f // tile
    cut = lambda j: jnp.minimum(j, steps - ONE)
    wide = lambda rows: pl.BlockSpec((rows, tile), lambda j: (ZERO, cut(j)))
    dma, vm = pltpu.SemaphoreType.DMA, pltpu.VMEM
    return pl.pallas_call(
        functools.partial(up_bwd_kernel, axis, steps), grid=(steps + TWO,),
        out_shape=(sds(((f + d) // WIDTH, d, WIDTH), F32), sds((ONE, f), F32), sds((tq, d), F32), sds((tp, d), F32),
                   sds((tq, d), BF16), sds((tp, d), BF16), sds((8, d), F32),
                   sds((total // 128, WIDTH), F32), sds((total // TWO, WIDTH), F32)),
        in_specs=[ANY, whole(t, d), whole(t, d), wide(t), pl.BlockSpec((tile, d), lambda j: (cut(j), ZERO)), wide(d),
                  ANY, whole(ONE, d), ANY, ANY, ANY],
        out_specs=(pl.BlockSpec((n, d, WIDTH), lambda j: (j, ZERO, ZERO)), wide(ONE), ANY, ANY, ANY, ANY,
                   whole(8, d), whole(total // 128, WIDTH), ANY),
        scratch_shapes=[vm((t, d), F32), vm((t, d), BF16), vm((t, d), F32), vm((t, d), BF16), vm((d, t), BF16), dma((4,)), dma((4,))]
        + scatter_scratch(UNITS_A),
        compiler_params=host(collective_id, 63), name="up_backward",
    )(dr2, dr2b, h, gp, w_down, w_up, r1, gain, ctx_q, ctx_p, part_a)


def attn_bwd_body(scale, head, group, low_ref, wo_ref, qkv_ref, probs_ref, out_ref, dctx_ref, pause, enter=lambda: None):
    rows_here, d = low_ref.shape
    pair = TWO * head
    dctx_ref[:rows_here, :] = mm(low_ref[ALL], wo_ref[ALL], NT).astype(BF16)
    enter()
    pause(ZERO)

    def one(g):
        at, k_at, v_at = (pl.ds(pl.multiple_of(part * d + g * pair, pair), pair) for part in range(THREE))
        q = split_heads(qkv_ref[:, at], head)
        k = qkv_ref[:, k_at]
        v = qkv_ref[:, v_at]
        p = probs_ref[ZERO, g]
        dc = split_heads(dctx_ref[:rows_here, at], head)
        dp = mm(dc, v, NT)
        pf = p.astype(F32)
        ds = (pf * (dp - row_sum(dp * pf)) * scale).astype(BF16)
        out_ref[:, at] = join_heads(mm(ds, k), head).astype(BF16)
        out_ref[:, k_at] = mm(ds, q, TN).astype(BF16)
        out_ref[:, v_at] = mm(p, dc, TN).astype(BF16)

    def some(i, _):
        for h in range(group):
            one(i * group + h)
        return ZERO
    lax.fori_loop(ZERO, d // (pair * group), some, ZERO)
    pause(ONE)


def attn_qkv_kernel(axis, scale, head, nq, n_pass, lowq_ref, lowp_ref, wo_ref, qkvq_ref, qkvp_ref, probq_ref, probp_ref,
                    xq_ref, xp_ref, w_ref, dr1q_hbm, dr1p_hbm, b_ref, piecea_ref,
                    dw_ref, db_ref, dhq_ref, dhp_ref, pieceb_ref, part_ref, a_ref, dq_ref, dp_ref, accq_ref, accp_ref, dctx_ref, sem, gsem, *scratch):
    j = pl.program_id(ZERO)
    tile = w_ref.shape[ZERO]
    per = dq_ref.shape[TWO] // tile
    first, last = nq + n_pass, nq + n_pass + per - ONE
    pa, pb = ring_plan(axis, UNITS_A), ring_plan(axis, UNITS_B)
    points = TWO
    steps = [3.2] * nq + [3.3] * n_pass + [4.3] * per
    slots = [sum(steps[:i]) + steps[i] * h / points for i in range(len(steps)) for h in range(points)]
    timed = timeline(scatter_rounds(pb, b_ref, part_ref, pieceb_ref, *scratch), *PACE_B)
    timed += timeline(gather_rounds(pa, piecea_ref, a_ref, gsem), *PACE_A)
    plan = place(timed, slots)
    pause = functools.partial(run_slot, plan, j, points)
    loads = ((dr1q_hbm, accq_ref), (dr1p_hbm, accp_ref))

    @pl.when(j == ZERO)
    def _():
        signal_peers(pa.peers)
        for src, dst in loads:
            copy(src, dst, sem.at[ZERO])

    def enter():
        @pl.when(j == ZERO)
        def _():
            await_peers(pa.peers)

    @pl.when(j < nq)
    def _():
        attn_bwd_body(scale, head, 4, lowq_ref, wo_ref, qkvq_ref, probq_ref, dq_ref.at[jnp.minimum(j, nq - ONE)], dctx_ref,
                      functools.partial(pause, (ZERO, nq)), enter)

    @pl.when((j >= nq) & (j < first))
    def _():
        attn_bwd_body(scale, head, 4, lowp_ref, wo_ref, qkvp_ref, probp_ref, dp_ref.at[jnp.clip(j - nq, ZERO, n_pass - ONE)], dctx_ref,
                      functools.partial(pause, (nq, first)))

    @pl.when(j == first - ONE)
    def _():
        for src, dst in loads:
            drain(dst, sem.at[ZERO])

    @pl.when(j >= first)
    def _():
        pause((first, last + ONE), ZERO)
        at = pl.ds(pl.multiple_of(jnp.maximum(j - first, ZERO) * tile, tile), tile)
        dq = dq_ref[:, :, at].reshape(-ONE, tile)
        dp = dp_ref[:, :, at].reshape(-ONE, tile)
        store_blocks(dw_ref, mm(dq, xq_ref[ALL], TN) + mm(dp, xp_ref[ALL], TN))
        db_ref[ALL] = col_sum(dq.astype(F32)) + col_sum(dp.astype(F32))
        pause((first, last + ONE), ONE)
        accq_ref[ALL] += mm(dq, w_ref[ALL])
        accp_ref[ALL] += mm(dp, w_ref[ALL])

    @pl.when(j == last)
    def _():
        dhq_ref[ALL] = accq_ref[ALL].astype(BF16)
        dhp_ref[ALL] = accp_ref[ALL].astype(BF16)


def attn_qkv_backward(axis, low_q, low_p, w_out, qkv_q, qkv_p, probs_q, probs_p, xq, xp, w_t, dr1_q, dr1_p, part_b, piece_a, head,
                      collective_id, tile=TILE):
    f, d = w_t.shape
    nq, pairs, _, lq = probs_q.shape
    n_pass, _, _, lp = probs_p.shape
    tq, tp = nq * lq, n_pass * lp
    per, cols, total = f // tile, d // WIDTH, part_b.shape[ZERO]
    jq = lambda j: jnp.minimum(j, nq - ONE)
    jp = lambda j: jnp.clip(j - nq, ZERO, n_pass - ONE)
    jt = lambda j: jnp.clip(j - nq - n_pass, ZERO, per - ONE)
    rows_of = lambda n, c, at: pl.BlockSpec((n, c), lambda j: (at(j), ZERO))
    probs_of = lambda n, at: pl.BlockSpec((ONE, pairs, TWO * n, n), lambda j: (at(j), ZERO, ZERO, ZERO))
    return pl.pallas_call(
        functools.partial(attn_qkv_kernel, axis, head ** -0.5, head, nq, n_pass), grid=(nq + n_pass + per,),
        out_shape=(sds((cols, f, WIDTH), F32), sds((ONE, f), F32), sds((tq, d), BF16), sds((tp, d), BF16),
                   sds((total // 128, WIDTH), F32), sds((total // TWO, WIDTH), F32), sds((piece_a.shape[ZERO] * 128, WIDTH), F32)),
        in_specs=[rows_of(lq, d, jq), rows_of(lp, d, jp), whole(d, d), rows_of(lq, f, jq), rows_of(lp, f, jp),
                  probs_of(lq, jq), probs_of(lp, jp), whole(tq, d), whole(tp, d), rows_of(tile, d, jt), ANY, ANY, ANY, whole(*piece_a.shape)],
        out_specs=(pl.BlockSpec((cols, tile, WIDTH), lambda j: (ZERO, jt(j), ZERO)), pl.BlockSpec((ONE, tile), lambda j: (ZERO, jt(j))),
                   whole(tq, d), whole(tp, d), whole(total // 128, WIDTH), ANY, ANY),
        scratch_shapes=[pltpu.VMEM((nq, lq, f), BF16), pltpu.VMEM((n_pass, lp, f), BF16), pltpu.VMEM((tq, d), F32),
                        pltpu.VMEM((tp, d), F32), pltpu.VMEM((lp, d), BF16), pltpu.SemaphoreType.DMA((ONE,)),
                        pltpu.SemaphoreType.DMA((GATHER_SEMS,))]
        + scatter_scratch(UNITS_B),
        compiler_params=host(collective_id, 63), name="attn_qkv_backward",
    )(low_q, low_p, w_out, qkv_q, qkv_p, probs_q, probs_p, xq, xp, w_t, dr1_q, dr1_p, part_b, piece_a)


def unpack_kernel(a_hbm, bc_ref, down_ref, up_ref, out_ref, qkv_ref, stage, sems, in_sem, out_sem):
    n_up = up_ref.shape[ONE] // WIDTH
    slots, _, rows_each, _ = stage.shape

    def cols(i):
        return pl.ds(i * WIDTH, WIDTH)

    def load(i):
        copy(a_hbm.at[:, pl.ds(i * rows_each, rows_each)], stage.at[i % slots], in_sem.at[i % slots])

    total = down_ref.shape[ZERO] // rows_each
    for i in range(slots):
        load(i)
    n, m, k = up_ref.shape[ZERO], qkv_ref.shape[ZERO], n_up + out_ref.shape[ONE] // WIDTH
    for i in range(k):
        copy(bc_ref.at[pl.ds(i * n, n)], up_ref.at[:, cols(i)] if i < n_up else out_ref.at[:, cols(i - n_up)], sems.at[ZERO])
    for i in range(qkv_ref.shape[ONE] // WIDTH):
        copy(bc_ref.at[pl.ds(k * n + i * m, m)], qkv_ref.at[:, cols(i)], sems.at[ZERO])
    for i in range(total):
        slot = i % slots
        drain(stage.at[slot], in_sem.at[slot])
        for k in range(stage.shape[ONE]):
            copy(stage.at[slot, k], down_ref.at[pl.ds(i * rows_each, rows_each), cols(k)], out_sem.at[slot])
        if i >= ONE and i - ONE + slots < total:
            drain(stage.at[(i - ONE) % slots], out_sem.at[(i - ONE) % slots])
            load(i - ONE + slots)
    for i in range(max(total - slots, ZERO), total):
        drain(stage.at[i % slots], out_sem.at[i % slots])
    drain(bc_ref, sems.at[ZERO])


def unpack(a, bc, d, f):
    ff = a.shape[ONE]
    vm = pl.BlockSpec(memory_space=pltpu.VMEM)
    slots = 4
    dma = pltpu.SemaphoreType.DMA
    return pl.pallas_call(
        unpack_kernel, out_shape=(sds((ff, d), F32), sds((d, ff), F32), sds((d, d), F32), sds((f, d), F32)),
        in_specs=[ANY, vm], out_specs=(ANY,) * 4,
        scratch_shapes=[pltpu.VMEM((slots, d // WIDTH, TILE, WIDTH), F32), dma((ONE,)), dma((slots,)), dma((slots,))],
        compiler_params=vmem(12), name="unpack",
    )(a, pltpu.with_memory_space_constraint(bc, pltpu.VMEM))


def solution(mesh):
    axis = mesh.axis_names[ZERO]
    n_dev = mesh.shape[axis]

    def local_step(q_hidden, q_mask, p_hidden, p_mask, w_qkv, b_qkv, w_out, b_out, ln1_gain, ln1_shift,
                   w_up, b_up, w_down, b_down, ln2_gain, ln2_shift):
        nq, _, d = q_hidden.shape
        n_pass, p_len = nq * p_hidden.shape[ONE], p_hidden.shape[TWO]
        _, three, heads, head = w_qkv.shape
        xq, xp = q_hidden.reshape(-ONE, d), p_hidden.reshape(-ONE, d)
        p_mask = p_mask.reshape(n_pass, p_len)
        wqkv_t = w_qkv.transpose(ONE, TWO, THREE, ZERO).reshape(-ONE, d)
        wo = w_out.reshape(-ONE, d)
        vecs = [v.reshape(ONE, d) for v in (b_out, ln1_gain, ln1_shift, b_down, ln2_gain, ln2_shift)]

        qkv_q, qkv_p = qkv_project(xq, xp, wqkv_t, b_qkv.reshape(ONE, -ONE))
        probs_q, ctx_q = attention(qkv_q, q_mask, head)
        probs_p, ctx_p = attention(qkv_p, p_mask, head)
        h, r1, g, gp, r2, pooled = ffn_forward(
            xq, xp, ctx_q, ctx_p, wo, vecs, q_mask, p_mask, w_up, b_up.reshape(ONE, -ONE), w_down)
        everyone = gather_embeddings(pooled, axis, ONE)
        mean_loss, d_pooled = loss_and_grad(everyone, pooled, axis, nq * n_dev)
        dwd, dr2, dr2b, dvec2 = down_backward(d_pooled, r2, q_mask, p_mask, vecs[4], g)
        dwb, dbu, dr1_q, dr1_p, low_q, low_p, dvec1, piece_a, _ = up_backward(
            axis, dr2, dr2b, h, gp, w_down, w_up, r1, vecs[ONE], ctx_q, ctx_p, dwd.reshape(-ONE, WIDTH), TWO)
        dwq, dbq, dh_q, dh_p, piece_b, _, a = attn_qkv_backward(
            axis, low_q, low_p, wo, qkv_q, qkv_p, probs_q, probs_p, xq, xp, wqkv_t, dr1_q, dr1_p, dwb.reshape(-ONE, WIDTH), piece_a, head, THREE)
        bc, small = finish_sum(axis, UNITS_B, UNITS_C, piece_b, dwq.reshape(-ONE, WIDTH), dvec1, dvec2, dbq, dbu, 4)
        d_down, d_up, d_out, d_qkv = unpack(a.reshape(dwd.shape), bc, d, three * d)
        vec, bias = small[:8], small[8:]
        return (mean_loss, dh_q.reshape(q_hidden.shape), dh_p.reshape(p_hidden.shape),
                d_qkv.reshape(three, heads, head, d).transpose(THREE, ZERO, ONE, TWO), bias[:three].reshape(b_qkv.shape),
                d_out.reshape(w_out.shape), vec[ZERO], vec[ONE], vec[TWO], d_up, bias[three:-ONE].reshape(-ONE),
                d_down, vec[THREE], vec[4], vec[5])

    in_specs = (P(axis),) * 4 + (P(),) * 12
    out_specs = (P(), P(axis), P(axis)) + (P(),) * 12
    return jax.shard_map(local_step, mesh=mesh, in_specs=in_specs, out_specs=out_specs, check_vma=False)
```

```python
import functools
import types
import jax
import jax.numpy as jnp
from jax import lax
from jax.experimental import pallas as pl
from jax.experimental.pallas import tpu as pltpu
from jax.sharding import PartitionSpec as P

ZERO, ONE, TWO, THREE, ALL = 0, 1, 2, 3, ...

F32 = jnp.float32
BF16 = jnp.bfloat16
LOGICAL = pl.DeviceIdType.LOGICAL
RING = 4
WIDTH = 256
COLOURS = range(6)
AXES = range(THREE)
RINGS = range(RING)
TURNS = range(RING * RING)
ANY = pl.BlockSpec(memory_space=pl.ANY)


def mesh_place(axis):
    me = lax.axis_index(axis)
    core = lax.rem(me, TWO)
    chip = lax.div(me, TWO)
    row = lax.div(chip, RING)
    return (lax.rem(chip, RING), lax.rem(row, RING), lax.div(row, RING)), core


def device_at(coords, core):
    return ((coords[TWO] * RING + coords[ONE]) * RING + coords[ZERO]) * TWO + core


def moved(coords, dim, by):
    out = list(coords)
    out[dim] = lax.rem(coords[dim] + by + TWO * RING, RING)
    return tuple(out)


def wrap(i):
    return lax.rem(i + 4 * RING, RING)


def rdma(src, dst, send, recv, to):
    pltpu.make_async_remote_copy(src_ref=src, dst_ref=dst, send_sem=send, recv_sem=recv,
                                 device_id=to, device_id_type=LOGICAL).start()


def copy(src, dst, sem):
    pltpu.make_async_copy(src, dst, sem).start()


def drain(ref, sem):
    pltpu.make_async_copy(ref, ref, sem).wait()


def carve(sems, *counts):
    out, at = [], ZERO
    for n in counts:
        out.append(lambda i, at=at: sems.at[at + i])
        at += n
    return out


def ring_plan(axis, units):
    coords, core = mesh_place(axis)
    p = types.SimpleNamespace(coords=coords, core=core, partner=device_at(coords, ONE - core))
    p.dims = [tuple((k // TWO + s) % THREE for s in AXES) for k in COLOURS]
    p.sign = [ONE - TWO * (k % TWO) for k in COLOURS]
    p.pos = [tuple(coords[d] for d in p.dims[k]) for k in COLOURS]
    p.nxt = [tuple(device_at(moved(coords, d, p.sign[k]), core) for d in p.dims[k]) for k in COLOURS]
    p.piece = [8 * u for u in units]
    p.lead = [sum(p.piece[:k]) for k in COLOURS]
    p.all = sum(p.piece)
    p.half = 64 * p.all
    p.base = core * p.half
    p.peers = [p.partner] + [device_at(moved(coords, d, by), core) for d in AXES for by in (ONE, THREE)]
    p.across = [device_at(moved(coords, d, TWO), core) for d in AXES]
    p.prv = [tuple(device_at(moved(coords, d, -p.sign[k]), core) for d in p.dims[k]) for k in COLOURS]
    return p


def rows(at, n):
    return pl.ds(pl.multiple_of(at, 8), n)


def place_of(p, k, ring, back):
    return wrap(p.pos[k][ring] - p.sign[k] * back)


def chunk_row(p, k, back):
    return 64 * p.lead[k] + place_of(p, k, ZERO, back) * (16 * p.piece[k])


def sub_row(p, k, row, back):
    return row + place_of(p, k, ONE, back) * (4 * p.piece[k])


def piece_row(p, k, row, back):
    return row + place_of(p, k, TWO, back) * p.piece[k]


GIVE = (TWO, ONE, THREE, ZERO)
TAKE = (ZERO, ONE, THREE, TWO)


def signal_peers(peers):
    barrier = pltpu.get_barrier_semaphore()
    for peer in peers:
        pl.semaphore_signal(barrier, inc=ONE, device_id=peer, device_id_type=LOGICAL)


def await_peers(peers):
    pl.semaphore_wait(pltpu.get_barrier_semaphore(), len(peers))


SCATTER_SEMS = 4 + THREE * 16 + TWO * 12 + 4 * THREE


def scatter_scratch(units):
    n = 8 * sum(units)
    vm = lambda *s: pltpu.VMEM(s + (WIDTH,), F32)
    return [vm(64 * n), vm(TWO, 4 * n), vm(THREE, RING, 4 * n), vm(THREE, 4 * n), vm(THREE, n), pltpu.SemaphoreType.DMA((SCATTER_SEMS,))]


def scatter_rounds(p, src, part, out, acc, stage, land1, land2, land3, sems):
    load_sem, swap_send, swap_recv, stage_sem, p1_send, p1_recv, p2_send, p2_recv, p3_send, p3_recv = carve(
        sems, 4, 16, 16, 16, 12, 12, THREE, THREE, THREE, THREE)
    n_sub, n_chunk = 4 * p.all, 16 * p.all
    far = p.half - p.base

    def turn_row(k, n):
        return sub_row(p, k, chunk_row(p, k, n // RING + ONE), GIVE[n % RING])

    def load(t):
        for k in COLOURS:
            r, m = chunk_row(p, k, t + ONE), 16 * p.piece[k]
            copy(src.at[rows(p.base + r, m)], acc.at[rows(r, m)], load_sem(t))

    def swap(n):
        for k in COLOURS:
            r, m = turn_row(k, n), 4 * p.piece[k]
            rdma(src.at[rows(far + r, m)], part.at[rows(r, m)], swap_send(n), swap_recv(n), p.partner)

    def fetch(n):
        drain(part.at[pl.ds(ZERO, n_sub)], swap_recv(n))
        for k in COLOURS:
            m = 4 * p.piece[k]
            copy(part.at[rows(turn_row(k, n), m)], stage.at[n % TWO, pl.ds(4 * p.lead[k], m)], stage_sem(n))

    def begin():
        for t in RINGS:
            load(t)
        for n in range(6):
            swap(n)

    def turn(n):
        t, i = n // RING, n % RING
        if n == ZERO:
            fetch(n)
        if n + 6 < 16:
            swap(n + 6)
        if n + ONE < 16:
            fetch(n + ONE)
        if i == ZERO:
            drain(acc.at[pl.ds(ZERO, n_chunk)], load_sem(t))
        drain(stage.at[n % TWO], stage_sem(n))
        if t > ZERO:
            drain(land1.at[t - ONE, i], p1_recv(n - 4))
        for k in COLOURS:
            at, m = rows(turn_row(k, n), 4 * p.piece[k]), pl.ds(4 * p.lead[k], 4 * p.piece[k])
            val = acc[at] + stage[n % TWO, m]
            acc[at] = val + land1[t - ONE, i, m] if t > ZERO else val
        if t < THREE:
            for k in COLOURS:
                at, m = rows(turn_row(k, n), 4 * p.piece[k]), pl.ds(4 * p.lead[k], 4 * p.piece[k])
                rdma(acc.at[at], land1.at[t, i, m], p1_send(n), p1_recv(n), p.nxt[k][ZERO])

    def pass_on(i, where, land, send, recv, ring):
        if i == TWO:
            drain(land.at[ZERO], recv(ZERO))
        for k in COLOURS:
            at, m = where(k, i)
            if i == TWO:
                acc[at] += land[ZERO, m]
        for k in COLOURS:
            at, m = where(k, i)
            rdma(acc.at[at], land.at[i, m], send(i), recv(i), (p.prv if i == ONE else p.nxt)[k][ring])

    def sub_at(k, i):
        return rows(turn_row(k, 12 + i), 4 * p.piece[k]), pl.ds(4 * p.lead[k], 4 * p.piece[k])

    def piece_at(k, i):
        return rows(piece_row(p, k, turn_row(k, 15), GIVE[i]), p.piece[k]), pl.ds(p.lead[k], p.piece[k])

    def second(i):
        pass_on(i, sub_at, land2, p2_send, p2_recv, ONE)

    def third():
        for i in (ONE, TWO):
            drain(land2.at[i], p2_recv(i))
        for k in COLOURS:
            at, m = sub_at(k, THREE)
            acc[at] += land2[ONE, m] + land2[TWO, m]
        for i in (ZERO, ONE):
            pass_on(i, piece_at, land3, p3_send, p3_recv, TWO)

    def fourth():
        pass_on(TWO, piece_at, land3, p3_send, p3_recv, TWO)

    def last():
        for i in (ONE, TWO):
            drain(land3.at[i], p3_recv(i))
        for k in COLOURS:
            at, m = piece_at(k, THREE)
            out[m] = acc[at] + (land3[ONE, m] + land3[TWO, m])

    def finish():
        for n in TURNS:
            drain(acc.at[pl.ds(ZERO, n_sub)], swap_send(n))
        for n in range(12):
            drain(acc.at[pl.ds(ZERO, n_sub)], p1_send(n))
        for t in AXES:
            drain(acc.at[pl.ds(ZERO, n_sub)], p2_send(t))
            drain(acc.at[pl.ds(ZERO, p.all)], p3_send(t))

    act = functools.partial
    def both(*fs):
        def run():
            for f in fs:
                f()
        return run
    steps = [begin] + [act(turn, n) for n in range(12)]
    steps += [both(act(turn, 12 + i), act(second, i)) for i in AXES] + [act(turn, 15), third, fourth, last, finish]
    return steps


GATHER_SEMS = ONE + TWO * (THREE + THREE + 12 + 16)


def gather_rounds(p, piece, out, sems):
    own_sem, a3_send, a3_recv, a2_send, a2_recv, a1_send, a1_recv, push_send, push_recv = carve(
        sems, ONE, THREE, THREE, THREE, THREE, 12, 12, 16, 16)
    n_sub = 4 * p.all

    def many(n):
        return out.at[pl.ds(ZERO, n)]

    def sub_at(k, c, s):
        return rows(p.base + sub_row(p, k, chunk_row(p, k, c), TAKE[s]), 4 * p.piece[k])

    def piece_at(k, g):
        return rows(p.base + piece_row(p, k, sub_row(p, k, chunk_row(p, k, ZERO), ZERO), TAKE[g]), p.piece[k])

    def both_ways(at, send, recv, ring, srcs=out):
        for k in COLOURS:
            src = out.at[at(k)] if srcs is out else srcs.at[pl.ds(p.lead[k], p.piece[k])]
            rdma(src, out.at[at(k)], send(ZERO), recv(ZERO), p.nxt[k][ring])
            rdma(src, out.at[at(k)], send(ONE), recv(ONE), p.prv[k][ring])

    def forward(at, send, recv, ring):
        for k in COLOURS:
            rdma(out.at[at(k)], out.at[at(k)], send(TWO), recv(TWO), p.nxt[k][ring])

    def third():
        for k in COLOURS:
            copy(piece.at[pl.ds(p.lead[k], p.piece[k])], out.at[piece_at(k, ZERO)], own_sem(ZERO))
        both_ways(lambda k: piece_at(k, ZERO), a3_send, a3_recv, TWO, piece)

    def fourth():
        drain(many(p.all), a3_recv(ZERO))
        forward(lambda k: piece_at(k, ONE), a3_send, a3_recv, TWO)

    def hop1(c, s):
        for k in COLOURS:
            if c < THREE:
                rdma(out.at[sub_at(k, c, s)], out.at[sub_at(k, c, s)], a1_send(RING * c + s), a1_recv(RING * c + s), p.nxt[k][ZERO])
            rdma(out.at[sub_at(k, c, s)], out.at[sub_at(k, c, s)], push_send(RING * c + s), push_recv(RING * c + s), p.partner)

    def second(s):
        if s == ZERO:
            for sem in (own_sem(ZERO), a3_recv(ONE), a3_recv(TWO)):
                drain(many(p.all), sem)
            both_ways(lambda k: sub_at(k, ZERO, ZERO), a2_send, a2_recv, ONE)
        else:
            drain(many(n_sub), a2_recv(s - ONE))
        if s == ONE:
            forward(lambda k: sub_at(k, ZERO, ONE), a2_send, a2_recv, ONE)
        hop1(ZERO, s)

    def first(c, s):
        drain(many(n_sub), a1_recv(RING * (c - ONE) + s))
        hop1(c, s)

    def finish():
        for t in AXES:
            drain(many(p.all), a3_send(t))
            drain(many(n_sub), a2_send(t))
        for n in range(12):
            drain(many(n_sub), a1_send(n))
        for n in TURNS:
            drain(many(n_sub), push_send(n))
            drain(many(n_sub), push_recv(n))

    act = functools.partial
    return ([third, fourth] + [act(second, s) for s in RINGS]
            + [act(first, c, s) for c in (ONE, TWO, THREE) for s in RINGS] + [finish])


def small_scratch(shape):
    return [pltpu.VMEM((4, THREE) + shape, F32), pltpu.SemaphoreType.DMA((8,))]


def small_rounds(p, src, out, land, sems):
    places = [(None, p.core, TWO)] + [(d, p.coords[d], RING) for d in AXES]

    def send(n):
        d, _, size = places[n]
        for by in range(ONE, size):
            to = p.partner if d is None else device_at(moved(p.coords, d, by), p.core)
            rdma(out, land.at[n, by - ONE], sems.at[n], sems.at[4 + n], to)

    def step(n):
        if n == ZERO:
            out[ALL] = src[ALL]
        else:
            _, place, size = places[n - ONE]
            got = land.at[n - ONE, pl.ds(ZERO, size - ONE)]
            drain(got, sems.at[4 + n - ONE])
            drain(got, sems.at[n - ONE])
            mine, total = out[ALL], None
            for q in range(size):
                val = mine
                for by in range(ONE, size):
                    val = jnp.where(lax.rem(place - q + size, size) == by, land[n - ONE, by - ONE], val)
                total = val if total is None else total + val
            out[ALL] = total
        if n < 4:
            send(n)

    return [functools.partial(step, n) for n in range(5)]


def spread(steps, slots):
    plan = [[] for _ in range(slots)]
    for i, s in enumerate(steps):
        plan[i * slots // len(steps)].append(s)
    return plan


def finish_kernel(axis, units_b, units_c, pieceb_ref, c_ref, a_ref, vec1_ref, vec2_ref, bq_ref, bu_ref, bc_out, small_out, part,
                  small_ref, piecec, a_sem, *scratch):
    sc, (gather_sem, gather_sem2, small_land, small_sem) = scratch[:6], scratch[6:]
    pb, pc = ring_plan(axis, units_b), ring_plan(axis, units_c)
    n_b, n_c = TWO * pb.half, TWO * pc.half
    b_out, c_out = bc_out.at[pl.ds(ZERO, n_b)], bc_out.at[pl.ds(n_b, n_c)]
    a_here = bc_out.at[pl.ds(n_b + n_c, bc_out.shape[ZERO] - n_b - n_c)]
    peers = pb.peers + pb.across
    signal_peers(peers)
    copy(a_ref.at[pl.ds(ZERO, a_here.shape[ZERO])], a_here, a_sem.at[ZERO])
    width = small_ref.shape[ONE]
    small_ref[ALL] = jnp.zeros_like(small_ref)
    small_ref[ZERO:THREE, :] = vec1_ref[ZERO:THREE, :]
    small_ref[THREE:6, :] = vec2_ref[ZERO:THREE, :]
    at = 8
    for ref in (bq_ref, bu_ref):
        for i in range(ref.shape[ONE] // width):
            small_ref[at:at + ONE, :] = ref[:, i * width:(i + ONE) * width]
            at += ONE
    await_peers(peers)
    reduce_c = scatter_rounds(pc, c_ref, part, piecec, *sc)
    gather_b = gather_rounds(pb, pieceb_ref, b_out, gather_sem)
    gather_c = gather_rounds(pc, piecec, c_out, gather_sem2)
    smalls = small_rounds(pb, small_ref, small_out, small_land, small_sem)
    main = reduce_c[:-ONE] + gather_c[:-ONE]
    fill = spread(gather_b[:-ONE], len(main) - 4)
    for i, f in enumerate(main):
        f()
        if i % THREE == ONE and i // THREE < len(smalls):
            smalls[i // THREE]()
        for f in fill[i] if i < len(fill) else ():
            f()
    for rounds in (reduce_c, gather_b, gather_c):
        rounds[-ONE]()
    drain(a_here, a_sem.at[ZERO])


def finish_sum(axis, units_b, units_c, piece_b, c, a, keep, vec1, vec2, bq, bu, collective_id):
    sds = jax.ShapeDtypeStruct
    dma = pltpu.SemaphoreType.DMA
    vm = pl.BlockSpec(memory_space=pltpu.VMEM)
    n = c.shape[ZERO]
    small = (16, vec1.shape[ONE])
    outs = pl.pallas_call(
        functools.partial(finish_kernel, axis, units_b, units_c),
        out_shape=(pltpu.VMEM((piece_b.shape[ZERO] * 128 + n + keep, WIDTH), F32), sds(small, F32), sds((n // TWO, WIDTH), F32)),
        in_specs=[vm, ANY, ANY, vm, vm, vm, vm], out_specs=(vm, vm, ANY),
        scratch_shapes=[pltpu.VMEM(small, F32), pltpu.VMEM((n // 128, WIDTH), F32), dma((ONE,))] + scatter_scratch(units_c)
        + [dma((GATHER_SEMS,)), dma((GATHER_SEMS,))] + small_scratch(small),
        compiler_params=pltpu.CompilerParams(collective_id=collective_id, has_side_effects=True, vmem_limit_bytes=17 * 1024 * 1024),
        name="finish_sum",
    )(piece_b, c, a, vec1, vec2, bq, bu)
    return outs[:TWO]


def gather_kernel(axis, pooled_ref, g_ref, e_ref, mine, theirs, swap_sem, sems_send, sems_recv, push_send, push_recv):
    coords, core = mesh_place(axis)
    partner = device_at(coords, ONE - core)
    width = e_ref.shape[ONE]
    lanes = pl.ds(pl.multiple_of(core * (width // TWO), 128), width // TWO)
    x, y, z = coords
    peers = [partner] + [device_at(moved(coords, d, by), core) for d in AXES for by in (ONE, TWO, THREE)]
    signal_peers(peers)
    size = row_sum(pooled_ref[ALL] * pooled_ref[ALL])
    e_ref[ALL] = pooled_ref[ALL] * jnp.where(size > 0.0, lax.rsqrt(size), 0.0)
    mine[ALL] = e_ref[ALL]
    await_peers(peers)

    rdma(e_ref, theirs, swap_sem.at[ZERO], swap_sem.at[ONE], partner)
    drain(theirs, swap_sem.at[ONE])
    first = jnp.where(core == ZERO, mine[:, lanes], theirs[:, lanes])
    second = jnp.where(core == ZERO, theirs[:, lanes], mine[:, lanes])
    g_ref[z, y, x, ZERO:4, lanes] = first[ZERO:4]
    g_ref[z, y, x, 4:8, lanes] = second[ZERO:4]
    g_ref[z, y, x, 8:16, lanes] = first[8:16]
    g_ref[z, y, x, 16:24, lanes] = second[8:16]
    drain(e_ref, swap_sem.at[ZERO])

    def view(a, stage):
        idx = [z, y, x]
        for s in range(stage):
            idx[TWO - (a + s) % THREE] = slice(None)
        return g_ref.at[idx[ZERO], idx[ONE], idx[TWO], pl.ds(8 * a, 8), lanes]

    for stage in range(THREE):
        for by in (ONE, THREE, TWO):
            for a in range(THREE):
                to = device_at(moved(coords, (a + stage) % THREE, by), core)
                rdma(view(a, stage), view(a, stage), sems_send.at[stage, by - ONE], sems_recv.at[stage, by - ONE], to)
        if stage == TWO:
            for a in range(THREE):
                rdma(view(a, TWO), view(a, TWO), push_send.at[ZERO], push_recv.at[ZERO], partner)
        for by in (ONE, THREE, TWO):
            n = 4 ** stage
            shape_like = g_ref.at[ZERO, ZERO, ZERO, :, lanes] if stage == ZERO else (
                g_ref.at[ZERO, ZERO, :, :, lanes] if stage == ONE else g_ref.at[ZERO, :, :, :, lanes])
            drain(shape_like, sems_recv.at[stage, by - ONE])
            if stage == TWO:
                for a in range(THREE):
                    far = moved(coords, (a + TWO) % THREE, RING - by)
                    idx = [far[TWO], far[ONE], far[ZERO]]
                    idx[TWO - a] = slice(None)
                    idx[TWO - (a + ONE) % THREE] = slice(None)
                    v = g_ref.at[idx[ZERO], idx[ONE], idx[TWO], pl.ds(8 * a, 8), lanes]
                    rdma(v, v, push_send.at[by], push_recv.at[by], partner)
    for stage in range(THREE):
        shape_like = g_ref.at[ZERO, ZERO, ZERO, :, lanes] if stage == ZERO else (
            g_ref.at[ZERO, ZERO, :, :, lanes] if stage == ONE else g_ref.at[ZERO, :, :, :, lanes])
        for by in (ONE, TWO, THREE):
            drain(shape_like, sems_send.at[stage, by - ONE])
    for by in range(4):
        drain(g_ref.at[ZERO, :, :, :, lanes], push_send.at[by])
        drain(g_ref.at[ZERO, :, :, :, lanes], push_recv.at[by])


def gather_embeddings(e, axis, collective_id):
    dma = pltpu.SemaphoreType.DMA
    width = e.shape[ONE]
    g = pl.pallas_call(
        functools.partial(gather_kernel, axis),
        out_shape=jax.ShapeDtypeStruct((RING, RING, RING, 24, width), F32),
        in_specs=[pl.BlockSpec(memory_space=pltpu.VMEM)],
        out_specs=pl.BlockSpec(memory_space=pltpu.VMEM),
        scratch_shapes=[pltpu.VMEM(e.shape, F32)] * THREE + [dma((TWO,)),
                        dma((THREE, THREE)), dma((THREE, THREE)), dma((4,)), dma((4,))],
        compiler_params=pltpu.CompilerParams(collective_id=collective_id, has_side_effects=True,
                                             vmem_limit_bytes=16 * 1024 * 1024),
        name="gather_embeddings",
    )(e)
    return g.reshape(RING ** THREE, 24, width)


def split3(x):
    hi = x.astype(BF16)
    rest = x - hi.astype(F32)
    mid = rest.astype(BF16)
    return hi, mid, (rest - mid.astype(F32)).astype(BF16)


def dot6(a, b, dims):
    low = mm(a[TWO], b[ZERO], dims) + mm(a[ZERO], b[TWO], dims) + mm(a[ONE], b[ONE], dims)
    return mm(a[ZERO], b[ZERO], dims) + (mm(a[ZERO], b[ONE], dims) + mm(a[ONE], b[ZERO], dims) + low)


def loss_kernel(axis, n_query, g_ref, pooled_ref, loss_ref, d_ref, logit_ref, lse_ref, q_ref, p_ref, dp_ref):
    me = lax.axis_index(axis)
    core, chip = lax.rem(me, TWO), lax.div(me, TWO)
    chips, _, width = g_ref.shape
    nq = chips * 8
    lanes = 128
    gs = 100.0 / n_query
    for i, part in enumerate(split3(g_ref[:, ZERO:8, :].reshape(nq, width))):
        q_ref[i] = part
    block = TWO * lanes

    def logits(b, _):
        at = pl.multiple_of(b * block, block)
        p = split3(g_ref[pl.ds(b * (block // 16), block // 16), 8:24, :].reshape(block, width))
        for i, part in enumerate(p):
            p_ref[i, pl.ds(at, block), :] = part
        logit_ref[:, pl.ds(at, block)] = dot6((q_ref[ZERO], q_ref[ONE], q_ref[TWO]), p, NT) * 100.0
        return ZERO

    lax.fori_loop(ZERO, chips * 16 // block, logits, ZERO)

    def rows_of(b, loss):
        at = pl.ds(pl.multiple_of(b * lanes, lanes), lanes)
        s = logit_ref[at, :]
        top = jnp.max(s, axis=ONE, keepdims=True)
        lse = jnp.log(row_sum(jnp.exp(s - top))) + top
        lse_ref[at, :] = jnp.broadcast_to(lse, (lanes, lanes))
        row = lax.broadcasted_iota(jnp.int32, s.shape, ZERO) + b * lanes
        col = lax.broadcasted_iota(jnp.int32, s.shape, ONE)
        return loss + col_sum(lse - row_sum(jnp.where(col == TWO * row, s, 0.0)))

    loss = lax.fori_loop(ZERO, nq // lanes, rows_of, jnp.zeros((ONE, ONE), F32))
    loss_ref[ALL] = jnp.broadcast_to(loss * (1.0 / n_query), loss_ref.shape)

    def weights(s, lse, row, col):
        row = lax.broadcasted_iota(jnp.int32, s.shape, ZERO) + row
        col = lax.broadcasted_iota(jnp.int32, s.shape, ONE) + col
        return jnp.exp(s - lse) * gs - jnp.where(col == TWO * row, gs, 0.0)

    at = pl.ds(pl.multiple_of(chip * 8, 8), 8)
    w = jnp.concatenate([x.astype(F32) for x in split3(weights(logit_ref[at, :], lse_ref[at, ZERO:ONE], chip * 8, ZERO))], axis=ZERO).astype(BF16)
    by_hi, by_mid, by_low = (mm(w, p_ref[i]) for i in range(THREE))
    dq = by_hi[ZERO:8] + (by_hi[8:16] + by_mid[ZERO:8] + (by_hi[16:24] + by_mid[8:16] + by_low[ZERO:8]))

    first = pl.multiple_of(lax.div(chip, 8) * lanes, lanes)
    w = weights(logit_ref[:, pl.ds(first, lanes)], lse_ref[ALL], ZERO, first)
    dp_ref[ALL] = dot6(split3(w.T), (q_ref[ZERO], q_ref[ONE], q_ref[TWO]), NN)
    dp = dp_ref[pl.ds(pl.multiple_of(lax.rem(chip, 8) * 16 + core * 8, 8), 8), :]

    def back(d, pooled):
        inv = lax.rsqrt(row_sum(pooled * pooled))
        e = pooled * inv
        return (d - e * row_sum(e * d)) * inv

    d_ref[ALL] = jnp.zeros_like(d_ref)
    d_ref[ZERO:4, :] = back(jnp.where(core == ZERO, dq[ZERO:4], dq[4:8]), pooled_ref[ZERO:4])
    d_ref[8:16, :] = back(dp, pooled_ref[8:16])


def loss_and_grad(g, pooled, axis, n_query):
    chips, _, width = g.shape
    nq, n_pass, lanes = chips * 8, chips * 16, 128
    vm = pl.BlockSpec(memory_space=pltpu.VMEM)
    loss, d = pl.pallas_call(
        functools.partial(loss_kernel, axis, n_query),
        out_shape=(jax.ShapeDtypeStruct((8, lanes), F32), jax.ShapeDtypeStruct(pooled.shape, F32)),
        in_specs=[vm] * TWO, out_specs=(vm,) * TWO,
        scratch_shapes=[pltpu.VMEM((nq, n_pass), F32), pltpu.VMEM((nq, lanes), F32), pltpu.VMEM((THREE, nq, width), BF16),
                        pltpu.VMEM((THREE, n_pass, width), BF16), pltpu.VMEM((lanes, width), F32)],
        compiler_params=vmem(28), name="loss_and_grad",
    )(g, pooled)
    return loss[ZERO, ZERO], d


NN = (((ONE,), (ZERO,)), ((), ()))
NT = (((ONE,), (ONE,)), ((), ()))
TN = (((ZERO,), (ZERO,)), ((), ()))
LN_EPS = 1e-12
NEG_FILL = -1e9
TILE = 512
UNITS_A, UNITS_B, UNITS_C = (THREE, THREE, THREE, THREE, TWO, TWO), (THREE, THREE, THREE, THREE, 4, 4), (TWO,) * 6
sds = jax.ShapeDtypeStruct


def mm(a, b, dims=NN):
    return lax.dot_general(a, b, dims, preferred_element_type=F32)


def vmem(mb=60):
    return pltpu.CompilerParams(vmem_limit_bytes=mb * 1024 * 1024)


def whole(*shape):
    return pl.BlockSpec(shape, lambda j: (ZERO,) * len(shape), pipeline_mode=pl.Buffered(ONE))


def across(rows, tile):
    return pl.BlockSpec((rows, tile), lambda j: (ZERO, j))


def down(tile, cols):
    return pl.BlockSpec((tile, cols), lambda j: (j, ZERO))


def row_mean(x):
    return jnp.mean(x, axis=ONE, keepdims=True)


def row_sum(x):
    return jnp.sum(x, axis=ONE, keepdims=True)


def col_sum(x):
    return jnp.sum(x, axis=ZERO, keepdims=True)


def qkv_kernel(xq_ref, xp_ref, w_ref, b_ref, oq_ref, op_ref, x_ref):
    tq = xq_ref.shape[ZERO]

    @pl.when(pl.program_id(ZERO) == ZERO)
    def _():
        x_ref[:tq, :] = xq_ref[ALL]
        x_ref[tq:, :] = xp_ref[ALL]
    y = (mm(x_ref[ALL], w_ref[ALL], NT) + b_ref[ALL]).astype(BF16)
    oq_ref[ALL] = y[:tq]
    op_ref[ALL] = y[tq:]


def qkv_project(xq, xp, w_t, b, tile=TILE):
    tq, d = xq.shape
    tp, f = xp.shape[ZERO], w_t.shape[ZERO]
    return pl.pallas_call(
        qkv_kernel, grid=(f // tile,),
        out_shape=(sds((tq, f), BF16), sds((tp, f), BF16)),
        in_specs=[whole(tq, d), whole(tp, d), down(tile, d), across(ONE, tile)],
        out_specs=(across(tq, tile), across(tp, tile)),
        scratch_shapes=[pltpu.VMEM((tq + tp, d), BF16)],
        compiler_params=vmem(), name="qkv_project",
    )(xq, xp, w_t, b)


def split_heads(pair, head):
    lane = lax.broadcasted_iota(jnp.int32, pair.shape, ONE)
    zero = jnp.zeros_like(pair)
    return jnp.concatenate([jnp.where(lane < head, pair, zero), jnp.where(lane >= head, pair, zero)], axis=ZERO)


def join_heads(stacked, head):
    t = stacked.shape[ZERO] // TWO
    lane = lax.broadcasted_iota(jnp.int32, (t, stacked.shape[ONE]), ONE)
    return jnp.where(lane < head, stacked[:t], stacked[t:])


def attn_kernel(scale, head, qkv_ref, mask_ref, probs_ref, ctx_ref):
    d = ctx_ref.shape[ONE]
    pair = TWO * head
    keep = mask_ref[ZERO] > ZERO
    for g in range(d // pair):
        at = pl.ds(g * pair, pair)
        q = split_heads(qkv_ref[:, at], head)
        k = qkv_ref[:, pl.ds(d + g * pair, pair)]
        v = qkv_ref[:, pl.ds(TWO * d + g * pair, pair)]
        s = jnp.where(keep, mm(q, k, NT) * scale, NEG_FILL)
        e = jnp.exp(s - jnp.max(s, axis=ONE, keepdims=True))
        p = (e / row_sum(e)).astype(BF16)
        probs_ref[ZERO, g] = p
        ctx_ref[:, at] = join_heads(mm(p, v), head).astype(BF16)


def attention(qkv, mask, head):
    n, seq = mask.shape
    d = qkv.shape[ONE] // THREE
    pairs = d // (TWO * head)
    return pl.pallas_call(
        functools.partial(attn_kernel, head ** -0.5, head), grid=(n,),
        out_shape=(sds((n, pairs, TWO * seq, seq), BF16), sds((n * seq, d), BF16)),
        in_specs=[down(seq, THREE * d), pl.BlockSpec((ONE, ONE, seq), lambda j: (j, ZERO, ZERO))],
        out_specs=(pl.BlockSpec((ONE, pairs, TWO * seq, seq), lambda j: (j, ZERO, ZERO, ZERO)), down(seq, d)),
        compiler_params=vmem(), name="attention",
    )(qkv, mask.reshape(n, ONE, seq))


def norm_rows(x):
    c = x - row_mean(x)
    r = lax.rsqrt(row_mean(c * c) + LN_EPS)
    return c * r, r


def norm_back(g, hat, r):
    return r * (g - row_mean(g) - hat * row_mean(g * hat))


ERFC = (0.07122347, -0.27794802, 0.29668747, -0.02018065, 0.21581222, 0.21731356, 0.24887118, 0.24822095)


def gelu_parts(u):
    bell = jnp.exp2(u * u * -0.7213475204)
    t = 1.0 / (1.0 + 0.311126984 * jnp.abs(u))
    poly = 0.5 * ERFC[ZERO]
    for c in ERFC[ONE:]:
        poly = poly * t + 0.5 * c
    tail = bell * (poly * t)
    return jnp.where(u >= 0.0, 1.0 - tail, tail), u * bell * 0.3989422804


def each_sequence(mq_ref, mp_ref, act):
    for first, lo, ref in ((ZERO, ZERO, mq_ref), (8, mq_ref.shape[ZERO] * mq_ref.shape[ONE], mp_ref)):
        n, seq = ref.shape

        def one(i, _):
            size = row_sum(ref[pl.ds(i, ONE), :].astype(F32))
            token = lax.broadcasted_iota(jnp.int32, (seq, ONE), ZERO).astype(F32)
            act(first + i, pl.ds(pl.multiple_of(lo + i * seq, 16), seq), jnp.where(token < size, 1.0 / size, 0.0))
            return ZERO
        lax.fori_loop(ZERO, n, one, ZERO)


def each_block(lo, hi, act, size=304):
    def one(i, _):
        act(pl.ds(pl.multiple_of(lo + i * size, 16), size))
        return ZERO
    lax.fori_loop(ZERO, (hi - lo) // size, one, ZERO)


def ffn_kernel(xq_ref, xp_ref, cq_ref, cp_ref, wo_ref, bo_ref, g1_ref, s1_ref, bd_ref, g2_ref, s2_ref, mq_ref, mp_ref,
               wu_ref, bu_ref, wd_ref, h_hbm, r1_hbm, g_ref, gp_ref, r2_hbm, pool_ref, h_ref, r1_ref, r2_ref, sems):
    j = pl.program_id(ZERO)
    t, tq = h_ref.shape[ZERO], cq_ref.shape[ZERO]
    saved = ((h_ref, h_hbm), (r1_ref, r1_hbm), (r2_ref, r2_hbm))

    @pl.when(j == ZERO)
    def _():
        for x_ref, c_ref, lo, size in ((xq_ref, cq_ref, ZERO, tq), (xp_ref, cp_ref, tq, 256)):
            def block(at):
                to = pl.ds(pl.multiple_of(lo + at.start, 16), size)
                r1 = x_ref[at, :].astype(F32) + mm(c_ref[at, :], wo_ref[ALL]) + bo_ref[ALL]
                r1_ref[to, :] = r1
                h = (norm_rows(r1)[ZERO] * g1_ref[ALL] + s1_ref[ALL]).astype(BF16)
                h_ref[to, :] = h
                r2_ref[to, :] = h.astype(F32) + bd_ref[ALL]
            each_block(ZERO, c_ref.shape[ZERO], block, size)
        for i in range(TWO):
            copy(*saved[i], sems.at[i])

    def block(at):
        u = mm(h_ref[at, :], wu_ref[ALL]) + bu_ref[ALL]
        cdf, upd = gelu_parts(u)
        g = (u * cdf).astype(BF16)
        g_ref[at, :] = g
        gp_ref[at, :] = cdf + upd
        r2_ref[at, :] += mm(g, wd_ref[ALL])
    each_block(ZERO, t, block)

    @pl.when(j == pl.num_programs(ZERO) - ONE)
    def _():
        copy(*saved[TWO], sems.at[TWO])
        pool_ref[ALL] = jnp.zeros_like(pool_ref)

        def pool(row, at, weight):
            y = norm_rows(r2_ref[at, :])[ZERO] * g2_ref[ALL] + s2_ref[ALL]
            pool_ref[pl.ds(row, ONE), :] = col_sum(y * weight)
        each_sequence(mq_ref, mp_ref, pool)
        for i in range(THREE):
            drain(saved[i][ZERO], sems.at[i])


def ffn_forward(xq, xp, ctx_q, ctx_p, w_out, vecs, mask_q, mask_p, w_up, b_up, w_down, tile=TWO * TILE):
    tq, d = xq.shape
    tp, f = xp.shape[ZERO], w_up.shape[ONE]
    t = tq + tp
    return pl.pallas_call(
        ffn_kernel, grid=(f // tile,),
        out_shape=(sds((t, d), BF16), sds((t, d), F32), sds((t, f), BF16), sds((t, f), F32), sds((t, d), F32), sds((16, d), F32)),
        in_specs=[whole(tq, d), whole(tp, d), whole(tq, d), whole(tp, d), whole(d, d), *(whole(ONE, d) for _ in vecs),
                  whole(*mask_q.shape), whole(*mask_p.shape), across(d, tile), across(ONE, tile), down(tile, d)],
        out_specs=(ANY, ANY, across(t, tile), across(t, tile), ANY, whole(16, d)),
        scratch_shapes=[pltpu.VMEM((t, d), BF16), pltpu.VMEM((t, d), F32), pltpu.VMEM((t, d), F32), pltpu.SemaphoreType.DMA((THREE,))],
        compiler_params=vmem(), name="ffn_forward",
    )(xq, xp, ctx_q, ctx_p, w_out, *vecs, mask_q, mask_p, w_up, b_up, w_down)


def store_blocks(ref, val):
    for c in range(ref.shape[ZERO]):
        ref[c] = val[:, c * WIDTH:(c + ONE) * WIDTH]


def down_bwd_kernel(dpool_ref, r2_ref, mq_ref, mp_ref, g2_ref, g_ref, dwd_ref, dr2_hbm, dr2b_hbm, dvec_ref, dr2_ref, dr2b_ref, sems):
    j = pl.program_id(ZERO)
    saved = ((dr2_ref, dr2_hbm), (dr2b_ref, dr2b_hbm))

    @pl.when(j == ZERO)
    def _():
        dvec_ref[ALL] = jnp.zeros_like(dvec_ref)

        def one(row, at, weight):
            hat, r = norm_rows(r2_ref[at, :])
            dy = weight * dpool_ref[pl.ds(row, ONE), :]
            dr2 = norm_back(dy * g2_ref[ALL], hat, r)
            dr2_ref[at, :] = dr2
            dr2b_ref[at, :] = dr2.astype(BF16)
            dvec_ref[ZERO:ONE, :] += col_sum(dr2)
            dvec_ref[ONE:TWO, :] += col_sum(dy * hat)
            dvec_ref[TWO:THREE, :] += col_sum(dy)
        each_sequence(mq_ref, mp_ref, one)
        for i in range(TWO):
            copy(*saved[i], sems.at[i])

    store_blocks(dwd_ref, mm(g_ref[ALL], dr2b_ref[ALL], TN))

    @pl.when(j == pl.num_programs(ZERO) - ONE)
    def _():
        for i in range(TWO):
            drain(saved[i][ZERO], sems.at[i])


def down_backward(dpool, r2, mask_q, mask_p, gain, g, tile=TWO * TILE):
    t, d = r2.shape
    f = g.shape[ONE]
    n = d // WIDTH
    return pl.pallas_call(
        down_bwd_kernel, grid=(f // tile,),
        out_shape=(sds((n, f, WIDTH), F32), sds((t, d), F32), sds((t, d), BF16), sds((8, d), F32)),
        in_specs=[whole(*dpool.shape), whole(t, d), whole(*mask_q.shape), whole(*mask_p.shape), whole(ONE, d), across(t, tile)],
        out_specs=(pl.BlockSpec((n, tile, WIDTH), lambda j: (ZERO, j, ZERO)), ANY, ANY, whole(8, d)),
        scratch_shapes=[pltpu.VMEM((t, d), F32), pltpu.VMEM((t, d), BF16), pltpu.SemaphoreType.DMA((TWO,))],
        compiler_params=vmem(), name="down_backward",
    )(dpool, r2, mask_q, mask_p, gain, g)


PACE_UP = (3.0, 2.5, 6.0, 4.0)
PACE_B = (4.5, 2.8, 5.5, 4.5)
PACE_A = (9.0, 3.2, 0.0, 0.0)
def place(timed, slot_times):
    plan = [[] for _ in slot_times]
    for t, f in sorted(timed, key=lambda x: x[ZERO]):
        plan[min([i for i, at in enumerate(slot_times) if at >= t], default=-ONE)].append(f)
    return plan


def timeline(steps, start, pace, before_third, before_last):
    n = len(steps)
    times = [0.0] + [start + pace * i for i in range(n - TWO)] + [1e3]
    if before_last:
        times[-4] = times[-5] + before_third
        times[-THREE] = times[-4] + before_last
        times[-TWO] = times[-THREE] + before_last
    return list(zip(times, steps))


def run_slot(plan, j, per, steps, point):
    for s in range(*steps):
        todo = plan[s * per + point]
        if todo:
            @pl.when(j == s)
            def _():
                for f in todo:
                    f()


def host(collective_id, mb):
    return pltpu.CompilerParams(collective_id=collective_id, has_side_effects=True, vmem_limit_bytes=mb * 1024 * 1024)


def up_bwd_kernel(axis, steps, dr2_hbm, dr2b_ref, h_ref, gp_ref, wd_ref, wu_ref, r1_hbm, g1_ref, cq_hbm, cp_hbm, a_ref,
                  dw_ref, dbu_ref, dr1q_hbm, dr1p_hbm, lowq_hbm, lowp_hbm, dvec_ref, piece_ref, part_ref,
                  dr1_ref, low_ref, r1_ref, ctx_ref, ht_ref, in_sem, out_sem, *scratch):
    j = pl.program_id(ZERO)
    t, tq, tp = dr1_ref.shape[ZERO], dr1q_hbm.shape[ZERO], dr1p_hbm.shape[ZERO]
    p = ring_plan(axis, UNITS_A)
    pace = 5.6
    timed = timeline(scatter_rounds(p, a_ref, part_ref, piece_ref, *scratch), *PACE_UP)
    points = THREE
    plan = place(timed, [pace * (s // points) + pace * (s % points) / points for s in range(points * (steps + TWO))])
    pause = functools.partial(run_slot, plan, j, points)
    q_rows, p_rows = pl.ds(ZERO, tq), pl.ds(tq, tp)
    late = ((r1_hbm, r1_ref), (cq_hbm, ctx_ref.at[q_rows]), (cp_hbm, ctx_ref.at[p_rows]))
    results = ((dr1_ref.at[q_rows], dr1q_hbm), (dr1_ref.at[p_rows], dr1p_hbm), (low_ref.at[q_rows], lowq_hbm), (low_ref.at[p_rows], lowp_hbm))

    @pl.when(j == ZERO)
    def _():
        signal_peers(p.peers)
        copy(dr2_hbm, dr1_ref, in_sem.at[ZERO])
        ht_ref[ALL] = h_ref[ALL].T
        drain(dr1_ref, in_sem.at[ZERO])
        for i in range(THREE):
            copy(*late[i], in_sem.at[ONE + i])

    @pl.when(j < steps)
    def _():
        dg = mm(dr2b_ref[ALL], wd_ref[ALL], NT).astype(BF16).astype(F32)
        dpre = dg * gp_ref[ALL]
        dbu_ref[ALL] = col_sum(dpre)
        dpre = dpre.astype(BF16)

        @pl.when(j == ZERO)
        def _():
            await_peers(p.peers)
        pause((ZERO, steps), ZERO)
        store_blocks(dw_ref, mm(ht_ref[ALL], dpre))
        pause((ZERO, steps), ONE)
        dr1_ref[ALL] += mm(dpre, wu_ref[ALL], NT)
        pause((ZERO, steps), TWO)

    def norm_backward(at):
        dy = dr1_ref[at, :].astype(BF16).astype(F32)
        hat, r = norm_rows(r1_ref[at, :])
        dr1 = norm_back(dy * g1_ref[ALL], hat, r)
        dr1_ref[at, :] = dr1
        low_ref[at, :] = dr1.astype(BF16)
        dvec_ref[ZERO:ONE, :] += col_sum(dr1)
        dvec_ref[ONE:TWO, :] += col_sum(dy * hat)
        dvec_ref[TWO:THREE, :] += col_sum(dy)

    @pl.when(j == steps)
    def _():
        dvec_ref[ALL] = jnp.zeros_like(dvec_ref)
        for i in range(THREE):
            drain(late[i][ONE], in_sem.at[ONE + i])
        each_block(ZERO, t, norm_backward)
        pause((steps, steps + ONE), ZERO)
        for i in range(4):
            copy(*results[i], out_sem.at[i])

    @pl.when(j >= steps)
    def _():
        half = dr1_ref.shape[ONE] // TWO
        at = pl.ds(pl.multiple_of(jnp.maximum(j - steps, ZERO) * half, half), half)
        pause((steps + ONE, steps + TWO), ZERO)
        pause((steps, steps + TWO), ONE)
        store_blocks(dw_ref, mm(ctx_ref[ALL], low_ref[:, at], TN))
        pause((steps, steps + TWO), TWO)

    @pl.when(j == steps + ONE)
    def _():
        for i in range(4):
            drain(results[i][ZERO], out_sem.at[i])


def up_backward(axis, dr2, dr2b, h, gp, w_down, w_up, r1, gain, ctx_q, ctx_p, part_a, collective_id, tile=TILE):
    t, d = h.shape
    f = w_up.shape[ONE]
    tq, tp = ctx_q.shape[ZERO], ctx_p.shape[ZERO]
    n, total, steps = tile // WIDTH, part_a.shape[ZERO], f // tile
    cut = lambda j: jnp.minimum(j, steps - ONE)
    wide = lambda rows: pl.BlockSpec((rows, tile), lambda j: (ZERO, cut(j)))
    dma, vm = pltpu.SemaphoreType.DMA, pltpu.VMEM
    return pl.pallas_call(
        functools.partial(up_bwd_kernel, axis, steps), grid=(steps + TWO,),
        out_shape=(sds(((f + d) // WIDTH, d, WIDTH), F32), sds((ONE, f), F32), sds((tq, d), F32), sds((tp, d), F32),
                   sds((tq, d), BF16), sds((tp, d), BF16), sds((8, d), F32),
                   sds((total // 128, WIDTH), F32), sds((total // TWO, WIDTH), F32)),
        in_specs=[ANY, whole(t, d), whole(t, d), wide(t), pl.BlockSpec((tile, d), lambda j: (cut(j), ZERO)), wide(d),
                  ANY, whole(ONE, d), ANY, ANY, ANY],
        out_specs=(pl.BlockSpec((n, d, WIDTH), lambda j: (j, ZERO, ZERO)), wide(ONE), ANY, ANY, ANY, ANY,
                   whole(8, d), whole(total // 128, WIDTH), ANY),
        scratch_shapes=[vm((t, d), F32), vm((t, d), BF16), vm((t, d), F32), vm((t, d), BF16), vm((d, t), BF16), dma((4,)), dma((4,))]
        + scatter_scratch(UNITS_A),
        compiler_params=host(collective_id, 63), name="up_backward",
    )(dr2, dr2b, h, gp, w_down, w_up, r1, gain, ctx_q, ctx_p, part_a)


def attn_bwd_body(scale, head, group, low_ref, wo_ref, qkv_ref, probs_ref, out_ref, dctx_ref, pause, enter=lambda: None):
    rows_here, d = low_ref.shape
    pair = TWO * head
    dctx_ref[:rows_here, :] = mm(low_ref[ALL], wo_ref[ALL], NT).astype(BF16)
    enter()
    pause(ZERO)

    def one(g):
        at, k_at, v_at = (pl.ds(pl.multiple_of(part * d + g * pair, pair), pair) for part in range(THREE))
        q = split_heads(qkv_ref[:, at], head)
        k = qkv_ref[:, k_at]
        v = qkv_ref[:, v_at]
        p = probs_ref[ZERO, g]
        dc = split_heads(dctx_ref[:rows_here, at], head)
        dp = mm(dc, v, NT)
        pf = p.astype(F32)
        ds = (pf * (dp - row_sum(dp * pf)) * scale).astype(BF16)
        out_ref[:, at] = join_heads(mm(ds, k), head).astype(BF16)
        out_ref[:, k_at] = mm(ds, q, TN).astype(BF16)
        out_ref[:, v_at] = mm(p, dc, TN).astype(BF16)

    def some(i, _):
        for h in range(group):
            one(i * group + h)
        return ZERO
    lax.fori_loop(ZERO, d // (pair * group), some, ZERO)
    pause(ONE)


def attn_qkv_kernel(axis, scale, head, nq, n_pass, lowq_ref, lowp_ref, wo_ref, qkvq_ref, qkvp_ref, probq_ref, probp_ref,
                    xq_ref, xp_ref, w_ref, dr1q_hbm, dr1p_hbm, b_ref, piecea_ref,
                    dw_ref, db_ref, dhq_ref, dhp_ref, pieceb_ref, part_ref, a_ref, dq_ref, dp_ref, accq_ref, accp_ref, dctx_ref, sem, gsem, *scratch):
    j = pl.program_id(ZERO)
    tile = w_ref.shape[ZERO]
    per = dq_ref.shape[TWO] // tile
    first, last = nq + n_pass, nq + n_pass + per - ONE
    pa, pb = ring_plan(axis, UNITS_A), ring_plan(axis, UNITS_B)
    points = TWO
    steps = [3.2] * nq + [3.3] * n_pass + [4.3] * per
    slots = [sum(steps[:i]) + steps[i] * h / points for i in range(len(steps)) for h in range(points)]
    timed = timeline(scatter_rounds(pb, b_ref, part_ref, pieceb_ref, *scratch), *PACE_B)
    timed += timeline(gather_rounds(pa, piecea_ref, a_ref, gsem), *PACE_A)
    plan = place(timed, slots)
    pause = functools.partial(run_slot, plan, j, points)
    loads = ((dr1q_hbm, accq_ref), (dr1p_hbm, accp_ref))

    @pl.when(j == ZERO)
    def _():
        signal_peers(pa.peers)
        for src, dst in loads:
            copy(src, dst, sem.at[ZERO])

    def enter():
        @pl.when(j == ZERO)
        def _():
            await_peers(pa.peers)

    @pl.when(j < nq)
    def _():
        attn_bwd_body(scale, head, ONE, lowq_ref, wo_ref, qkvq_ref, probq_ref, dq_ref.at[jnp.minimum(j, nq - ONE)], dctx_ref,
                      functools.partial(pause, (ZERO, nq)), enter)

    @pl.when((j >= nq) & (j < first))
    def _():
        attn_bwd_body(scale, head, TWO, lowp_ref, wo_ref, qkvp_ref, probp_ref, dp_ref.at[jnp.clip(j - nq, ZERO, n_pass - ONE)], dctx_ref,
                      functools.partial(pause, (nq, first)))

    @pl.when(j == first - ONE)
    def _():
        for src, dst in loads:
            drain(dst, sem.at[ZERO])

    @pl.when(j >= first)
    def _():
        pause((first, last + ONE), ZERO)
        at = pl.ds(pl.multiple_of(jnp.maximum(j - first, ZERO) * tile, tile), tile)
        dq = dq_ref[:, :, at].reshape(-ONE, tile)
        dp = dp_ref[:, :, at].reshape(-ONE, tile)
        store_blocks(dw_ref, mm(dq, xq_ref[ALL], TN) + mm(dp, xp_ref[ALL], TN))
        db_ref[ALL] = col_sum(dq.astype(F32)) + col_sum(dp.astype(F32))
        pause((first, last + ONE), ONE)
        accq_ref[ALL] += mm(dq, w_ref[ALL])
        accp_ref[ALL] += mm(dp, w_ref[ALL])

    @pl.when(j == last)
    def _():
        dhq_ref[ALL] = accq_ref[ALL].astype(BF16)
        dhp_ref[ALL] = accp_ref[ALL].astype(BF16)


def attn_qkv_backward(axis, low_q, low_p, w_out, qkv_q, qkv_p, probs_q, probs_p, xq, xp, w_t, dr1_q, dr1_p, part_b, piece_a, head,
                      collective_id, tile=TILE):
    f, d = w_t.shape
    nq, pairs, _, lq = probs_q.shape
    n_pass, _, _, lp = probs_p.shape
    tq, tp = nq * lq, n_pass * lp
    per, cols, total = f // tile, d // WIDTH, part_b.shape[ZERO]
    jq = lambda j: jnp.minimum(j, nq - ONE)
    jp = lambda j: jnp.clip(j - nq, ZERO, n_pass - ONE)
    jt = lambda j: jnp.clip(j - nq - n_pass, ZERO, per - ONE)
    rows_of = lambda n, c, at: pl.BlockSpec((n, c), lambda j: (at(j), ZERO))
    probs_of = lambda n, at: pl.BlockSpec((ONE, pairs, TWO * n, n), lambda j: (at(j), ZERO, ZERO, ZERO))
    return pl.pallas_call(
        functools.partial(attn_qkv_kernel, axis, head ** -0.5, head, nq, n_pass), grid=(nq + n_pass + per,),
        out_shape=(sds((cols, f, WIDTH), F32), sds((ONE, f), F32), sds((tq, d), BF16), sds((tp, d), BF16),
                   sds((total // 128, WIDTH), F32), sds((total // TWO, WIDTH), F32), sds((piece_a.shape[ZERO] * 128, WIDTH), F32)),
        in_specs=[rows_of(lq, d, jq), rows_of(lp, d, jp), whole(d, d), rows_of(lq, f, jq), rows_of(lp, f, jp),
                  probs_of(lq, jq), probs_of(lp, jp), whole(tq, d), whole(tp, d), rows_of(tile, d, jt), ANY, ANY, ANY, whole(*piece_a.shape)],
        out_specs=(pl.BlockSpec((cols, tile, WIDTH), lambda j: (ZERO, jt(j), ZERO)), pl.BlockSpec((ONE, tile), lambda j: (ZERO, jt(j))),
                   whole(tq, d), whole(tp, d), whole(total // 128, WIDTH), ANY, ANY),
        scratch_shapes=[pltpu.VMEM((nq, lq, f), BF16), pltpu.VMEM((n_pass, lp, f), BF16), pltpu.VMEM((tq, d), F32),
                        pltpu.VMEM((tp, d), F32), pltpu.VMEM((lp, d), BF16), pltpu.SemaphoreType.DMA((ONE,)),
                        pltpu.SemaphoreType.DMA((GATHER_SEMS,))]
        + scatter_scratch(UNITS_B),
        compiler_params=host(collective_id, 63), name="attn_qkv_backward",
    )(low_q, low_p, w_out, qkv_q, qkv_p, probs_q, probs_p, xq, xp, w_t, dr1_q, dr1_p, part_b, piece_a)


def unpack_kernel(a_hbm, sums_ref, down_ref, up_ref, out_ref, qkv_ref, stage, sem, in_sem, out_sem):
    def cols(i):
        return pl.ds(i * WIDTH, WIDTH)

    slots, rows_each, _ = stage.shape
    n, ff, f = up_ref.shape[ZERO], down_ref.shape[ZERO], qkv_ref.shape[ZERO]
    kept = sums_ref.shape[ZERO] - (up_ref.shape[ONE] + out_ref.shape[ONE]) // WIDTH * n - qkv_ref.shape[ONE] // WIDTH * f
    todo = [(kept + i * rows_each) for i in range((down_ref.shape[ONE] // WIDTH * ff - kept) // rows_each)]

    def load(i):
        copy(a_hbm.at[pl.ds(todo[i], rows_each)], stage.at[i % slots], in_sem.at[i % slots])

    for i in range(slots):
        load(i)
    at = ZERO
    for ref, size in ((up_ref, n), (out_ref, n), (qkv_ref, f), (down_ref, ff)):
        for i in range(ref.shape[ONE] // WIDTH):
            if at < sums_ref.shape[ZERO]:
                copy(sums_ref.at[pl.ds(at, size)], ref.at[:, cols(i)], sem.at[ZERO])
            at += size
    for i, row in enumerate(todo):
        slot = i % slots
        drain(stage.at[slot], in_sem.at[slot])
        copy(stage.at[slot], down_ref.at[pl.ds(row % ff, rows_each), cols(row // ff)], out_sem.at[slot])
        if i >= ONE and i - ONE + slots < len(todo):
            drain(stage.at[slot], out_sem.at[(i - ONE) % slots])
            load(i - ONE + slots)
    for i in range(max(len(todo) - slots, ZERO), len(todo)):
        drain(stage.at[ZERO], out_sem.at[i % slots])
    drain(sums_ref, sem.at[ZERO])


def unpack(a, sums, d, ff, f):
    slots = 4
    dma = pltpu.SemaphoreType.DMA
    return pl.pallas_call(
        unpack_kernel, out_shape=(sds((ff, d), F32), sds((d, ff), F32), sds((d, d), F32), sds((f, d), F32)),
        in_specs=[ANY, pl.BlockSpec(memory_space=pltpu.VMEM)], out_specs=(ANY,) * 4,
        scratch_shapes=[pltpu.VMEM((slots, TWO * TILE, WIDTH), F32), dma((ONE,)), dma((slots,)), dma((slots,))],
        compiler_params=vmem(8), name="unpack",
    )(a, pltpu.with_memory_space_constraint(sums, pltpu.VMEM))


def solution(mesh):
    axis = mesh.axis_names[ZERO]
    n_dev = mesh.shape[axis]

    def local_step(q_hidden, q_mask, p_hidden, p_mask, w_qkv, b_qkv, w_out, b_out, ln1_gain, ln1_shift,
                   w_up, b_up, w_down, b_down, ln2_gain, ln2_shift):
        nq, _, d = q_hidden.shape
        n_pass, p_len = nq * p_hidden.shape[ONE], p_hidden.shape[TWO]
        _, three, heads, head = w_qkv.shape
        xq, xp = q_hidden.reshape(-ONE, d), p_hidden.reshape(-ONE, d)
        p_mask = p_mask.reshape(n_pass, p_len)
        wqkv_t = w_qkv.transpose(ONE, TWO, THREE, ZERO).reshape(-ONE, d)
        wo = w_out.reshape(-ONE, d)
        vecs = [v.reshape(ONE, d) for v in (b_out, ln1_gain, ln1_shift, b_down, ln2_gain, ln2_shift)]

        qkv_q, qkv_p = qkv_project(xq, xp, wqkv_t, b_qkv.reshape(ONE, -ONE))
        probs_q, ctx_q = attention(qkv_q, q_mask, head)
        probs_p, ctx_p = attention(qkv_p, p_mask, head)
        h, r1, g, gp, r2, pooled = ffn_forward(
            xq, xp, ctx_q, ctx_p, wo, vecs, q_mask, p_mask, w_up, b_up.reshape(ONE, -ONE), w_down)
        everyone = gather_embeddings(pooled, axis, ONE)
        mean_loss, d_pooled = loss_and_grad(everyone, pooled, axis, nq * n_dev)
        dwd, dr2, dr2b, dvec2 = down_backward(d_pooled, r2, q_mask, p_mask, vecs[4], g)
        dwb, dbu, dr1_q, dr1_p, low_q, low_p, dvec1, piece_a, _ = up_backward(
            axis, dr2, dr2b, h, gp, w_down, w_up, r1, vecs[ONE], ctx_q, ctx_p, dwd.reshape(-ONE, WIDTH), TWO)
        dwq, dbq, dh_q, dh_p, piece_b, _, a = attn_qkv_backward(
            axis, low_q, low_p, wo, qkv_q, qkv_p, probs_q, probs_p, xq, xp, wqkv_t, dr1_q, dr1_p, dwb.reshape(-ONE, WIDTH), piece_a, head, THREE)
        sums, small = finish_sum(axis, UNITS_B, UNITS_C, piece_b, dwq.reshape(-ONE, WIDTH), a, THREE * w_down.shape[ZERO],
                                 dvec1, dvec2, dbq, dbu, 4)
        d_down, d_up, d_out, d_qkv = unpack(a, sums, d, w_down.shape[ZERO], three * d)
        vec, bias = small[:8], small[8:]
        return (mean_loss, dh_q.reshape(q_hidden.shape), dh_p.reshape(p_hidden.shape),
                d_qkv.reshape(three, heads, head, d).transpose(THREE, ZERO, ONE, TWO), bias[:three].reshape(b_qkv.shape),
                d_out.reshape(w_out.shape), vec[ZERO], vec[ONE], vec[TWO], d_up, bias[three:-ONE].reshape(-ONE),
                d_down, vec[THREE], vec[4], vec[5])

    in_specs = (P(axis),) * 4 + (P(),) * 12
    out_specs = (P(), P(axis), P(axis)) + (P(),) * 12
    return jax.shard_map(local_step, mesh=mesh, in_specs=in_specs, out_specs=out_specs, check_vma=False)
```

```python
import functools
import types
import jax
import jax.numpy as jnp
from jax import lax
from jax.experimental import pallas as pl
from jax.experimental.pallas import tpu as pltpu
from jax.sharding import PartitionSpec as P

ZERO, ONE, TWO, THREE, ALL = 0, 1, 2, 3, ...

F32 = jnp.float32
BF16 = jnp.bfloat16
LOGICAL = pl.DeviceIdType.LOGICAL
RING = 4
WIDTH = 256
COLOURS = range(6)
AXES = range(THREE)
RINGS = range(RING)
TURNS = range(RING * RING)
ANY = pl.BlockSpec(memory_space=pl.ANY)


def mesh_place(axis):
    me = lax.axis_index(axis)
    core = lax.rem(me, TWO)
    chip = lax.div(me, TWO)
    row = lax.div(chip, RING)
    return (lax.rem(chip, RING), lax.rem(row, RING), lax.div(row, RING)), core


def device_at(coords, core):
    return ((coords[TWO] * RING + coords[ONE]) * RING + coords[ZERO]) * TWO + core


def moved(coords, dim, by):
    out = list(coords)
    out[dim] = lax.rem(coords[dim] + by + TWO * RING, RING)
    return tuple(out)


def wrap(i):
    return lax.rem(i + 4 * RING, RING)


def rdma(src, dst, send, recv, to):
    pltpu.make_async_remote_copy(src_ref=src, dst_ref=dst, send_sem=send, recv_sem=recv,
                                 device_id=to, device_id_type=LOGICAL).start()


def copy(src, dst, sem):
    pltpu.make_async_copy(src, dst, sem).start()


def drain(ref, sem):
    pltpu.make_async_copy(ref, ref, sem).wait()


def carve(sems, *counts):
    out, at = [], ZERO
    for n in counts:
        out.append(lambda i, at=at: sems.at[at + i])
        at += n
    return out


def ring_plan(axis, units):
    coords, core = mesh_place(axis)
    p = types.SimpleNamespace(coords=coords, core=core, partner=device_at(coords, ONE - core))
    p.dims = [tuple((k // TWO + s) % THREE for s in AXES) for k in COLOURS]
    p.sign = [ONE - TWO * (k % TWO) for k in COLOURS]
    p.pos = [tuple(coords[d] for d in p.dims[k]) for k in COLOURS]
    p.nxt = [tuple(device_at(moved(coords, d, p.sign[k]), core) for d in p.dims[k]) for k in COLOURS]
    p.piece = [8 * u for u in units]
    p.lead = [sum(p.piece[:k]) for k in COLOURS]
    p.all = sum(p.piece)
    p.half = 64 * p.all
    p.base = core * p.half
    p.peers = [p.partner] + [device_at(moved(coords, d, by), core) for d in AXES for by in (ONE, THREE)]
    p.across = [device_at(moved(coords, d, TWO), core) for d in AXES]
    p.prv = [tuple(device_at(moved(coords, d, -p.sign[k]), core) for d in p.dims[k]) for k in COLOURS]
    return p


def rows(at, n):
    return pl.ds(pl.multiple_of(at, 8), n)


def place_of(p, k, ring, back):
    return wrap(p.pos[k][ring] - p.sign[k] * back)


def chunk_row(p, k, back):
    return 64 * p.lead[k] + place_of(p, k, ZERO, back) * (16 * p.piece[k])


def sub_row(p, k, row, back):
    return row + place_of(p, k, ONE, back) * (4 * p.piece[k])


def piece_row(p, k, row, back):
    return row + place_of(p, k, TWO, back) * p.piece[k]


GIVE = (TWO, ONE, THREE, ZERO)
TAKE = (ZERO, ONE, THREE, TWO)


def signal_peers(peers):
    barrier = pltpu.get_barrier_semaphore()
    for peer in peers:
        pl.semaphore_signal(barrier, inc=ONE, device_id=peer, device_id_type=LOGICAL)


def await_peers(peers):
    pl.semaphore_wait(pltpu.get_barrier_semaphore(), len(peers))


SCATTER_SEMS = 4 + THREE * 16 + TWO * 12 + 4 * THREE


def scatter_scratch(units):
    n = 8 * sum(units)
    vm = lambda *s: pltpu.VMEM(s + (WIDTH,), F32)
    return [vm(64 * n), vm(TWO, 4 * n), vm(THREE, RING, 4 * n), vm(THREE, 4 * n), vm(THREE, n), pltpu.SemaphoreType.DMA((SCATTER_SEMS,))]


def scatter_rounds(p, src, part, out, acc, stage, land1, land2, land3, sems):
    load_sem, swap_send, swap_recv, stage_sem, p1_send, p1_recv, p2_send, p2_recv, p3_send, p3_recv = carve(
        sems, 4, 16, 16, 16, 12, 12, THREE, THREE, THREE, THREE)
    n_sub, n_chunk = 4 * p.all, 16 * p.all
    far = p.half - p.base

    def turn_row(k, n):
        return sub_row(p, k, chunk_row(p, k, n // RING + ONE), GIVE[n % RING])

    def load(t):
        for k in COLOURS:
            r, m = chunk_row(p, k, t + ONE), 16 * p.piece[k]
            copy(src.at[rows(p.base + r, m)], acc.at[rows(r, m)], load_sem(t))

    def swap(n):
        for k in COLOURS:
            r, m = turn_row(k, n), 4 * p.piece[k]
            rdma(src.at[rows(far + r, m)], part.at[rows(r, m)], swap_send(n), swap_recv(n), p.partner)

    def fetch(n):
        drain(part.at[pl.ds(ZERO, n_sub)], swap_recv(n))
        for k in COLOURS:
            m = 4 * p.piece[k]
            copy(part.at[rows(turn_row(k, n), m)], stage.at[n % TWO, pl.ds(4 * p.lead[k], m)], stage_sem(n))

    def begin():
        for t in RINGS:
            load(t)
        for n in range(6):
            swap(n)

    def turn(n):
        t, i = n // RING, n % RING
        if n == ZERO:
            fetch(n)
        if n + 6 < 16:
            swap(n + 6)
        if n + ONE < 16:
            fetch(n + ONE)
        if i == ZERO:
            drain(acc.at[pl.ds(ZERO, n_chunk)], load_sem(t))
        drain(stage.at[n % TWO], stage_sem(n))
        if t > ZERO:
            drain(land1.at[t - ONE, i], p1_recv(n - 4))
        for k in COLOURS:
            at, m = rows(turn_row(k, n), 4 * p.piece[k]), pl.ds(4 * p.lead[k], 4 * p.piece[k])
            val = acc[at] + stage[n % TWO, m]
            acc[at] = val + land1[t - ONE, i, m] if t > ZERO else val
        if t < THREE:
            for k in COLOURS:
                at, m = rows(turn_row(k, n), 4 * p.piece[k]), pl.ds(4 * p.lead[k], 4 * p.piece[k])
                rdma(acc.at[at], land1.at[t, i, m], p1_send(n), p1_recv(n), p.nxt[k][ZERO])

    def pass_on(i, where, land, send, recv, ring):
        if i == TWO:
            drain(land.at[ZERO], recv(ZERO))
        for k in COLOURS:
            at, m = where(k, i)
            if i == TWO:
                acc[at] += land[ZERO, m]
        for k in COLOURS:
            at, m = where(k, i)
            rdma(acc.at[at], land.at[i, m], send(i), recv(i), (p.prv if i == ONE else p.nxt)[k][ring])

    def sub_at(k, i):
        return rows(turn_row(k, 12 + i), 4 * p.piece[k]), pl.ds(4 * p.lead[k], 4 * p.piece[k])

    def piece_at(k, i):
        return rows(piece_row(p, k, turn_row(k, 15), GIVE[i]), p.piece[k]), pl.ds(p.lead[k], p.piece[k])

    def second(i):
        pass_on(i, sub_at, land2, p2_send, p2_recv, ONE)

    def third():
        for i in (ONE, TWO):
            drain(land2.at[i], p2_recv(i))
        for k in COLOURS:
            at, m = sub_at(k, THREE)
            acc[at] += land2[ONE, m] + land2[TWO, m]
        for i in (ZERO, ONE):
            pass_on(i, piece_at, land3, p3_send, p3_recv, TWO)

    def fourth():
        pass_on(TWO, piece_at, land3, p3_send, p3_recv, TWO)

    def last():
        for i in (ONE, TWO):
            drain(land3.at[i], p3_recv(i))
        for k in COLOURS:
            at, m = piece_at(k, THREE)
            out[m] = acc[at] + (land3[ONE, m] + land3[TWO, m])

    def finish():
        for n in TURNS:
            drain(acc.at[pl.ds(ZERO, n_sub)], swap_send(n))
        for n in range(12):
            drain(acc.at[pl.ds(ZERO, n_sub)], p1_send(n))
        for t in AXES:
            drain(acc.at[pl.ds(ZERO, n_sub)], p2_send(t))
            drain(acc.at[pl.ds(ZERO, p.all)], p3_send(t))

    act = functools.partial
    def both(*fs):
        def run():
            for f in fs:
                f()
        return run
    steps = [begin] + [act(turn, n) for n in range(12)]
    steps += [both(act(turn, 12 + i), act(second, i)) for i in AXES] + [act(turn, 15), third, fourth, last, finish]
    return steps


GATHER_SEMS = ONE + TWO * (THREE + THREE + 12 + 16)


def gather_rounds(p, piece, out, sems):
    own_sem, a3_send, a3_recv, a2_send, a2_recv, a1_send, a1_recv, push_send, push_recv = carve(
        sems, ONE, THREE, THREE, THREE, THREE, 12, 12, 16, 16)
    n_sub = 4 * p.all

    def many(n):
        return out.at[pl.ds(ZERO, n)]

    def sub_at(k, c, s):
        return rows(p.base + sub_row(p, k, chunk_row(p, k, c), TAKE[s]), 4 * p.piece[k])

    def piece_at(k, g):
        return rows(p.base + piece_row(p, k, sub_row(p, k, chunk_row(p, k, ZERO), ZERO), TAKE[g]), p.piece[k])

    def both_ways(at, send, recv, ring, srcs=out):
        for k in COLOURS:
            src = out.at[at(k)] if srcs is out else srcs.at[pl.ds(p.lead[k], p.piece[k])]
            rdma(src, out.at[at(k)], send(ZERO), recv(ZERO), p.nxt[k][ring])
            rdma(src, out.at[at(k)], send(ONE), recv(ONE), p.prv[k][ring])

    def forward(at, send, recv, ring):
        for k in COLOURS:
            rdma(out.at[at(k)], out.at[at(k)], send(TWO), recv(TWO), p.nxt[k][ring])

    def third():
        for k in COLOURS:
            copy(piece.at[pl.ds(p.lead[k], p.piece[k])], out.at[piece_at(k, ZERO)], own_sem(ZERO))
        both_ways(lambda k: piece_at(k, ZERO), a3_send, a3_recv, TWO, piece)

    def fourth():
        drain(many(p.all), a3_recv(ZERO))
        forward(lambda k: piece_at(k, ONE), a3_send, a3_recv, TWO)

    def hop1(c, s):
        for k in COLOURS:
            if c < THREE:
                rdma(out.at[sub_at(k, c, s)], out.at[sub_at(k, c, s)], a1_send(RING * c + s), a1_recv(RING * c + s), p.nxt[k][ZERO])
            rdma(out.at[sub_at(k, c, s)], out.at[sub_at(k, c, s)], push_send(RING * c + s), push_recv(RING * c + s), p.partner)

    def second(s):
        if s == ZERO:
            for sem in (own_sem(ZERO), a3_recv(ONE), a3_recv(TWO)):
                drain(many(p.all), sem)
            both_ways(lambda k: sub_at(k, ZERO, ZERO), a2_send, a2_recv, ONE)
        else:
            drain(many(n_sub), a2_recv(s - ONE))
        if s == ONE:
            forward(lambda k: sub_at(k, ZERO, ONE), a2_send, a2_recv, ONE)
        hop1(ZERO, s)

    def first(c, s):
        drain(many(n_sub), a1_recv(RING * (c - ONE) + s))
        hop1(c, s)

    def finish():
        for t in AXES:
            drain(many(p.all), a3_send(t))
            drain(many(n_sub), a2_send(t))
        for n in range(12):
            drain(many(n_sub), a1_send(n))
        for n in TURNS:
            drain(many(n_sub), push_send(n))
            drain(many(n_sub), push_recv(n))

    act = functools.partial
    return ([third, fourth] + [act(second, s) for s in RINGS]
            + [act(first, c, s) for c in (ONE, TWO, THREE) for s in RINGS] + [finish])


def small_scratch(shape):
    return [pltpu.VMEM((4, THREE) + shape, F32), pltpu.SemaphoreType.DMA((8,))]


def small_rounds(p, src, out, land, sems):
    places = [(None, p.core, TWO)] + [(d, p.coords[d], RING) for d in AXES]

    def send(n):
        d, _, size = places[n]
        for by in range(ONE, size):
            to = p.partner if d is None else device_at(moved(p.coords, d, by), p.core)
            rdma(out, land.at[n, by - ONE], sems.at[n], sems.at[4 + n], to)

    def step(n):
        if n == ZERO:
            out[ALL] = src[ALL]
        else:
            _, place, size = places[n - ONE]
            got = land.at[n - ONE, pl.ds(ZERO, size - ONE)]
            drain(got, sems.at[4 + n - ONE])
            drain(got, sems.at[n - ONE])
            mine, total = out[ALL], None
            for q in range(size):
                val = mine
                for by in range(ONE, size):
                    val = jnp.where(lax.rem(place - q + size, size) == by, land[n - ONE, by - ONE], val)
                total = val if total is None else total + val
            out[ALL] = total
        if n < 4:
            send(n)

    return [functools.partial(step, n) for n in range(5)]


def spread(steps, slots):
    plan = [[] for _ in range(slots)]
    for i, s in enumerate(steps):
        plan[i * slots // len(steps)].append(s)
    return plan


def finish_kernel(axis, units_b, units_c, pieceb_ref, c_ref, a_ref, vec1_ref, vec2_ref, bq_ref, bu_ref, bc_out, small_out, part,
                  small_ref, piecec, a_sem, *scratch):
    sc, (gather_sem, gather_sem2, small_land, small_sem) = scratch[:6], scratch[6:]
    pb, pc = ring_plan(axis, units_b), ring_plan(axis, units_c)
    n_b, n_c = TWO * pb.half, TWO * pc.half
    b_out, c_out = bc_out.at[pl.ds(ZERO, n_b)], bc_out.at[pl.ds(n_b, n_c)]
    a_here = bc_out.at[pl.ds(n_b + n_c, bc_out.shape[ZERO] - n_b - n_c)]
    peers = pb.peers + pb.across
    signal_peers(peers)
    width = small_ref.shape[ONE]
    small_ref[ALL] = jnp.zeros_like(small_ref)
    small_ref[ZERO:THREE, :] = vec1_ref[ZERO:THREE, :]
    small_ref[THREE:6, :] = vec2_ref[ZERO:THREE, :]
    at = 8
    for ref in (bq_ref, bu_ref):
        for i in range(ref.shape[ONE] // width):
            small_ref[at:at + ONE, :] = ref[:, i * width:(i + ONE) * width]
            at += ONE
    await_peers(peers)
    reduce_c = scatter_rounds(pc, c_ref, part, piecec, *sc)
    gather_b = gather_rounds(pb, pieceb_ref, b_out, gather_sem)
    gather_c = gather_rounds(pc, piecec, c_out, gather_sem2)
    smalls = small_rounds(pb, small_ref, small_out, small_land, small_sem)
    main = reduce_c[:-ONE] + gather_c[:-ONE]
    fill = spread(gather_b[:-ONE], len(main) - 4)
    for i, f in enumerate(main):
        f()
        if i == 16:
            copy(a_ref.at[pl.ds(ZERO, a_here.shape[ZERO])], a_here, a_sem.at[ZERO])
        if i % THREE == ONE and i // THREE < len(smalls):
            smalls[i // THREE]()
        for f in fill[i] if i < len(fill) else ():
            f()
    for rounds in (reduce_c, gather_b, gather_c):
        rounds[-ONE]()
    drain(a_here, a_sem.at[ZERO])


def finish_sum(axis, units_b, units_c, piece_b, c, a, keep, vec1, vec2, bq, bu, collective_id):
    sds = jax.ShapeDtypeStruct
    dma = pltpu.SemaphoreType.DMA
    vm = pl.BlockSpec(memory_space=pltpu.VMEM)
    n = c.shape[ZERO]
    small = (16, vec1.shape[ONE])
    outs = pl.pallas_call(
        functools.partial(finish_kernel, axis, units_b, units_c),
        out_shape=(pltpu.VMEM((piece_b.shape[ZERO] * 128 + n + keep, WIDTH), F32), sds(small, F32), sds((n // TWO, WIDTH), F32)),
        in_specs=[vm, ANY, ANY, vm, vm, vm, vm], out_specs=(vm, vm, ANY),
        scratch_shapes=[pltpu.VMEM(small, F32), pltpu.VMEM((n // 128, WIDTH), F32), dma((ONE,))] + scatter_scratch(units_c)
        + [dma((GATHER_SEMS,)), dma((GATHER_SEMS,))] + small_scratch(small),
        compiler_params=pltpu.CompilerParams(collective_id=collective_id, has_side_effects=True, vmem_limit_bytes=17 * 1024 * 1024),
        name="finish_sum",
    )(piece_b, c, a, vec1, vec2, bq, bu)
    return outs[:TWO]


def gather_kernel(axis, pooled_ref, g_ref, e_ref, mine, theirs, swap_sem, sems_send, sems_recv, push_send, push_recv):
    coords, core = mesh_place(axis)
    partner = device_at(coords, ONE - core)
    width = e_ref.shape[ONE]
    lanes = pl.ds(pl.multiple_of(core * (width // TWO), 128), width // TWO)
    x, y, z = coords
    peers = [partner] + [device_at(moved(coords, d, by), core) for d in AXES for by in (ONE, TWO, THREE)]
    signal_peers(peers)
    size = row_sum(pooled_ref[ALL] * pooled_ref[ALL])
    e_ref[ALL] = pooled_ref[ALL] * jnp.where(size > 0.0, lax.rsqrt(size), 0.0)
    mine[ALL] = e_ref[ALL]
    await_peers(peers)

    rdma(e_ref, theirs, swap_sem.at[ZERO], swap_sem.at[ONE], partner)
    drain(theirs, swap_sem.at[ONE])
    first = jnp.where(core == ZERO, mine[:, lanes], theirs[:, lanes])
    second = jnp.where(core == ZERO, theirs[:, lanes], mine[:, lanes])
    g_ref[z, y, x, ZERO:4, lanes] = first[ZERO:4]
    g_ref[z, y, x, 4:8, lanes] = second[ZERO:4]
    g_ref[z, y, x, 8:16, lanes] = first[8:16]
    g_ref[z, y, x, 16:24, lanes] = second[8:16]
    drain(e_ref, swap_sem.at[ZERO])

    def view(a, stage):
        idx = [z, y, x]
        for s in range(stage):
            idx[TWO - (a + s) % THREE] = slice(None)
        return g_ref.at[idx[ZERO], idx[ONE], idx[TWO], pl.ds(8 * a, 8), lanes]

    for stage in range(THREE):
        for by in (ONE, THREE, TWO):
            for a in range(THREE):
                to = device_at(moved(coords, (a + stage) % THREE, by), core)
                rdma(view(a, stage), view(a, stage), sems_send.at[stage, by - ONE], sems_recv.at[stage, by - ONE], to)
        if stage == TWO:
            for a in range(THREE):
                rdma(view(a, TWO), view(a, TWO), push_send.at[ZERO], push_recv.at[ZERO], partner)
        for by in (ONE, THREE, TWO):
            n = 4 ** stage
            shape_like = g_ref.at[ZERO, ZERO, ZERO, :, lanes] if stage == ZERO else (
                g_ref.at[ZERO, ZERO, :, :, lanes] if stage == ONE else g_ref.at[ZERO, :, :, :, lanes])
            drain(shape_like, sems_recv.at[stage, by - ONE])
            if stage == TWO:
                for a in range(THREE):
                    far = moved(coords, (a + TWO) % THREE, RING - by)
                    idx = [far[TWO], far[ONE], far[ZERO]]
                    idx[TWO - a] = slice(None)
                    idx[TWO - (a + ONE) % THREE] = slice(None)
                    v = g_ref.at[idx[ZERO], idx[ONE], idx[TWO], pl.ds(8 * a, 8), lanes]
                    rdma(v, v, push_send.at[by], push_recv.at[by], partner)
    for stage in range(THREE):
        shape_like = g_ref.at[ZERO, ZERO, ZERO, :, lanes] if stage == ZERO else (
            g_ref.at[ZERO, ZERO, :, :, lanes] if stage == ONE else g_ref.at[ZERO, :, :, :, lanes])
        for by in (ONE, TWO, THREE):
            drain(shape_like, sems_send.at[stage, by - ONE])
    for by in range(4):
        drain(g_ref.at[ZERO, :, :, :, lanes], push_send.at[by])
        drain(g_ref.at[ZERO, :, :, :, lanes], push_recv.at[by])


def gather_embeddings(e, axis, collective_id):
    dma = pltpu.SemaphoreType.DMA
    width = e.shape[ONE]
    g = pl.pallas_call(
        functools.partial(gather_kernel, axis),
        out_shape=jax.ShapeDtypeStruct((RING, RING, RING, 24, width), F32),
        in_specs=[pl.BlockSpec(memory_space=pltpu.VMEM)],
        out_specs=pl.BlockSpec(memory_space=pltpu.VMEM),
        scratch_shapes=[pltpu.VMEM(e.shape, F32)] * THREE + [dma((TWO,)),
                        dma((THREE, THREE)), dma((THREE, THREE)), dma((4,)), dma((4,))],
        compiler_params=pltpu.CompilerParams(collective_id=collective_id, has_side_effects=True,
                                             vmem_limit_bytes=16 * 1024 * 1024),
        name="gather_embeddings",
    )(e)
    return g.reshape(RING ** THREE, 24, width)


def split3(x):
    hi = x.astype(BF16)
    rest = x - hi.astype(F32)
    mid = rest.astype(BF16)
    return hi, mid, (rest - mid.astype(F32)).astype(BF16)


def dot6(a, b, dims):
    low = mm(a[TWO], b[ZERO], dims) + mm(a[ZERO], b[TWO], dims) + mm(a[ONE], b[ONE], dims)
    return mm(a[ZERO], b[ZERO], dims) + (mm(a[ZERO], b[ONE], dims) + mm(a[ONE], b[ZERO], dims) + low)


def loss_kernel(axis, n_query, g_ref, pooled_ref, loss_ref, d_ref, logit_ref, lse_ref, q_ref, p_ref, dp_ref):
    me = lax.axis_index(axis)
    core, chip = lax.rem(me, TWO), lax.div(me, TWO)
    chips, _, width = g_ref.shape
    nq = chips * 8
    lanes = 128
    gs = 100.0 / n_query
    for i, part in enumerate(split3(g_ref[:, ZERO:8, :].reshape(nq, width))):
        q_ref[i] = part
    block = TWO * lanes

    def logits(b, _):
        at = pl.multiple_of(b * block, block)
        p = split3(g_ref[pl.ds(b * (block // 16), block // 16), 8:24, :].reshape(block, width))
        for i, part in enumerate(p):
            p_ref[i, pl.ds(at, block), :] = part
        logit_ref[:, pl.ds(at, block)] = dot6((q_ref[ZERO], q_ref[ONE], q_ref[TWO]), p, NT) * 100.0
        return ZERO

    lax.fori_loop(ZERO, chips * 16 // block, logits, ZERO)

    def rows_of(b, loss):
        at = pl.ds(pl.multiple_of(b * lanes, lanes), lanes)
        s = logit_ref[at, :]
        top = jnp.max(s, axis=ONE, keepdims=True)
        lse = jnp.log(row_sum(jnp.exp(s - top))) + top
        lse_ref[at, :] = jnp.broadcast_to(lse, (lanes, lanes))
        row = lax.broadcasted_iota(jnp.int32, s.shape, ZERO) + b * lanes
        col = lax.broadcasted_iota(jnp.int32, s.shape, ONE)
        return loss + col_sum(lse - row_sum(jnp.where(col == TWO * row, s, 0.0)))

    loss = lax.fori_loop(ZERO, nq // lanes, rows_of, jnp.zeros((ONE, ONE), F32))
    loss_ref[ALL] = jnp.broadcast_to(loss * (1.0 / n_query), loss_ref.shape)

    def weights(s, lse, row, col):
        row = lax.broadcasted_iota(jnp.int32, s.shape, ZERO) + row
        col = lax.broadcasted_iota(jnp.int32, s.shape, ONE) + col
        return jnp.exp(s - lse) * gs - jnp.where(col == TWO * row, gs, 0.0)

    at = pl.ds(pl.multiple_of(chip * 8, 8), 8)
    w = jnp.concatenate([x.astype(F32) for x in split3(weights(logit_ref[at, :], lse_ref[at, ZERO:ONE], chip * 8, ZERO))], axis=ZERO).astype(BF16)
    by_hi, by_mid, by_low = (mm(w, p_ref[i]) for i in range(THREE))
    dq = by_hi[ZERO:8] + (by_hi[8:16] + by_mid[ZERO:8] + (by_hi[16:24] + by_mid[8:16] + by_low[ZERO:8]))

    first = pl.multiple_of(lax.div(chip, 8) * lanes, lanes)
    w = weights(logit_ref[:, pl.ds(first, lanes)], lse_ref[ALL], ZERO, first)
    dp_ref[ALL] = dot6(split3(w.T), (q_ref[ZERO], q_ref[ONE], q_ref[TWO]), NN)
    dp = dp_ref[pl.ds(pl.multiple_of(lax.rem(chip, 8) * 16 + core * 8, 8), 8), :]

    def back(d, pooled):
        inv = lax.rsqrt(row_sum(pooled * pooled))
        e = pooled * inv
        return (d - e * row_sum(e * d)) * inv

    d_ref[ALL] = jnp.zeros_like(d_ref)
    d_ref[ZERO:4, :] = back(jnp.where(core == ZERO, dq[ZERO:4], dq[4:8]), pooled_ref[ZERO:4])
    d_ref[8:16, :] = back(dp, pooled_ref[8:16])


def loss_and_grad(g, pooled, axis, n_query):
    chips, _, width = g.shape
    nq, n_pass, lanes = chips * 8, chips * 16, 128
    vm = pl.BlockSpec(memory_space=pltpu.VMEM)
    loss, d = pl.pallas_call(
        functools.partial(loss_kernel, axis, n_query),
        out_shape=(jax.ShapeDtypeStruct((8, lanes), F32), jax.ShapeDtypeStruct(pooled.shape, F32)),
        in_specs=[vm] * TWO, out_specs=(vm,) * TWO,
        scratch_shapes=[pltpu.VMEM((nq, n_pass), F32), pltpu.VMEM((nq, lanes), F32), pltpu.VMEM((THREE, nq, width), BF16),
                        pltpu.VMEM((THREE, n_pass, width), BF16), pltpu.VMEM((lanes, width), F32)],
        compiler_params=vmem(28), name="loss_and_grad",
    )(g, pooled)
    return loss[ZERO, ZERO], d


NN = (((ONE,), (ZERO,)), ((), ()))
NT = (((ONE,), (ONE,)), ((), ()))
TN = (((ZERO,), (ZERO,)), ((), ()))
LN_EPS = 1e-12
NEG_FILL = -1e9
TILE = 512
UNITS_A, UNITS_B, UNITS_C = (THREE, THREE, THREE, THREE, TWO, TWO), (THREE, THREE, THREE, THREE, 4, 4), (TWO,) * 6
sds = jax.ShapeDtypeStruct


def mm(a, b, dims=NN):
    return lax.dot_general(a, b, dims, preferred_element_type=F32)


def vmem(mb=60):
    return pltpu.CompilerParams(vmem_limit_bytes=mb * 1024 * 1024)


def whole(*shape):
    return pl.BlockSpec(shape, lambda j: (ZERO,) * len(shape), pipeline_mode=pl.Buffered(ONE))


def across(rows, tile):
    return pl.BlockSpec((rows, tile), lambda j: (ZERO, j))


def down(tile, cols):
    return pl.BlockSpec((tile, cols), lambda j: (j, ZERO))


def row_mean(x):
    return jnp.mean(x, axis=ONE, keepdims=True)


def row_sum(x):
    return jnp.sum(x, axis=ONE, keepdims=True)


def col_sum(x):
    return jnp.sum(x, axis=ZERO, keepdims=True)


def qkv_kernel(xq_ref, xp_ref, w_ref, b_ref, oq_ref, op_ref, x_ref):
    tq = xq_ref.shape[ZERO]

    @pl.when(pl.program_id(ZERO) == ZERO)
    def _():
        x_ref[:tq, :] = xq_ref[ALL]
        x_ref[tq:, :] = xp_ref[ALL]
    y = (mm(x_ref[ALL], w_ref[ALL], NT) + b_ref[ALL]).astype(BF16)
    oq_ref[ALL] = y[:tq]
    op_ref[ALL] = y[tq:]


def qkv_project(xq, xp, w_t, b, tile=TILE):
    tq, d = xq.shape
    tp, f = xp.shape[ZERO], w_t.shape[ZERO]
    return pl.pallas_call(
        qkv_kernel, grid=(f // tile,),
        out_shape=(sds((tq, f), BF16), sds((tp, f), BF16)),
        in_specs=[whole(tq, d), whole(tp, d), down(tile, d), across(ONE, tile)],
        out_specs=(across(tq, tile), across(tp, tile)),
        scratch_shapes=[pltpu.VMEM((tq + tp, d), BF16)],
        compiler_params=vmem(), name="qkv_project",
    )(xq, xp, w_t, b)


def split_heads(pair, head):
    lane = lax.broadcasted_iota(jnp.int32, pair.shape, ONE)
    zero = jnp.zeros_like(pair)
    return jnp.concatenate([jnp.where(lane < head, pair, zero), jnp.where(lane >= head, pair, zero)], axis=ZERO)


def join_heads(stacked, head):
    t = stacked.shape[ZERO] // TWO
    lane = lax.broadcasted_iota(jnp.int32, (t, stacked.shape[ONE]), ONE)
    return jnp.where(lane < head, stacked[:t], stacked[t:])


def attn_kernel(scale, head, qkv_ref, mask_ref, probs_ref, ctx_ref):
    d = ctx_ref.shape[ONE]
    pair = TWO * head
    keep = mask_ref[ZERO] > ZERO
    for g in range(d // pair):
        at = pl.ds(g * pair, pair)
        q = split_heads(qkv_ref[:, at], head)
        k = qkv_ref[:, pl.ds(d + g * pair, pair)]
        v = qkv_ref[:, pl.ds(TWO * d + g * pair, pair)]
        s = jnp.where(keep, mm(q, k, NT) * scale, NEG_FILL)
        e = jnp.exp(s - jnp.max(s, axis=ONE, keepdims=True))
        p = (e / row_sum(e)).astype(BF16)
        probs_ref[ZERO, g] = p
        ctx_ref[:, at] = join_heads(mm(p, v), head).astype(BF16)


def attention(qkv, mask, head):
    n, seq = mask.shape
    d = qkv.shape[ONE] // THREE
    pairs = d // (TWO * head)
    return pl.pallas_call(
        functools.partial(attn_kernel, head ** -0.5, head), grid=(n,),
        out_shape=(sds((n, pairs, TWO * seq, seq), BF16), sds((n * seq, d), BF16)),
        in_specs=[down(seq, THREE * d), pl.BlockSpec((ONE, ONE, seq), lambda j: (j, ZERO, ZERO))],
        out_specs=(pl.BlockSpec((ONE, pairs, TWO * seq, seq), lambda j: (j, ZERO, ZERO, ZERO)), down(seq, d)),
        compiler_params=vmem(), name="attention",
    )(qkv, mask.reshape(n, ONE, seq))


def norm_rows(x):
    c = x - row_mean(x)
    r = lax.rsqrt(row_mean(c * c) + LN_EPS)
    return c * r, r


def norm_back(g, hat, r):
    return r * (g - row_mean(g) - hat * row_mean(g * hat))


ERFC = (0.07122347, -0.27794802, 0.29668747, -0.02018065, 0.21581222, 0.21731356, 0.24887118, 0.24822095)


def gelu_parts(u):
    bell = jnp.exp2(u * u * -0.7213475204)
    t = 1.0 / (1.0 + 0.311126984 * jnp.abs(u))
    poly = 0.5 * ERFC[ZERO]
    for c in ERFC[ONE:]:
        poly = poly * t + 0.5 * c
    tail = bell * (poly * t)
    return jnp.where(u >= 0.0, 1.0 - tail, tail), u * bell * 0.3989422804


def each_sequence(mq_ref, mp_ref, act):
    for first, lo, ref in ((ZERO, ZERO, mq_ref), (8, mq_ref.shape[ZERO] * mq_ref.shape[ONE], mp_ref)):
        n, seq = ref.shape

        def one(i, _):
            size = row_sum(ref[pl.ds(i, ONE), :].astype(F32))
            token = lax.broadcasted_iota(jnp.int32, (seq, ONE), ZERO).astype(F32)
            act(first + i, pl.ds(pl.multiple_of(lo + i * seq, 16), seq), jnp.where(token < size, 1.0 / size, 0.0))
            return ZERO
        lax.fori_loop(ZERO, n, one, ZERO)


def each_block(lo, hi, act, size=304):
    def one(i, _):
        act(pl.ds(pl.multiple_of(lo + i * size, 16), size))
        return ZERO
    lax.fori_loop(ZERO, (hi - lo) // size, one, ZERO)


def ffn_kernel(xq_ref, xp_ref, cq_ref, cp_ref, wo_ref, bo_ref, g1_ref, s1_ref, bd_ref, g2_ref, s2_ref, mq_ref, mp_ref,
               wu_ref, bu_ref, wd_ref, h_hbm, r1_hbm, g_ref, gp_ref, r2_hbm, pool_ref, h_ref, r1_ref, r2_ref, sems):
    j = pl.program_id(ZERO)
    t, tq = h_ref.shape[ZERO], cq_ref.shape[ZERO]
    saved = ((h_ref, h_hbm), (r1_ref, r1_hbm), (r2_ref, r2_hbm))

    @pl.when(j == ZERO)
    def _():
        for x_ref, c_ref, lo, size in ((xq_ref, cq_ref, ZERO, tq), (xp_ref, cp_ref, tq, 128)):
            def block(at):
                to = pl.ds(pl.multiple_of(lo + at.start, 16), size)
                r1 = x_ref[at, :].astype(F32) + mm(c_ref[at, :], wo_ref[ALL]) + bo_ref[ALL]
                r1_ref[to, :] = r1
                h = (norm_rows(r1)[ZERO] * g1_ref[ALL] + s1_ref[ALL]).astype(BF16)
                h_ref[to, :] = h
                r2_ref[to, :] = h.astype(F32) + bd_ref[ALL]
            each_block(ZERO, c_ref.shape[ZERO], block, size)
        for i in range(TWO):
            copy(*saved[i], sems.at[i])

    def block(at):
        u = mm(h_ref[at, :], wu_ref[ALL]) + bu_ref[ALL]
        cdf, upd = gelu_parts(u)
        g = (u * cdf).astype(BF16)
        g_ref[at, :] = g
        gp_ref[at, :] = cdf + upd
        r2_ref[at, :] += mm(g, wd_ref[ALL])
    each_block(ZERO, t, block)

    @pl.when(j == pl.num_programs(ZERO) - ONE)
    def _():
        copy(*saved[TWO], sems.at[TWO])
        pool_ref[ALL] = jnp.zeros_like(pool_ref)

        def pool(row, at, weight):
            y = norm_rows(r2_ref[at, :])[ZERO] * g2_ref[ALL] + s2_ref[ALL]
            pool_ref[pl.ds(row, ONE), :] = col_sum(y * weight)
        each_sequence(mq_ref, mp_ref, pool)
        for i in range(THREE):
            drain(saved[i][ZERO], sems.at[i])


def ffn_forward(xq, xp, ctx_q, ctx_p, w_out, vecs, mask_q, mask_p, w_up, b_up, w_down, tile=TWO * TILE):
    tq, d = xq.shape
    tp, f = xp.shape[ZERO], w_up.shape[ONE]
    t = tq + tp
    return pl.pallas_call(
        ffn_kernel, grid=(f // tile,),
        out_shape=(sds((t, d), BF16), sds((t, d), F32), sds((t, f), BF16), sds((t, f), F32), sds((t, d), F32), sds((16, d), F32)),
        in_specs=[whole(tq, d), whole(tp, d), whole(tq, d), whole(tp, d), whole(d, d), *(whole(ONE, d) for _ in vecs),
                  whole(*mask_q.shape), whole(*mask_p.shape), across(d, tile), across(ONE, tile), down(tile, d)],
        out_specs=(ANY, ANY, across(t, tile), across(t, tile), ANY, whole(16, d)),
        scratch_shapes=[pltpu.VMEM((t, d), BF16), pltpu.VMEM((t, d), F32), pltpu.VMEM((t, d), F32), pltpu.SemaphoreType.DMA((THREE,))],
        compiler_params=vmem(), name="ffn_forward",
    )(xq, xp, ctx_q, ctx_p, w_out, *vecs, mask_q, mask_p, w_up, b_up, w_down)


def store_blocks(ref, val):
    for c in range(ref.shape[ZERO]):
        ref[c] = val[:, c * WIDTH:(c + ONE) * WIDTH]


def down_bwd_kernel(dpool_ref, r2_ref, mq_ref, mp_ref, g2_ref, g_ref, dwd_ref, dr2_hbm, dr2b_hbm, dvec_ref, dr2_ref, dr2b_ref, sems):
    j = pl.program_id(ZERO)
    saved = ((dr2_ref, dr2_hbm), (dr2b_ref, dr2b_hbm))

    @pl.when(j == ZERO)
    def _():
        dvec_ref[ALL] = jnp.zeros_like(dvec_ref)

        def one(row, at, weight):
            hat, r = norm_rows(r2_ref[at, :])
            dy = weight * dpool_ref[pl.ds(row, ONE), :]
            dr2 = norm_back(dy * g2_ref[ALL], hat, r)
            dr2_ref[at, :] = dr2
            dr2b_ref[at, :] = dr2.astype(BF16)
            dvec_ref[ZERO:ONE, :] += col_sum(dr2)
            dvec_ref[ONE:TWO, :] += col_sum(dy * hat)
            dvec_ref[TWO:THREE, :] += col_sum(dy)
        each_sequence(mq_ref, mp_ref, one)
        for i in range(TWO):
            copy(*saved[i], sems.at[i])

    store_blocks(dwd_ref, mm(g_ref[ALL], dr2b_ref[ALL], TN))

    @pl.when(j == pl.num_programs(ZERO) - ONE)
    def _():
        for i in range(TWO):
            drain(saved[i][ZERO], sems.at[i])


def down_backward(dpool, r2, mask_q, mask_p, gain, g, tile=TWO * TILE):
    t, d = r2.shape
    f = g.shape[ONE]
    n = d // WIDTH
    return pl.pallas_call(
        down_bwd_kernel, grid=(f // tile,),
        out_shape=(sds((n, f, WIDTH), F32), sds((t, d), F32), sds((t, d), BF16), sds((8, d), F32)),
        in_specs=[whole(*dpool.shape), whole(t, d), whole(*mask_q.shape), whole(*mask_p.shape), whole(ONE, d), across(t, tile)],
        out_specs=(pl.BlockSpec((n, tile, WIDTH), lambda j: (ZERO, j, ZERO)), ANY, ANY, whole(8, d)),
        scratch_shapes=[pltpu.VMEM((t, d), F32), pltpu.VMEM((t, d), BF16), pltpu.SemaphoreType.DMA((TWO,))],
        compiler_params=vmem(), name="down_backward",
    )(dpool, r2, mask_q, mask_p, gain, g)


PACE_UP = (3.0, 2.5, 6.0, 4.0)
PACE_B = (4.5, 2.8, 5.5, 4.5)
PACE_A = (9.0, 3.2, 0.0, 0.0)
def place(timed, slot_times):
    plan = [[] for _ in slot_times]
    for t, f in sorted(timed, key=lambda x: x[ZERO]):
        plan[min([i for i, at in enumerate(slot_times) if at >= t], default=-ONE)].append(f)
    return plan


def timeline(steps, start, pace, before_third, before_last):
    n = len(steps)
    times = [0.0] + [start + pace * i for i in range(n - TWO)] + [1e3]
    if before_last:
        times[-4] = times[-5] + before_third
        times[-THREE] = times[-4] + before_last
        times[-TWO] = times[-THREE] + before_last
    return list(zip(times, steps))


def run_slot(plan, j, per, steps, point):
    for s in range(*steps):
        todo = plan[s * per + point]
        if todo:
            @pl.when(j == s)
            def _():
                for f in todo:
                    f()


def host(collective_id, mb):
    return pltpu.CompilerParams(collective_id=collective_id, has_side_effects=True, vmem_limit_bytes=mb * 1024 * 1024)


def up_bwd_kernel(axis, steps, dr2_hbm, dr2b_ref, h_ref, gp_ref, wd_ref, wu_ref, r1_hbm, g1_ref, cq_hbm, cp_hbm, a_ref,
                  dw_ref, dbu_ref, dr1q_hbm, dr1p_hbm, lowq_hbm, lowp_hbm, dvec_ref, piece_ref, part_ref,
                  dr1_ref, low_ref, r1_ref, ctx_ref, ht_ref, in_sem, out_sem, *scratch):
    j = pl.program_id(ZERO)
    t, tq, tp = dr1_ref.shape[ZERO], dr1q_hbm.shape[ZERO], dr1p_hbm.shape[ZERO]
    p = ring_plan(axis, UNITS_A)
    pace = 5.6
    timed = timeline(scatter_rounds(p, a_ref, part_ref, piece_ref, *scratch), *PACE_UP)
    points = THREE
    plan = place(timed, [pace * (s // points) + pace * (s % points) / points for s in range(points * (steps + TWO))])
    pause = functools.partial(run_slot, plan, j, points)
    q_rows, p_rows = pl.ds(ZERO, tq), pl.ds(tq, tp)
    late = ((r1_hbm, r1_ref), (cq_hbm, ctx_ref.at[q_rows]), (cp_hbm, ctx_ref.at[p_rows]))
    results = ((dr1_ref.at[q_rows], dr1q_hbm), (dr1_ref.at[p_rows], dr1p_hbm), (low_ref.at[q_rows], lowq_hbm), (low_ref.at[p_rows], lowp_hbm))

    @pl.when(j == ZERO)
    def _():
        signal_peers(p.peers)
        copy(dr2_hbm, dr1_ref, in_sem.at[ZERO])
        ht_ref[ALL] = h_ref[ALL].T
        drain(dr1_ref, in_sem.at[ZERO])
        for i in range(THREE):
            copy(*late[i], in_sem.at[ONE + i])

    @pl.when(j < steps)
    def _():
        dg = mm(dr2b_ref[ALL], wd_ref[ALL], NT).astype(BF16).astype(F32)
        dpre = dg * gp_ref[ALL]
        dbu_ref[ALL] = col_sum(dpre)
        dpre = dpre.astype(BF16)

        @pl.when(j == ZERO)
        def _():
            await_peers(p.peers)
        pause((ZERO, steps), ZERO)
        store_blocks(dw_ref, mm(ht_ref[ALL], dpre))
        pause((ZERO, steps), ONE)
        dr1_ref[ALL] += mm(dpre, wu_ref[ALL], NT)
        pause((ZERO, steps), TWO)

    def norm_backward(at):
        dy = dr1_ref[at, :].astype(BF16).astype(F32)
        hat, r = norm_rows(r1_ref[at, :])
        dr1 = norm_back(dy * g1_ref[ALL], hat, r)
        dr1_ref[at, :] = dr1
        low_ref[at, :] = dr1.astype(BF16)
        dvec_ref[ZERO:ONE, :] += col_sum(dr1)
        dvec_ref[ONE:TWO, :] += col_sum(dy * hat)
        dvec_ref[TWO:THREE, :] += col_sum(dy)

    @pl.when(j == steps)
    def _():
        dvec_ref[ALL] = jnp.zeros_like(dvec_ref)
        for i in range(THREE):
            drain(late[i][ONE], in_sem.at[ONE + i])
        each_block(ZERO, t, norm_backward)
        pause((steps, steps + ONE), ZERO)
        for i in range(4):
            copy(*results[i], out_sem.at[i])

    @pl.when(j >= steps)
    def _():
        half = dr1_ref.shape[ONE] // TWO
        at = pl.ds(pl.multiple_of(jnp.maximum(j - steps, ZERO) * half, half), half)
        pause((steps + ONE, steps + TWO), ZERO)
        pause((steps, steps + TWO), ONE)
        store_blocks(dw_ref, mm(ctx_ref[ALL], low_ref[:, at], TN))
        pause((steps, steps + TWO), TWO)

    @pl.when(j == steps + ONE)
    def _():
        for i in range(4):
            drain(results[i][ZERO], out_sem.at[i])


def up_backward(axis, dr2, dr2b, h, gp, w_down, w_up, r1, gain, ctx_q, ctx_p, part_a, collective_id, tile=TILE):
    t, d = h.shape
    f = w_up.shape[ONE]
    tq, tp = ctx_q.shape[ZERO], ctx_p.shape[ZERO]
    n, total, steps = tile // WIDTH, part_a.shape[ZERO], f // tile
    cut = lambda j: jnp.minimum(j, steps - ONE)
    wide = lambda rows: pl.BlockSpec((rows, tile), lambda j: (ZERO, cut(j)))
    dma, vm = pltpu.SemaphoreType.DMA, pltpu.VMEM
    return pl.pallas_call(
        functools.partial(up_bwd_kernel, axis, steps), grid=(steps + TWO,),
        out_shape=(sds(((f + d) // WIDTH, d, WIDTH), F32), sds((ONE, f), F32), sds((tq, d), F32), sds((tp, d), F32),
                   sds((tq, d), BF16), sds((tp, d), BF16), sds((8, d), F32),
                   sds((total // 128, WIDTH), F32), sds((total // TWO, WIDTH), F32)),
        in_specs=[ANY, whole(t, d), whole(t, d), wide(t), pl.BlockSpec((tile, d), lambda j: (cut(j), ZERO)), wide(d),
                  ANY, whole(ONE, d), ANY, ANY, ANY],
        out_specs=(pl.BlockSpec((n, d, WIDTH), lambda j: (j, ZERO, ZERO)), wide(ONE), ANY, ANY, ANY, ANY,
                   whole(8, d), whole(total // 128, WIDTH), ANY),
        scratch_shapes=[vm((t, d), F32), vm((t, d), BF16), vm((t, d), F32), vm((t, d), BF16), vm((d, t), BF16), dma((4,)), dma((4,))]
        + scatter_scratch(UNITS_A),
        compiler_params=host(collective_id, 63), name="up_backward",
    )(dr2, dr2b, h, gp, w_down, w_up, r1, gain, ctx_q, ctx_p, part_a)


def attn_bwd_body(scale, head, group, low_ref, wo_ref, qkv_ref, probs_ref, out_ref, dctx_ref, pause, enter=lambda: None):
    rows_here, d = low_ref.shape
    pair = TWO * head
    dctx_ref[:rows_here, :] = mm(low_ref[ALL], wo_ref[ALL], NT).astype(BF16)
    enter()
    pause(ZERO)

    def one(g):
        at, k_at, v_at = (pl.ds(pl.multiple_of(part * d + g * pair, pair), pair) for part in range(THREE))
        q = split_heads(qkv_ref[:, at], head)
        k = qkv_ref[:, k_at]
        v = qkv_ref[:, v_at]
        p = probs_ref[ZERO, g]
        dc = split_heads(dctx_ref[:rows_here, at], head)
        dp = mm(dc, v, NT)
        pf = p.astype(F32)
        ds = (pf * (dp - row_sum(dp * pf)) * scale).astype(BF16)
        out_ref[:, at] = join_heads(mm(ds, k), head).astype(BF16)
        out_ref[:, k_at] = mm(ds, q, TN).astype(BF16)
        out_ref[:, v_at] = mm(p, dc, TN).astype(BF16)

    def some(i, _):
        for h in range(group):
            one(i * group + h)
        return ZERO
    lax.fori_loop(ZERO, d // (pair * group), some, ZERO)
    pause(ONE)


def attn_qkv_kernel(axis, scale, head, nq, n_pass, lowq_ref, lowp_ref, wo_ref, qkvq_ref, qkvp_ref, probq_ref, probp_ref,
                    xq_ref, xp_ref, w_ref, dr1q_hbm, dr1p_hbm, b_ref, piecea_ref,
                    dw_ref, db_ref, dhq_ref, dhp_ref, pieceb_ref, part_ref, a_ref, dq_ref, dp_ref, accq_ref, accp_ref, dctx_ref, sem, gsem, *scratch):
    j = pl.program_id(ZERO)
    tile = w_ref.shape[ZERO]
    per = dq_ref.shape[TWO] // tile
    first, last = nq + n_pass, nq + n_pass + per - ONE
    pa, pb = ring_plan(axis, UNITS_A), ring_plan(axis, UNITS_B)
    points = TWO
    steps = [3.2] * nq + [3.3] * n_pass + [4.3] * per
    slots = [sum(steps[:i]) + steps[i] * h / points for i in range(len(steps)) for h in range(points)]
    timed = timeline(scatter_rounds(pb, b_ref, part_ref, pieceb_ref, *scratch), *PACE_B)
    timed += timeline(gather_rounds(pa, piecea_ref, a_ref, gsem), *PACE_A)
    plan = place(timed, slots)
    pause = functools.partial(run_slot, plan, j, points)
    loads = ((dr1q_hbm, accq_ref), (dr1p_hbm, accp_ref))

    @pl.when(j == ZERO)
    def _():
        signal_peers(pa.peers)
        for src, dst in loads:
            copy(src, dst, sem.at[ZERO])

    def enter():
        @pl.when(j == ZERO)
        def _():
            await_peers(pa.peers)

    @pl.when(j < nq)
    def _():
        attn_bwd_body(scale, head, TWO, lowq_ref, wo_ref, qkvq_ref, probq_ref, dq_ref.at[jnp.minimum(j, nq - ONE)], dctx_ref,
                      functools.partial(pause, (ZERO, nq)), enter)

    @pl.when((j >= nq) & (j < first))
    def _():
        attn_bwd_body(scale, head, TWO, lowp_ref, wo_ref, qkvp_ref, probp_ref, dp_ref.at[jnp.clip(j - nq, ZERO, n_pass - ONE)], dctx_ref,
                      functools.partial(pause, (nq, first)))

    @pl.when(j == first - ONE)
    def _():
        for src, dst in loads:
            drain(dst, sem.at[ZERO])

    @pl.when(j >= first)
    def _():
        pause((first, last + ONE), ZERO)
        at = pl.ds(pl.multiple_of(jnp.maximum(j - first, ZERO) * tile, tile), tile)
        dq = dq_ref[:, :, at].reshape(-ONE, tile)
        dp = dp_ref[:, :, at].reshape(-ONE, tile)
        store_blocks(dw_ref, mm(dq, xq_ref[ALL], TN) + mm(dp, xp_ref[ALL], TN))
        db_ref[ALL] = col_sum(dq.astype(F32)) + col_sum(dp.astype(F32))
        pause((first, last + ONE), ONE)
        accq_ref[ALL] += mm(dq, w_ref[ALL])
        accp_ref[ALL] += mm(dp, w_ref[ALL])

    @pl.when(j == last)
    def _():
        dhq_ref[ALL] = accq_ref[ALL].astype(BF16)
        dhp_ref[ALL] = accp_ref[ALL].astype(BF16)


def attn_qkv_backward(axis, low_q, low_p, w_out, qkv_q, qkv_p, probs_q, probs_p, xq, xp, w_t, dr1_q, dr1_p, part_b, piece_a, head,
                      collective_id, tile=TILE):
    f, d = w_t.shape
    nq, pairs, _, lq = probs_q.shape
    n_pass, _, _, lp = probs_p.shape
    tq, tp = nq * lq, n_pass * lp
    per, cols, total = f // tile, d // WIDTH, part_b.shape[ZERO]
    jq = lambda j: jnp.minimum(j, nq - ONE)
    jp = lambda j: jnp.clip(j - nq, ZERO, n_pass - ONE)
    jt = lambda j: jnp.clip(j - nq - n_pass, ZERO, per - ONE)
    rows_of = lambda n, c, at: pl.BlockSpec((n, c), lambda j: (at(j), ZERO))
    probs_of = lambda n, at: pl.BlockSpec((ONE, pairs, TWO * n, n), lambda j: (at(j), ZERO, ZERO, ZERO))
    return pl.pallas_call(
        functools.partial(attn_qkv_kernel, axis, head ** -0.5, head, nq, n_pass), grid=(nq + n_pass + per,),
        out_shape=(sds((cols, f, WIDTH), F32), sds((ONE, f), F32), sds((tq, d), BF16), sds((tp, d), BF16),
                   sds((total // 128, WIDTH), F32), sds((total // TWO, WIDTH), F32), sds((piece_a.shape[ZERO] * 128, WIDTH), F32)),
        in_specs=[rows_of(lq, d, jq), rows_of(lp, d, jp), whole(d, d), rows_of(lq, f, jq), rows_of(lp, f, jp),
                  probs_of(lq, jq), probs_of(lp, jp), whole(tq, d), whole(tp, d), rows_of(tile, d, jt), ANY, ANY, ANY, whole(*piece_a.shape)],
        out_specs=(pl.BlockSpec((cols, tile, WIDTH), lambda j: (ZERO, jt(j), ZERO)), pl.BlockSpec((ONE, tile), lambda j: (ZERO, jt(j))),
                   whole(tq, d), whole(tp, d), whole(total // 128, WIDTH), ANY, ANY),
        scratch_shapes=[pltpu.VMEM((nq, lq, f), BF16), pltpu.VMEM((n_pass, lp, f), BF16), pltpu.VMEM((tq, d), F32),
                        pltpu.VMEM((tp, d), F32), pltpu.VMEM((lp, d), BF16), pltpu.SemaphoreType.DMA((ONE,)),
                        pltpu.SemaphoreType.DMA((GATHER_SEMS,))]
        + scatter_scratch(UNITS_B),
        compiler_params=host(collective_id, 63), name="attn_qkv_backward",
    )(low_q, low_p, w_out, qkv_q, qkv_p, probs_q, probs_p, xq, xp, w_t, dr1_q, dr1_p, part_b, piece_a)


def unpack_kernel(a_hbm, sums_ref, down_ref, up_ref, out_ref, qkv_ref, stage, sem, in_sem, out_sem):
    def cols(i):
        return pl.ds(i * WIDTH, WIDTH)

    slots, rows_each, _ = stage.shape
    n, ff, f = up_ref.shape[ZERO], down_ref.shape[ZERO], qkv_ref.shape[ZERO]
    kept = sums_ref.shape[ZERO] - (up_ref.shape[ONE] + out_ref.shape[ONE]) // WIDTH * n - qkv_ref.shape[ONE] // WIDTH * f
    todo = [(kept + i * rows_each) for i in range((down_ref.shape[ONE] // WIDTH * ff - kept) // rows_each)]

    def load(i):
        copy(a_hbm.at[pl.ds(todo[i], rows_each)], stage.at[i % slots], in_sem.at[i % slots])

    for i in range(slots):
        load(i)
    at = ZERO
    for ref, size in ((up_ref, n), (out_ref, n), (qkv_ref, f), (down_ref, ff)):
        for i in range(ref.shape[ONE] // WIDTH):
            if at < sums_ref.shape[ZERO]:
                copy(sums_ref.at[pl.ds(at, size)], ref.at[:, cols(i)], sem.at[ZERO])
            at += size
    for i, row in enumerate(todo):
        slot = i % slots
        drain(stage.at[slot], in_sem.at[slot])
        copy(stage.at[slot], down_ref.at[pl.ds(row % ff, rows_each), cols(row // ff)], out_sem.at[slot])
        if i >= ONE and i - ONE + slots < len(todo):
            drain(stage.at[slot], out_sem.at[(i - ONE) % slots])
            load(i - ONE + slots)
    for i in range(max(len(todo) - slots, ZERO), len(todo)):
        drain(stage.at[ZERO], out_sem.at[i % slots])
    drain(sums_ref, sem.at[ZERO])


def unpack(a, sums, d, ff, f):
    slots = 4
    dma = pltpu.SemaphoreType.DMA
    return pl.pallas_call(
        unpack_kernel, out_shape=(sds((ff, d), F32), sds((d, ff), F32), sds((d, d), F32), sds((f, d), F32)),
        in_specs=[ANY, pl.BlockSpec(memory_space=pltpu.VMEM)], out_specs=(ANY,) * 4,
        scratch_shapes=[pltpu.VMEM((slots, TWO * TILE, WIDTH), F32), dma((ONE,)), dma((slots,)), dma((slots,))],
        compiler_params=vmem(8), name="unpack",
    )(a, pltpu.with_memory_space_constraint(sums, pltpu.VMEM))


def solution(mesh):
    axis = mesh.axis_names[ZERO]
    n_dev = mesh.shape[axis]

    def local_step(q_hidden, q_mask, p_hidden, p_mask, w_qkv, b_qkv, w_out, b_out, ln1_gain, ln1_shift,
                   w_up, b_up, w_down, b_down, ln2_gain, ln2_shift):
        nq, _, d = q_hidden.shape
        n_pass, p_len = nq * p_hidden.shape[ONE], p_hidden.shape[TWO]
        _, three, heads, head = w_qkv.shape
        xq, xp = q_hidden.reshape(-ONE, d), p_hidden.reshape(-ONE, d)
        p_mask = p_mask.reshape(n_pass, p_len)
        wqkv_t = w_qkv.transpose(ONE, TWO, THREE, ZERO).reshape(-ONE, d)
        wo = w_out.reshape(-ONE, d)
        vecs = [v.reshape(ONE, d) for v in (b_out, ln1_gain, ln1_shift, b_down, ln2_gain, ln2_shift)]

        qkv_q, qkv_p = qkv_project(xq, xp, wqkv_t, b_qkv.reshape(ONE, -ONE))
        probs_q, ctx_q = attention(qkv_q, q_mask, head)
        probs_p, ctx_p = attention(qkv_p, p_mask, head)
        h, r1, g, gp, r2, pooled = ffn_forward(
            xq, xp, ctx_q, ctx_p, wo, vecs, q_mask, p_mask, w_up, b_up.reshape(ONE, -ONE), w_down)
        everyone = gather_embeddings(pooled, axis, ONE)
        mean_loss, d_pooled = loss_and_grad(everyone, pooled, axis, nq * n_dev)
        dwd, dr2, dr2b, dvec2 = down_backward(d_pooled, r2, q_mask, p_mask, vecs[4], g)
        dwb, dbu, dr1_q, dr1_p, low_q, low_p, dvec1, piece_a, _ = up_backward(
            axis, dr2, dr2b, h, gp, w_down, w_up, r1, vecs[ONE], ctx_q, ctx_p, dwd.reshape(-ONE, WIDTH), TWO)
        dwq, dbq, dh_q, dh_p, piece_b, _, a = attn_qkv_backward(
            axis, low_q, low_p, wo, qkv_q, qkv_p, probs_q, probs_p, xq, xp, wqkv_t, dr1_q, dr1_p, dwb.reshape(-ONE, WIDTH), piece_a, head, THREE)
        sums, small = finish_sum(axis, UNITS_B, UNITS_C, piece_b, dwq.reshape(-ONE, WIDTH), a, THREE * w_down.shape[ZERO],
                                 dvec1, dvec2, dbq, dbu, 4)
        d_down, d_up, d_out, d_qkv = unpack(a, sums, d, w_down.shape[ZERO], three * d)
        vec, bias = small[:8], small[8:]
        return (mean_loss, dh_q.reshape(q_hidden.shape), dh_p.reshape(p_hidden.shape),
                d_qkv.reshape(three, heads, head, d).transpose(THREE, ZERO, ONE, TWO), bias[:three].reshape(b_qkv.shape),
                d_out.reshape(w_out.shape), vec[ZERO], vec[ONE], vec[TWO], d_up, bias[three:-ONE].reshape(-ONE),
                d_down, vec[THREE], vec[4], vec[5])

    in_specs = (P(axis),) * 4 + (P(),) * 12
    out_specs = (P(), P(axis), P(axis)) + (P(),) * 12
    return jax.shard_map(local_step, mesh=mesh, in_specs=in_specs, out_specs=out_specs, check_vma=False)
```

```python
import functools
import types
import jax
import jax.numpy as jnp
from jax import lax
from jax.experimental import pallas as pl
from jax.experimental.pallas import tpu as pltpu
from jax.sharding import PartitionSpec as P

ZERO, ONE, TWO, THREE, ALL = 0, 1, 2, 3, ...

F32 = jnp.float32
BF16 = jnp.bfloat16
LOGICAL = pl.DeviceIdType.LOGICAL
RING = 4
WIDTH = 256
COLOURS = range(6)
AXES = range(THREE)
RINGS = range(RING)
TURNS = range(RING * RING)
ANY = pl.BlockSpec(memory_space=pl.ANY)


def mesh_place(axis):
    me = lax.axis_index(axis)
    core = lax.rem(me, TWO)
    chip = lax.div(me, TWO)
    row = lax.div(chip, RING)
    return (lax.rem(chip, RING), lax.rem(row, RING), lax.div(row, RING)), core


def device_at(coords, core):
    return ((coords[TWO] * RING + coords[ONE]) * RING + coords[ZERO]) * TWO + core


def moved(coords, dim, by):
    out = list(coords)
    out[dim] = lax.rem(coords[dim] + by + TWO * RING, RING)
    return tuple(out)


def wrap(i):
    return lax.rem(i + 4 * RING, RING)


def rdma(src, dst, send, recv, to):
    pltpu.make_async_remote_copy(src_ref=src, dst_ref=dst, send_sem=send, recv_sem=recv,
                                 device_id=to, device_id_type=LOGICAL).start()


def copy(src, dst, sem):
    pltpu.make_async_copy(src, dst, sem).start()


def drain(ref, sem):
    pltpu.make_async_copy(ref, ref, sem).wait()


def carve(sems, *counts):
    out, at = [], ZERO
    for n in counts:
        out.append(lambda i, at=at: sems.at[at + i])
        at += n
    return out


def ring_plan(axis, units):
    coords, core = mesh_place(axis)
    p = types.SimpleNamespace(coords=coords, core=core, partner=device_at(coords, ONE - core))
    p.dims = [tuple((k // TWO + s) % THREE for s in AXES) for k in COLOURS]
    p.sign = [ONE - TWO * (k % TWO) for k in COLOURS]
    p.pos = [tuple(coords[d] for d in p.dims[k]) for k in COLOURS]
    p.nxt = [tuple(device_at(moved(coords, d, p.sign[k]), core) for d in p.dims[k]) for k in COLOURS]
    p.piece = [8 * u for u in units]
    p.lead = [sum(p.piece[:k]) for k in COLOURS]
    p.all = sum(p.piece)
    p.half = 64 * p.all
    p.base = core * p.half
    p.peers = [p.partner] + [device_at(moved(coords, d, by), core) for d in AXES for by in (ONE, THREE)]
    p.across = [device_at(moved(coords, d, TWO), core) for d in AXES]
    p.prv = [tuple(device_at(moved(coords, d, -p.sign[k]), core) for d in p.dims[k]) for k in COLOURS]
    return p


def rows(at, n):
    return pl.ds(pl.multiple_of(at, 8), n)


def place_of(p, k, ring, back):
    return wrap(p.pos[k][ring] - p.sign[k] * back)


def chunk_row(p, k, back):
    return 64 * p.lead[k] + place_of(p, k, ZERO, back) * (16 * p.piece[k])


def sub_row(p, k, row, back):
    return row + place_of(p, k, ONE, back) * (4 * p.piece[k])


def piece_row(p, k, row, back):
    return row + place_of(p, k, TWO, back) * p.piece[k]


GIVE = (TWO, ONE, THREE, ZERO)
TAKE = (ZERO, ONE, THREE, TWO)


def signal_peers(peers):
    barrier = pltpu.get_barrier_semaphore()
    for peer in peers:
        pl.semaphore_signal(barrier, inc=ONE, device_id=peer, device_id_type=LOGICAL)


def await_peers(peers):
    pl.semaphore_wait(pltpu.get_barrier_semaphore(), len(peers))


SCATTER_SEMS = 4 + THREE * 16 + TWO * 12 + 4 * THREE


def scatter_scratch(units):
    n = 8 * sum(units)
    vm = lambda *s: pltpu.VMEM(s + (WIDTH,), F32)
    return [vm(64 * n), vm(TWO, 4 * n), vm(THREE, RING, 4 * n), vm(THREE, 4 * n), vm(THREE, n), pltpu.SemaphoreType.DMA((SCATTER_SEMS,))]


def scatter_rounds(p, src, part, out, acc, stage, land1, land2, land3, sems):
    load_sem, swap_send, swap_recv, stage_sem, p1_send, p1_recv, p2_send, p2_recv, p3_send, p3_recv = carve(
        sems, 4, 16, 16, 16, 12, 12, THREE, THREE, THREE, THREE)
    n_sub, n_chunk = 4 * p.all, 16 * p.all
    far = p.half - p.base

    def turn_row(k, n):
        return sub_row(p, k, chunk_row(p, k, n // RING + ONE), GIVE[n % RING])

    def load(t):
        for k in COLOURS:
            r, m = chunk_row(p, k, t + ONE), 16 * p.piece[k]
            copy(src.at[rows(p.base + r, m)], acc.at[rows(r, m)], load_sem(t))

    def swap(n):
        for k in COLOURS:
            r, m = turn_row(k, n), 4 * p.piece[k]
            rdma(src.at[rows(far + r, m)], part.at[rows(r, m)], swap_send(n), swap_recv(n), p.partner)

    def fetch(n):
        drain(part.at[pl.ds(ZERO, n_sub)], swap_recv(n))
        for k in COLOURS:
            m = 4 * p.piece[k]
            copy(part.at[rows(turn_row(k, n), m)], stage.at[n % TWO, pl.ds(4 * p.lead[k], m)], stage_sem(n))

    def begin():
        for t in RINGS:
            load(t)
        for n in range(6):
            swap(n)

    def turn(n):
        t, i = n // RING, n % RING
        if n == ZERO:
            fetch(n)
        if n + 6 < 16:
            swap(n + 6)
        if n + ONE < 16:
            fetch(n + ONE)
        if i == ZERO:
            drain(acc.at[pl.ds(ZERO, n_chunk)], load_sem(t))
        drain(stage.at[n % TWO], stage_sem(n))
        if t > ZERO:
            drain(land1.at[t - ONE, i], p1_recv(n - 4))
        for k in COLOURS:
            at, m = rows(turn_row(k, n), 4 * p.piece[k]), pl.ds(4 * p.lead[k], 4 * p.piece[k])
            val = acc[at] + stage[n % TWO, m]
            acc[at] = val + land1[t - ONE, i, m] if t > ZERO else val
        if t < THREE:
            for k in COLOURS:
                at, m = rows(turn_row(k, n), 4 * p.piece[k]), pl.ds(4 * p.lead[k], 4 * p.piece[k])
                rdma(acc.at[at], land1.at[t, i, m], p1_send(n), p1_recv(n), p.nxt[k][ZERO])

    def pass_on(i, where, land, send, recv, ring):
        if i == TWO:
            drain(land.at[ZERO], recv(ZERO))
        for k in COLOURS:
            at, m = where(k, i)
            if i == TWO:
                acc[at] += land[ZERO, m]
        for k in COLOURS:
            at, m = where(k, i)
            rdma(acc.at[at], land.at[i, m], send(i), recv(i), (p.prv if i == ONE else p.nxt)[k][ring])

    def sub_at(k, i):
        return rows(turn_row(k, 12 + i), 4 * p.piece[k]), pl.ds(4 * p.lead[k], 4 * p.piece[k])

    def piece_at(k, i):
        return rows(piece_row(p, k, turn_row(k, 15), GIVE[i]), p.piece[k]), pl.ds(p.lead[k], p.piece[k])

    def second(i):
        pass_on(i, sub_at, land2, p2_send, p2_recv, ONE)

    def third():
        for i in (ONE, TWO):
            drain(land2.at[i], p2_recv(i))
        for k in COLOURS:
            at, m = sub_at(k, THREE)
            acc[at] += land2[ONE, m] + land2[TWO, m]
        for i in (ZERO, ONE):
            pass_on(i, piece_at, land3, p3_send, p3_recv, TWO)

    def fourth():
        pass_on(TWO, piece_at, land3, p3_send, p3_recv, TWO)

    def last():
        for i in (ONE, TWO):
            drain(land3.at[i], p3_recv(i))
        for k in COLOURS:
            at, m = piece_at(k, THREE)
            out[m] = acc[at] + (land3[ONE, m] + land3[TWO, m])

    def finish():
        for n in TURNS:
            drain(acc.at[pl.ds(ZERO, n_sub)], swap_send(n))
        for n in range(12):
            drain(acc.at[pl.ds(ZERO, n_sub)], p1_send(n))
        for t in AXES:
            drain(acc.at[pl.ds(ZERO, n_sub)], p2_send(t))
            drain(acc.at[pl.ds(ZERO, p.all)], p3_send(t))

    act = functools.partial
    def both(*fs):
        def run():
            for f in fs:
                f()
        return run
    steps = [begin] + [act(turn, n) for n in range(12)]
    steps += [both(act(turn, 12 + i), act(second, i)) for i in AXES] + [act(turn, 15), third, fourth, last, finish]
    return steps


GATHER_SEMS = ONE + TWO * (THREE + THREE + 12 + 16)


def gather_rounds(p, piece, out, sems):
    own_sem, a3_send, a3_recv, a2_send, a2_recv, a1_send, a1_recv, push_send, push_recv = carve(
        sems, ONE, THREE, THREE, THREE, THREE, 12, 12, 16, 16)
    n_sub = 4 * p.all

    def many(n):
        return out.at[pl.ds(ZERO, n)]

    def sub_at(k, c, s):
        return rows(p.base + sub_row(p, k, chunk_row(p, k, c), TAKE[s]), 4 * p.piece[k])

    def piece_at(k, g):
        return rows(p.base + piece_row(p, k, sub_row(p, k, chunk_row(p, k, ZERO), ZERO), TAKE[g]), p.piece[k])

    def both_ways(at, send, recv, ring, srcs=out):
        for k in COLOURS:
            src = out.at[at(k)] if srcs is out else srcs.at[pl.ds(p.lead[k], p.piece[k])]
            rdma(src, out.at[at(k)], send(ZERO), recv(ZERO), p.nxt[k][ring])
            rdma(src, out.at[at(k)], send(ONE), recv(ONE), p.prv[k][ring])

    def forward(at, send, recv, ring):
        for k in COLOURS:
            rdma(out.at[at(k)], out.at[at(k)], send(TWO), recv(TWO), p.nxt[k][ring])

    def third():
        for k in COLOURS:
            copy(piece.at[pl.ds(p.lead[k], p.piece[k])], out.at[piece_at(k, ZERO)], own_sem(ZERO))
        both_ways(lambda k: piece_at(k, ZERO), a3_send, a3_recv, TWO, piece)

    def fourth():
        drain(many(p.all), a3_recv(ZERO))
        forward(lambda k: piece_at(k, ONE), a3_send, a3_recv, TWO)

    def hop1(c, s):
        for k in COLOURS:
            if c < THREE:
                rdma(out.at[sub_at(k, c, s)], out.at[sub_at(k, c, s)], a1_send(RING * c + s), a1_recv(RING * c + s), p.nxt[k][ZERO])
            rdma(out.at[sub_at(k, c, s)], out.at[sub_at(k, c, s)], push_send(RING * c + s), push_recv(RING * c + s), p.partner)

    def second(s):
        if s == ZERO:
            for sem in (own_sem(ZERO), a3_recv(ONE), a3_recv(TWO)):
                drain(many(p.all), sem)
            both_ways(lambda k: sub_at(k, ZERO, ZERO), a2_send, a2_recv, ONE)
        else:
            drain(many(n_sub), a2_recv(s - ONE))
        if s == ONE:
            forward(lambda k: sub_at(k, ZERO, ONE), a2_send, a2_recv, ONE)
        hop1(ZERO, s)

    def first(c, s):
        drain(many(n_sub), a1_recv(RING * (c - ONE) + s))
        hop1(c, s)

    def finish():
        for t in AXES:
            drain(many(p.all), a3_send(t))
            drain(many(n_sub), a2_send(t))
        for n in range(12):
            drain(many(n_sub), a1_send(n))
        for n in TURNS:
            drain(many(n_sub), push_send(n))
            drain(many(n_sub), push_recv(n))

    act = functools.partial
    return ([third, fourth] + [act(second, s) for s in RINGS]
            + [act(first, c, s) for c in (ONE, TWO, THREE) for s in RINGS] + [finish])


def small_scratch(shape):
    return [pltpu.VMEM((4, THREE) + shape, F32), pltpu.SemaphoreType.DMA((8,))]


def small_rounds(p, src, out, land, sems):
    places = [(None, p.core, TWO)] + [(d, p.coords[d], RING) for d in AXES]

    def send(n):
        d, _, size = places[n]
        for by in range(ONE, size):
            to = p.partner if d is None else device_at(moved(p.coords, d, by), p.core)
            rdma(out, land.at[n, by - ONE], sems.at[n], sems.at[4 + n], to)

    def step(n):
        if n == ZERO:
            out[ALL] = src[ALL]
        else:
            _, place, size = places[n - ONE]
            got = land.at[n - ONE, pl.ds(ZERO, size - ONE)]
            drain(got, sems.at[4 + n - ONE])
            drain(got, sems.at[n - ONE])
            mine, total = out[ALL], None
            for q in range(size):
                val = mine
                for by in range(ONE, size):
                    val = jnp.where(lax.rem(place - q + size, size) == by, land[n - ONE, by - ONE], val)
                total = val if total is None else total + val
            out[ALL] = total
        if n < 4:
            send(n)

    return [functools.partial(step, n) for n in range(5)]


def spread(steps, slots):
    plan = [[] for _ in range(slots)]
    for i, s in enumerate(steps):
        plan[i * slots // len(steps)].append(s)
    return plan


def finish_kernel(axis, units_b, units_c, pieceb_ref, c_ref, a_ref, vec1_ref, vec2_ref, bq_ref, bu_ref, bc_out, small_out, part,
                  small_ref, piecec, a_sem, *scratch):
    sc, (gather_sem, gather_sem2, small_land, small_sem) = scratch[:6], scratch[6:]
    pb, pc = ring_plan(axis, units_b), ring_plan(axis, units_c)
    n_b, n_c = TWO * pb.half, TWO * pc.half
    b_out, c_out = bc_out.at[pl.ds(ZERO, n_b)], bc_out.at[pl.ds(n_b, n_c)]
    a_here = bc_out.at[pl.ds(n_b + n_c, bc_out.shape[ZERO] - n_b - n_c)]
    peers = pb.peers + pb.across
    signal_peers(peers)
    width = small_ref.shape[ONE]
    small_ref[ALL] = jnp.zeros_like(small_ref)
    small_ref[ZERO:THREE, :] = vec1_ref[ZERO:THREE, :]
    small_ref[THREE:6, :] = vec2_ref[ZERO:THREE, :]
    at = 8
    for ref in (bq_ref, bu_ref):
        for i in range(ref.shape[ONE] // width):
            small_ref[at:at + ONE, :] = ref[:, i * width:(i + ONE) * width]
            at += ONE
    await_peers(peers)
    reduce_c = scatter_rounds(pc, c_ref, part, piecec, *sc)
    gather_b = gather_rounds(pb, pieceb_ref, b_out, gather_sem)
    gather_c = gather_rounds(pc, piecec, c_out, gather_sem2)
    smalls = small_rounds(pb, small_ref, small_out, small_land, small_sem)
    main = reduce_c[:-ONE] + gather_c[:-ONE]
    fill = spread(gather_b[:-ONE], len(main) - 4)
    for i, f in enumerate(main):
        f()
        if i == 16:
            copy(a_ref.at[pl.ds(ZERO, a_here.shape[ZERO])], a_here, a_sem.at[ZERO])
        if i % THREE == ONE and i // THREE < len(smalls):
            smalls[i // THREE]()
        for f in fill[i] if i < len(fill) else ():
            f()
    for rounds in (reduce_c, gather_b, gather_c):
        rounds[-ONE]()
    drain(a_here, a_sem.at[ZERO])


def finish_sum(axis, units_b, units_c, piece_b, c, a, keep, vec1, vec2, bq, bu, collective_id):
    sds = jax.ShapeDtypeStruct
    dma = pltpu.SemaphoreType.DMA
    vm = pl.BlockSpec(memory_space=pltpu.VMEM)
    n = c.shape[ZERO]
    small = (16, vec1.shape[ONE])
    outs = pl.pallas_call(
        functools.partial(finish_kernel, axis, units_b, units_c),
        out_shape=(pltpu.VMEM((piece_b.shape[ZERO] * 128 + n + keep, WIDTH), F32), sds(small, F32), sds((n // TWO, WIDTH), F32)),
        in_specs=[vm, ANY, ANY, vm, vm, vm, vm], out_specs=(vm, vm, ANY),
        scratch_shapes=[pltpu.VMEM(small, F32), pltpu.VMEM((n // 128, WIDTH), F32), dma((ONE,))] + scatter_scratch(units_c)
        + [dma((GATHER_SEMS,)), dma((GATHER_SEMS,))] + small_scratch(small),
        compiler_params=pltpu.CompilerParams(collective_id=collective_id, has_side_effects=True, vmem_limit_bytes=17 * 1024 * 1024),
        name="finish_sum",
    )(piece_b, c, a, vec1, vec2, bq, bu)
    return outs[:TWO]


def gather_kernel(axis, pooled_ref, g_ref, e_ref, mine, theirs, swap_sem, sems_send, sems_recv, push_send, push_recv):
    coords, core = mesh_place(axis)
    partner = device_at(coords, ONE - core)
    width = e_ref.shape[ONE]
    lanes = pl.ds(pl.multiple_of(core * (width // TWO), 128), width // TWO)
    x, y, z = coords
    peers = [partner] + [device_at(moved(coords, d, by), core) for d in AXES for by in (ONE, TWO, THREE)]
    signal_peers(peers)
    size = row_sum(pooled_ref[ALL] * pooled_ref[ALL])
    e_ref[ALL] = pooled_ref[ALL] * jnp.where(size > 0.0, lax.rsqrt(size), 0.0)
    mine[ALL] = e_ref[ALL]
    await_peers(peers)

    rdma(e_ref, theirs, swap_sem.at[ZERO], swap_sem.at[ONE], partner)
    drain(theirs, swap_sem.at[ONE])
    first = jnp.where(core == ZERO, mine[:, lanes], theirs[:, lanes])
    second = jnp.where(core == ZERO, theirs[:, lanes], mine[:, lanes])
    g_ref[z, y, x, ZERO:4, lanes] = first[ZERO:4]
    g_ref[z, y, x, 4:8, lanes] = second[ZERO:4]
    g_ref[z, y, x, 8:16, lanes] = first[8:16]
    g_ref[z, y, x, 16:24, lanes] = second[8:16]
    drain(e_ref, swap_sem.at[ZERO])

    def view(a, stage):
        idx = [z, y, x]
        for s in range(stage):
            idx[TWO - (a + s) % THREE] = slice(None)
        return g_ref.at[idx[ZERO], idx[ONE], idx[TWO], pl.ds(8 * a, 8), lanes]

    for stage in range(THREE):
        for by in (ONE, THREE, TWO):
            for a in range(THREE):
                to = device_at(moved(coords, (a + stage) % THREE, by), core)
                rdma(view(a, stage), view(a, stage), sems_send.at[stage, by - ONE], sems_recv.at[stage, by - ONE], to)
        if stage == TWO:
            for a in range(THREE):
                rdma(view(a, TWO), view(a, TWO), push_send.at[ZERO], push_recv.at[ZERO], partner)
        for by in (ONE, THREE, TWO):
            n = 4 ** stage
            shape_like = g_ref.at[ZERO, ZERO, ZERO, :, lanes] if stage == ZERO else (
                g_ref.at[ZERO, ZERO, :, :, lanes] if stage == ONE else g_ref.at[ZERO, :, :, :, lanes])
            drain(shape_like, sems_recv.at[stage, by - ONE])
            if stage == TWO:
                for a in range(THREE):
                    far = moved(coords, (a + TWO) % THREE, RING - by)
                    idx = [far[TWO], far[ONE], far[ZERO]]
                    idx[TWO - a] = slice(None)
                    idx[TWO - (a + ONE) % THREE] = slice(None)
                    v = g_ref.at[idx[ZERO], idx[ONE], idx[TWO], pl.ds(8 * a, 8), lanes]
                    rdma(v, v, push_send.at[by], push_recv.at[by], partner)
    for stage in range(THREE):
        shape_like = g_ref.at[ZERO, ZERO, ZERO, :, lanes] if stage == ZERO else (
            g_ref.at[ZERO, ZERO, :, :, lanes] if stage == ONE else g_ref.at[ZERO, :, :, :, lanes])
        for by in (ONE, TWO, THREE):
            drain(shape_like, sems_send.at[stage, by - ONE])
    for by in range(4):
        drain(g_ref.at[ZERO, :, :, :, lanes], push_send.at[by])
        drain(g_ref.at[ZERO, :, :, :, lanes], push_recv.at[by])


def gather_embeddings(e, axis, collective_id):
    dma = pltpu.SemaphoreType.DMA
    width = e.shape[ONE]
    g = pl.pallas_call(
        functools.partial(gather_kernel, axis),
        out_shape=jax.ShapeDtypeStruct((RING, RING, RING, 24, width), F32),
        in_specs=[pl.BlockSpec(memory_space=pltpu.VMEM)],
        out_specs=pl.BlockSpec(memory_space=pltpu.VMEM),
        scratch_shapes=[pltpu.VMEM(e.shape, F32)] * THREE + [dma((TWO,)),
                        dma((THREE, THREE)), dma((THREE, THREE)), dma((4,)), dma((4,))],
        compiler_params=pltpu.CompilerParams(collective_id=collective_id, has_side_effects=True,
                                             vmem_limit_bytes=16 * 1024 * 1024),
        name="gather_embeddings",
    )(e)
    return g.reshape(RING ** THREE, 24, width)


def split3(x):
    hi = x.astype(BF16)
    rest = x - hi.astype(F32)
    mid = rest.astype(BF16)
    return hi, mid, (rest - mid.astype(F32)).astype(BF16)


def dot6(a, b, dims):
    low = mm(a[TWO], b[ZERO], dims) + mm(a[ZERO], b[TWO], dims) + mm(a[ONE], b[ONE], dims)
    return mm(a[ZERO], b[ZERO], dims) + (mm(a[ZERO], b[ONE], dims) + mm(a[ONE], b[ZERO], dims) + low)


def loss_kernel(axis, n_query, g_ref, pooled_ref, loss_ref, d_ref, logit_ref, lse_ref, q_ref, p_ref, dp_ref):
    me = lax.axis_index(axis)
    core, chip = lax.rem(me, TWO), lax.div(me, TWO)
    chips, _, width = g_ref.shape
    nq = chips * 8
    lanes = 128
    gs = 100.0 / n_query
    for i, part in enumerate(split3(g_ref[:, ZERO:8, :].reshape(nq, width))):
        q_ref[i] = part
    block = TWO * lanes

    def logits(b, _):
        at = pl.multiple_of(b * block, block)
        p = split3(g_ref[pl.ds(b * (block // 16), block // 16), 8:24, :].reshape(block, width))
        for i, part in enumerate(p):
            p_ref[i, pl.ds(at, block), :] = part
        logit_ref[:, pl.ds(at, block)] = dot6((q_ref[ZERO], q_ref[ONE], q_ref[TWO]), p, NT) * 100.0
        return ZERO

    lax.fori_loop(ZERO, chips * 16 // block, logits, ZERO)

    def rows_of(b, loss):
        at = pl.ds(pl.multiple_of(b * lanes, lanes), lanes)
        s = logit_ref[at, :]
        top = jnp.max(s, axis=ONE, keepdims=True)
        lse = jnp.log(row_sum(jnp.exp(s - top))) + top
        lse_ref[at, :] = jnp.broadcast_to(lse, (lanes, lanes))
        row = lax.broadcasted_iota(jnp.int32, s.shape, ZERO) + b * lanes
        col = lax.broadcasted_iota(jnp.int32, s.shape, ONE)
        return loss + col_sum(lse - row_sum(jnp.where(col == TWO * row, s, 0.0)))

    loss = lax.fori_loop(ZERO, nq // lanes, rows_of, jnp.zeros((ONE, ONE), F32))
    loss_ref[ALL] = jnp.broadcast_to(loss * (1.0 / n_query), loss_ref.shape)

    def weights(s, lse, row, col):
        row = lax.broadcasted_iota(jnp.int32, s.shape, ZERO) + row
        col = lax.broadcasted_iota(jnp.int32, s.shape, ONE) + col
        return jnp.exp(s - lse) * gs - jnp.where(col == TWO * row, gs, 0.0)

    at = pl.ds(pl.multiple_of(chip * 8, 8), 8)
    w = jnp.concatenate([x.astype(F32) for x in split3(weights(logit_ref[at, :], lse_ref[at, ZERO:ONE], chip * 8, ZERO))], axis=ZERO).astype(BF16)
    by_hi, by_mid, by_low = (mm(w, p_ref[i]) for i in range(THREE))
    dq = by_hi[ZERO:8] + (by_hi[8:16] + by_mid[ZERO:8] + (by_hi[16:24] + by_mid[8:16] + by_low[ZERO:8]))

    first = pl.multiple_of(lax.div(chip, 8) * lanes, lanes)
    w = weights(logit_ref[:, pl.ds(first, lanes)], lse_ref[ALL], ZERO, first)
    dp_ref[ALL] = dot6(split3(w.T), (q_ref[ZERO], q_ref[ONE], q_ref[TWO]), NN)
    dp = dp_ref[pl.ds(pl.multiple_of(lax.rem(chip, 8) * 16 + core * 8, 8), 8), :]

    def back(d, pooled):
        inv = lax.rsqrt(row_sum(pooled * pooled))
        e = pooled * inv
        return (d - e * row_sum(e * d)) * inv

    d_ref[ALL] = jnp.zeros_like(d_ref)
    d_ref[ZERO:4, :] = back(jnp.where(core == ZERO, dq[ZERO:4], dq[4:8]), pooled_ref[ZERO:4])
    d_ref[8:16, :] = back(dp, pooled_ref[8:16])


def loss_and_grad(g, pooled, axis, n_query):
    chips, _, width = g.shape
    nq, n_pass, lanes = chips * 8, chips * 16, 128
    vm = pl.BlockSpec(memory_space=pltpu.VMEM)
    loss, d = pl.pallas_call(
        functools.partial(loss_kernel, axis, n_query),
        out_shape=(jax.ShapeDtypeStruct((8, lanes), F32), jax.ShapeDtypeStruct(pooled.shape, F32)),
        in_specs=[vm] * TWO, out_specs=(vm,) * TWO,
        scratch_shapes=[pltpu.VMEM((nq, n_pass), F32), pltpu.VMEM((nq, lanes), F32), pltpu.VMEM((THREE, nq, width), BF16),
                        pltpu.VMEM((THREE, n_pass, width), BF16), pltpu.VMEM((lanes, width), F32)],
        compiler_params=vmem(28), name="loss_and_grad",
    )(g, pooled)
    return loss[ZERO, ZERO], d


NN = (((ONE,), (ZERO,)), ((), ()))
NT = (((ONE,), (ONE,)), ((), ()))
TN = (((ZERO,), (ZERO,)), ((), ()))
LN_EPS = 1e-12
NEG_FILL = -1e9
TILE = 512
UNITS_A, UNITS_B, UNITS_C = (THREE, THREE, THREE, THREE, TWO, TWO), (THREE, THREE, THREE, THREE, 4, 4), (TWO,) * 6
sds = jax.ShapeDtypeStruct


def mm(a, b, dims=NN):
    return lax.dot_general(a, b, dims, preferred_element_type=F32)


def vmem(mb=60):
    return pltpu.CompilerParams(vmem_limit_bytes=mb * 1024 * 1024)


def whole(*shape):
    return pl.BlockSpec(shape, lambda j: (ZERO,) * len(shape), pipeline_mode=pl.Buffered(ONE))


def across(rows, tile):
    return pl.BlockSpec((rows, tile), lambda j: (ZERO, j))


def down(tile, cols):
    return pl.BlockSpec((tile, cols), lambda j: (j, ZERO))


def row_mean(x):
    return jnp.mean(x, axis=ONE, keepdims=True)


def row_sum(x):
    return jnp.sum(x, axis=ONE, keepdims=True)


def col_sum(x):
    return jnp.sum(x, axis=ZERO, keepdims=True)


def qkv_kernel(xq_ref, xp_ref, w_ref, b_ref, oq_ref, op_ref, x_ref):
    tq = xq_ref.shape[ZERO]

    @pl.when(pl.program_id(ZERO) == ZERO)
    def _():
        x_ref[:tq, :] = xq_ref[ALL]
        x_ref[tq:, :] = xp_ref[ALL]
    y = (mm(x_ref[ALL], w_ref[ALL], NT) + b_ref[ALL]).astype(BF16)
    oq_ref[ALL] = y[:tq]
    op_ref[ALL] = y[tq:]


def qkv_project(xq, xp, w_t, b, tile=TILE):
    tq, d = xq.shape
    tp, f = xp.shape[ZERO], w_t.shape[ZERO]
    return pl.pallas_call(
        qkv_kernel, grid=(f // tile,),
        out_shape=(sds((tq, f), BF16), sds((tp, f), BF16)),
        in_specs=[whole(tq, d), whole(tp, d), down(tile, d), across(ONE, tile)],
        out_specs=(across(tq, tile), across(tp, tile)),
        scratch_shapes=[pltpu.VMEM((tq + tp, d), BF16)],
        compiler_params=vmem(), name="qkv_project",
    )(xq, xp, w_t, b)


def split_heads(pair, head):
    lane = lax.broadcasted_iota(jnp.int32, pair.shape, ONE)
    zero = jnp.zeros_like(pair)
    return jnp.concatenate([jnp.where(lane < head, pair, zero), jnp.where(lane >= head, pair, zero)], axis=ZERO)


def join_heads(stacked, head):
    t = stacked.shape[ZERO] // TWO
    lane = lax.broadcasted_iota(jnp.int32, (t, stacked.shape[ONE]), ONE)
    return jnp.where(lane < head, stacked[:t], stacked[t:])


def attn_kernel(scale, head, qkv_ref, mask_ref, probs_ref, ctx_ref):
    d = ctx_ref.shape[ONE]
    pair = TWO * head
    keep = mask_ref[ZERO] > ZERO
    for g in range(d // pair):
        at = pl.ds(g * pair, pair)
        q = split_heads(qkv_ref[:, at], head)
        k = qkv_ref[:, pl.ds(d + g * pair, pair)]
        v = qkv_ref[:, pl.ds(TWO * d + g * pair, pair)]
        s = jnp.where(keep, mm(q, k, NT) * scale, NEG_FILL)
        e = jnp.exp(s - jnp.max(s, axis=ONE, keepdims=True))
        p = (e / row_sum(e)).astype(BF16)
        probs_ref[ZERO, g] = p
        ctx_ref[:, at] = join_heads(mm(p, v), head).astype(BF16)


def attention(qkv, mask, head):
    n, seq = mask.shape
    d = qkv.shape[ONE] // THREE
    pairs = d // (TWO * head)
    return pl.pallas_call(
        functools.partial(attn_kernel, head ** -0.5, head), grid=(n,),
        out_shape=(sds((n, pairs, TWO * seq, seq), BF16), sds((n * seq, d), BF16)),
        in_specs=[down(seq, THREE * d), pl.BlockSpec((ONE, ONE, seq), lambda j: (j, ZERO, ZERO))],
        out_specs=(pl.BlockSpec((ONE, pairs, TWO * seq, seq), lambda j: (j, ZERO, ZERO, ZERO)), down(seq, d)),
        compiler_params=vmem(), name="attention",
    )(qkv, mask.reshape(n, ONE, seq))


def norm_rows(x):
    c = x - row_mean(x)
    r = lax.rsqrt(row_mean(c * c) + LN_EPS)
    return c * r, r


def norm_back(g, hat, r):
    return r * (g - row_mean(g) - hat * row_mean(g * hat))


ERFC = (0.07122347, -0.27794802, 0.29668747, -0.02018065, 0.21581222, 0.21731356, 0.24887118, 0.24822095)


def gelu_parts(u):
    bell = jnp.exp2(u * u * -0.7213475204)
    t = 1.0 / (1.0 + 0.311126984 * jnp.abs(u))
    poly = 0.5 * ERFC[ZERO]
    for c in ERFC[ONE:]:
        poly = poly * t + 0.5 * c
    tail = bell * (poly * t)
    return jnp.where(u >= 0.0, 1.0 - tail, tail), u * bell * 0.3989422804


def each_sequence(mq_ref, mp_ref, act):
    for first, lo, ref in ((ZERO, ZERO, mq_ref), (8, mq_ref.shape[ZERO] * mq_ref.shape[ONE], mp_ref)):
        n, seq = ref.shape

        def one(i, _):
            size = row_sum(ref[pl.ds(i, ONE), :].astype(F32))
            token = lax.broadcasted_iota(jnp.int32, (seq, ONE), ZERO).astype(F32)
            act(first + i, pl.ds(pl.multiple_of(lo + i * seq, 16), seq), jnp.where(token < size, 1.0 / size, 0.0))
            return ZERO
        lax.fori_loop(ZERO, n, one, ZERO)


def each_block(lo, hi, act, size=304):
    def one(i, _):
        act(pl.ds(pl.multiple_of(lo + i * size, 16), size))
        return ZERO
    lax.fori_loop(ZERO, (hi - lo) // size, one, ZERO)


def ffn_kernel(xq_ref, xp_ref, cq_ref, cp_ref, wo_ref, bo_ref, g1_ref, s1_ref, bd_ref, g2_ref, s2_ref, mq_ref, mp_ref,
               wu_ref, bu_ref, wd_ref, h_hbm, r1_hbm, g_ref, gp_ref, r2_hbm, pool_ref, h_ref, r1_ref, r2_ref, sems):
    j = pl.program_id(ZERO)
    t, tq = h_ref.shape[ZERO], cq_ref.shape[ZERO]
    saved = ((h_ref, h_hbm), (r1_ref, r1_hbm), (r2_ref, r2_hbm))

    @pl.when(j == ZERO)
    def _():
        for x_ref, c_ref, lo, size in ((xq_ref, cq_ref, ZERO, tq), (xp_ref, cp_ref, tq, 256)):
            def block(at):
                to = pl.ds(pl.multiple_of(lo + at.start, 16), size)
                r1 = x_ref[at, :].astype(F32) + mm(c_ref[at, :], wo_ref[ALL]) + bo_ref[ALL]
                r1_ref[to, :] = r1
                h = (norm_rows(r1)[ZERO] * g1_ref[ALL] + s1_ref[ALL]).astype(BF16)
                h_ref[to, :] = h
                r2_ref[to, :] = h.astype(F32) + bd_ref[ALL]
            each_block(ZERO, c_ref.shape[ZERO], block, size)
        for i in range(TWO):
            copy(*saved[i], sems.at[i])

    def block(at):
        u = mm(h_ref[at, :], wu_ref[ALL]) + bu_ref[ALL]
        cdf, upd = gelu_parts(u)
        g = (u * cdf).astype(BF16)
        g_ref[at, :] = g
        gp_ref[at, :] = cdf + upd
        r2_ref[at, :] += mm(g, wd_ref[ALL])
    each_block(ZERO, t, block)

    @pl.when(j == pl.num_programs(ZERO) - ONE)
    def _():
        copy(*saved[TWO], sems.at[TWO])
        pool_ref[ALL] = jnp.zeros_like(pool_ref)

        def pool(row, at, weight):
            y = norm_rows(r2_ref[at, :])[ZERO] * g2_ref[ALL] + s2_ref[ALL]
            pool_ref[pl.ds(row, ONE), :] = col_sum(y * weight)
        each_sequence(mq_ref, mp_ref, pool)
        for i in range(THREE):
            drain(saved[i][ZERO], sems.at[i])


def ffn_forward(xq, xp, ctx_q, ctx_p, w_out, vecs, mask_q, mask_p, w_up, b_up, w_down, tile=TWO * TILE):
    tq, d = xq.shape
    tp, f = xp.shape[ZERO], w_up.shape[ONE]
    t = tq + tp
    return pl.pallas_call(
        ffn_kernel, grid=(f // tile,),
        out_shape=(sds((t, d), BF16), sds((t, d), F32), sds((t, f), BF16), sds((t, f), F32), sds((t, d), F32), sds((16, d), F32)),
        in_specs=[whole(tq, d), whole(tp, d), whole(tq, d), whole(tp, d), whole(d, d), *(whole(ONE, d) for _ in vecs),
                  whole(*mask_q.shape), whole(*mask_p.shape), across(d, tile), across(ONE, tile), down(tile, d)],
        out_specs=(ANY, ANY, across(t, tile), across(t, tile), ANY, whole(16, d)),
        scratch_shapes=[pltpu.VMEM((t, d), BF16), pltpu.VMEM((t, d), F32), pltpu.VMEM((t, d), F32), pltpu.SemaphoreType.DMA((THREE,))],
        compiler_params=vmem(), name="ffn_forward",
    )(xq, xp, ctx_q, ctx_p, w_out, *vecs, mask_q, mask_p, w_up, b_up, w_down)


def store_blocks(ref, val):
    for c in range(ref.shape[ZERO]):
        ref[c] = val[:, c * WIDTH:(c + ONE) * WIDTH]


def down_bwd_kernel(dpool_ref, r2_ref, mq_ref, mp_ref, g2_ref, g_ref, dwd_ref, dr2_hbm, dr2b_hbm, dvec_ref, dr2_ref, dr2b_ref, sems):
    j = pl.program_id(ZERO)
    saved = ((dr2_ref, dr2_hbm), (dr2b_ref, dr2b_hbm))

    @pl.when(j == ZERO)
    def _():
        dvec_ref[ALL] = jnp.zeros_like(dvec_ref)

        def one(row, at, weight):
            hat, r = norm_rows(r2_ref[at, :])
            dy = weight * dpool_ref[pl.ds(row, ONE), :]
            dr2 = norm_back(dy * g2_ref[ALL], hat, r)
            dr2_ref[at, :] = dr2
            dr2b_ref[at, :] = dr2.astype(BF16)
            dvec_ref[ZERO:ONE, :] += col_sum(dr2)
            dvec_ref[ONE:TWO, :] += col_sum(dy * hat)
            dvec_ref[TWO:THREE, :] += col_sum(dy)
        each_sequence(mq_ref, mp_ref, one)
        for i in range(TWO):
            copy(*saved[i], sems.at[i])

    store_blocks(dwd_ref, mm(g_ref[ALL], dr2b_ref[ALL], TN))

    @pl.when(j == pl.num_programs(ZERO) - ONE)
    def _():
        for i in range(TWO):
            drain(saved[i][ZERO], sems.at[i])


def down_backward(dpool, r2, mask_q, mask_p, gain, g, tile=TILE):
    t, d = r2.shape
    f = g.shape[ONE]
    n = d // WIDTH
    return pl.pallas_call(
        down_bwd_kernel, grid=(f // tile,),
        out_shape=(sds((n, f, WIDTH), F32), sds((t, d), F32), sds((t, d), BF16), sds((8, d), F32)),
        in_specs=[whole(*dpool.shape), whole(t, d), whole(*mask_q.shape), whole(*mask_p.shape), whole(ONE, d), across(t, tile)],
        out_specs=(pl.BlockSpec((n, tile, WIDTH), lambda j: (ZERO, j, ZERO)), ANY, ANY, whole(8, d)),
        scratch_shapes=[pltpu.VMEM((t, d), F32), pltpu.VMEM((t, d), BF16), pltpu.SemaphoreType.DMA((TWO,))],
        compiler_params=vmem(), name="down_backward",
    )(dpool, r2, mask_q, mask_p, gain, g)


PACE_UP = (3.0, 2.5, 6.0, 4.0)
PACE_B = (4.5, 3.0, 5.0, 4.0)
PACE_A = (6.0, 3.4, 0.0, 0.0)
def place(timed, slot_times):
    plan = [[] for _ in slot_times]
    for t, f in sorted(timed, key=lambda x: x[ZERO]):
        plan[min([i for i, at in enumerate(slot_times) if at >= t], default=-ONE)].append(f)
    return plan


def timeline(steps, start, pace, before_third, before_last):
    n = len(steps)
    times = [0.0] + [start + pace * i for i in range(n - TWO)] + [1e3]
    if before_last:
        times[-4] = times[-5] + before_third
        times[-THREE] = times[-4] + before_last
        times[-TWO] = times[-THREE] + before_last
    return list(zip(times, steps))


def run_slot(plan, j, per, steps, point):
    for s in range(*steps):
        todo = plan[s * per + point]
        if todo:
            @pl.when(j == s)
            def _():
                for f in todo:
                    f()


def host(collective_id, mb):
    return pltpu.CompilerParams(collective_id=collective_id, has_side_effects=True, vmem_limit_bytes=mb * 1024 * 1024)


def up_bwd_kernel(axis, steps, dr2_hbm, dr2b_ref, h_ref, gp_ref, wd_ref, wu_ref, r1_hbm, g1_ref, cq_hbm, cp_hbm, a_ref,
                  dw_ref, dbu_ref, dr1q_hbm, dr1p_hbm, lowq_hbm, lowp_hbm, dvec_ref, piece_ref, part_ref,
                  dr1_ref, low_ref, r1_ref, ctx_ref, ht_ref, in_sem, out_sem, *scratch):
    j = pl.program_id(ZERO)
    t, tq, tp = dr1_ref.shape[ZERO], dr1q_hbm.shape[ZERO], dr1p_hbm.shape[ZERO]
    p = ring_plan(axis, UNITS_A)
    pace = 5.6
    timed = timeline(scatter_rounds(p, a_ref, part_ref, piece_ref, *scratch), *PACE_UP)
    points = THREE
    plan = place(timed, [pace * (s // points) + pace * (s % points) / points for s in range(points * (steps + TWO))])
    pause = functools.partial(run_slot, plan, j, points)
    q_rows, p_rows = pl.ds(ZERO, tq), pl.ds(tq, tp)
    late = ((r1_hbm, r1_ref), (cq_hbm, ctx_ref.at[q_rows]), (cp_hbm, ctx_ref.at[p_rows]))
    results = ((dr1_ref.at[q_rows], dr1q_hbm), (dr1_ref.at[p_rows], dr1p_hbm), (low_ref.at[q_rows], lowq_hbm), (low_ref.at[p_rows], lowp_hbm))

    @pl.when(j == ZERO)
    def _():
        signal_peers(p.peers)
        copy(dr2_hbm, dr1_ref, in_sem.at[ZERO])
        ht_ref[ALL] = h_ref[ALL].T
        drain(dr1_ref, in_sem.at[ZERO])
        for i in range(THREE):
            copy(*late[i], in_sem.at[ONE + i])

    @pl.when(j < steps)
    def _():
        dg = mm(dr2b_ref[ALL], wd_ref[ALL], NT).astype(BF16).astype(F32)
        dpre = dg * gp_ref[ALL]
        dbu_ref[ALL] = col_sum(dpre)
        dpre = dpre.astype(BF16)

        @pl.when(j == ZERO)
        def _():
            await_peers(p.peers)
        pause((ZERO, steps), ZERO)
        store_blocks(dw_ref, mm(ht_ref[ALL], dpre))
        pause((ZERO, steps), ONE)
        dr1_ref[ALL] += mm(dpre, wu_ref[ALL], NT)
        pause((ZERO, steps), TWO)

    def norm_backward(at):
        dy = dr1_ref[at, :].astype(BF16).astype(F32)
        hat, r = norm_rows(r1_ref[at, :])
        dr1 = norm_back(dy * g1_ref[ALL], hat, r)
        dr1_ref[at, :] = dr1
        low_ref[at, :] = dr1.astype(BF16)
        dvec_ref[ZERO:ONE, :] += col_sum(dr1)
        dvec_ref[ONE:TWO, :] += col_sum(dy * hat)
        dvec_ref[TWO:THREE, :] += col_sum(dy)

    @pl.when(j == steps)
    def _():
        dvec_ref[ALL] = jnp.zeros_like(dvec_ref)
        for i in range(THREE):
            drain(late[i][ONE], in_sem.at[ONE + i])
        each_block(ZERO, t, norm_backward)
        pause((steps, steps + ONE), ZERO)
        for i in range(4):
            copy(*results[i], out_sem.at[i])

    @pl.when(j >= steps)
    def _():
        half = dr1_ref.shape[ONE] // TWO
        at = pl.ds(pl.multiple_of(jnp.maximum(j - steps, ZERO) * half, half), half)
        pause((steps + ONE, steps + TWO), ZERO)
        pause((steps, steps + TWO), ONE)
        store_blocks(dw_ref, mm(ctx_ref[ALL], low_ref[:, at], TN))
        pause((steps, steps + TWO), TWO)

    @pl.when(j == steps + ONE)
    def _():
        for i in range(4):
            drain(results[i][ZERO], out_sem.at[i])


def up_backward(axis, dr2, dr2b, h, gp, w_down, w_up, r1, gain, ctx_q, ctx_p, part_a, collective_id, tile=TILE):
    t, d = h.shape
    f = w_up.shape[ONE]
    tq, tp = ctx_q.shape[ZERO], ctx_p.shape[ZERO]
    n, total, steps = tile // WIDTH, part_a.shape[ZERO], f // tile
    cut = lambda j: jnp.minimum(j, steps - ONE)
    wide = lambda rows: pl.BlockSpec((rows, tile), lambda j: (ZERO, cut(j)))
    dma, vm = pltpu.SemaphoreType.DMA, pltpu.VMEM
    return pl.pallas_call(
        functools.partial(up_bwd_kernel, axis, steps), grid=(steps + TWO,),
        out_shape=(sds(((f + d) // WIDTH, d, WIDTH), F32), sds((ONE, f), F32), sds((tq, d), F32), sds((tp, d), F32),
                   sds((tq, d), BF16), sds((tp, d), BF16), sds((8, d), F32),
                   sds((total // 128, WIDTH), F32), sds((total // TWO, WIDTH), F32)),
        in_specs=[ANY, whole(t, d), whole(t, d), wide(t), pl.BlockSpec((tile, d), lambda j: (cut(j), ZERO)), wide(d),
                  ANY, whole(ONE, d), ANY, ANY, ANY],
        out_specs=(pl.BlockSpec((n, d, WIDTH), lambda j: (j, ZERO, ZERO)), wide(ONE), ANY, ANY, ANY, ANY,
                   whole(8, d), whole(total // 128, WIDTH), ANY),
        scratch_shapes=[vm((t, d), F32), vm((t, d), BF16), vm((t, d), F32), vm((t, d), BF16), vm((d, t), BF16), dma((4,)), dma((4,))]
        + scatter_scratch(UNITS_A),
        compiler_params=host(collective_id, 63), name="up_backward",
    )(dr2, dr2b, h, gp, w_down, w_up, r1, gain, ctx_q, ctx_p, part_a)


def attn_bwd_body(scale, head, group, low_ref, wo_ref, qkv_ref, probs_ref, out_ref, dctx_ref, pause, enter=lambda: None):
    rows_here, d = low_ref.shape
    pair = TWO * head
    dctx_ref[:rows_here, :] = mm(low_ref[ALL], wo_ref[ALL], NT).astype(BF16)
    enter()
    pause(ZERO)

    def one(g):
        at, k_at, v_at = (pl.ds(pl.multiple_of(part * d + g * pair, pair), pair) for part in range(THREE))
        q = split_heads(qkv_ref[:, at], head)
        k = qkv_ref[:, k_at]
        v = qkv_ref[:, v_at]
        p = probs_ref[ZERO, g]
        dc = split_heads(dctx_ref[:rows_here, at], head)
        dp = mm(dc, v, NT)
        pf = p.astype(F32)
        ds = (pf * (dp - row_sum(dp * pf)) * scale).astype(BF16)
        out_ref[:, at] = join_heads(mm(ds, k), head).astype(BF16)
        out_ref[:, k_at] = mm(ds, q, TN).astype(BF16)
        out_ref[:, v_at] = mm(p, dc, TN).astype(BF16)

    def some(i, _):
        for h in range(group):
            one(i * group + h)
        return ZERO
    lax.fori_loop(ZERO, d // (pair * group), some, ZERO)
    pause(ONE)


def attn_qkv_kernel(axis, scale, head, nq, n_pass, lowq_ref, lowp_ref, wo_ref, qkvq_ref, qkvp_ref, probq_ref, probp_ref,
                    xq_ref, xp_ref, w_ref, dr1q_hbm, dr1p_hbm, b_ref, piecea_ref,
                    dw_ref, db_ref, dhq_ref, dhp_ref, pieceb_ref, part_ref, a_ref, dq_ref, dp_ref, accq_ref, accp_ref, dctx_ref, sem, gsem, *scratch):
    j = pl.program_id(ZERO)
    tile = w_ref.shape[ZERO]
    per = dq_ref.shape[TWO] // tile
    first, last = nq + n_pass, nq + n_pass + per - ONE
    pa, pb = ring_plan(axis, UNITS_A), ring_plan(axis, UNITS_B)
    points = TWO
    steps = [3.2] * nq + [3.3] * n_pass + [4.3] * per
    slots = [sum(steps[:i]) + steps[i] * h / points for i in range(len(steps)) for h in range(points)]
    timed = timeline(scatter_rounds(pb, b_ref, part_ref, pieceb_ref, *scratch), *PACE_B)
    timed += timeline(gather_rounds(pa, piecea_ref, a_ref, gsem), *PACE_A)
    plan = place(timed, slots)
    pause = functools.partial(run_slot, plan, j, points)
    loads = ((dr1q_hbm, accq_ref), (dr1p_hbm, accp_ref))

    @pl.when(j == ZERO)
    def _():
        signal_peers(pa.peers)
        for src, dst in loads:
            copy(src, dst, sem.at[ZERO])

    def enter():
        @pl.when(j == ZERO)
        def _():
            await_peers(pa.peers)

    @pl.when(j < nq)
    def _():
        attn_bwd_body(scale, head, TWO, lowq_ref, wo_ref, qkvq_ref, probq_ref, dq_ref.at[jnp.minimum(j, nq - ONE)], dctx_ref,
                      functools.partial(pause, (ZERO, nq)), enter)

    @pl.when((j >= nq) & (j < first))
    def _():
        attn_bwd_body(scale, head, TWO, lowp_ref, wo_ref, qkvp_ref, probp_ref, dp_ref.at[jnp.clip(j - nq, ZERO, n_pass - ONE)], dctx_ref,
                      functools.partial(pause, (nq, first)))

    @pl.when(j == first - ONE)
    def _():
        for src, dst in loads:
            drain(dst, sem.at[ZERO])

    @pl.when(j >= first)
    def _():
        pause((first, last + ONE), ZERO)
        at = pl.ds(pl.multiple_of(jnp.maximum(j - first, ZERO) * tile, tile), tile)
        dq = dq_ref[:, :, at].reshape(-ONE, tile)
        dp = dp_ref[:, :, at].reshape(-ONE, tile)
        store_blocks(dw_ref, mm(dq, xq_ref[ALL], TN) + mm(dp, xp_ref[ALL], TN))
        db_ref[ALL] = col_sum(dq.astype(F32)) + col_sum(dp.astype(F32))
        pause((first, last + ONE), ONE)
        accq_ref[ALL] += mm(dq, w_ref[ALL])
        accp_ref[ALL] += mm(dp, w_ref[ALL])

    @pl.when(j == last)
    def _():
        dhq_ref[ALL] = accq_ref[ALL].astype(BF16)
        dhp_ref[ALL] = accp_ref[ALL].astype(BF16)


def attn_qkv_backward(axis, low_q, low_p, w_out, qkv_q, qkv_p, probs_q, probs_p, xq, xp, w_t, dr1_q, dr1_p, part_b, piece_a, head,
                      collective_id, tile=TILE):
    f, d = w_t.shape
    nq, pairs, _, lq = probs_q.shape
    n_pass, _, _, lp = probs_p.shape
    tq, tp = nq * lq, n_pass * lp
    per, cols, total = f // tile, d // WIDTH, part_b.shape[ZERO]
    jq = lambda j: jnp.minimum(j, nq - ONE)
    jp = lambda j: jnp.clip(j - nq, ZERO, n_pass - ONE)
    jt = lambda j: jnp.clip(j - nq - n_pass, ZERO, per - ONE)
    rows_of = lambda n, c, at: pl.BlockSpec((n, c), lambda j: (at(j), ZERO))
    probs_of = lambda n, at: pl.BlockSpec((ONE, pairs, TWO * n, n), lambda j: (at(j), ZERO, ZERO, ZERO))
    return pl.pallas_call(
        functools.partial(attn_qkv_kernel, axis, head ** -0.5, head, nq, n_pass), grid=(nq + n_pass + per,),
        out_shape=(sds((cols, f, WIDTH), F32), sds((ONE, f), F32), sds((tq, d), BF16), sds((tp, d), BF16),
                   sds((total // 128, WIDTH), F32), sds((total // TWO, WIDTH), F32), sds((piece_a.shape[ZERO] * 128, WIDTH), F32)),
        in_specs=[rows_of(lq, d, jq), rows_of(lp, d, jp), whole(d, d), rows_of(lq, f, jq), rows_of(lp, f, jp),
                  probs_of(lq, jq), probs_of(lp, jp), whole(tq, d), whole(tp, d), rows_of(tile, d, jt), ANY, ANY, ANY, whole(*piece_a.shape)],
        out_specs=(pl.BlockSpec((cols, tile, WIDTH), lambda j: (ZERO, jt(j), ZERO)), pl.BlockSpec((ONE, tile), lambda j: (ZERO, jt(j))),
                   whole(tq, d), whole(tp, d), whole(total // 128, WIDTH), ANY, ANY),
        scratch_shapes=[pltpu.VMEM((nq, lq, f), BF16), pltpu.VMEM((n_pass, lp, f), BF16), pltpu.VMEM((tq, d), F32),
                        pltpu.VMEM((tp, d), F32), pltpu.VMEM((lp, d), BF16), pltpu.SemaphoreType.DMA((ONE,)),
                        pltpu.SemaphoreType.DMA((GATHER_SEMS,))]
        + scatter_scratch(UNITS_B),
        compiler_params=host(collective_id, 63), name="attn_qkv_backward",
    )(low_q, low_p, w_out, qkv_q, qkv_p, probs_q, probs_p, xq, xp, w_t, dr1_q, dr1_p, part_b, piece_a)


def unpack_kernel(a_hbm, sums_ref, down_ref, up_ref, out_ref, qkv_ref, stage, sem, in_sem, out_sem):
    def cols(i):
        return pl.ds(i * WIDTH, WIDTH)

    slots, rows_each, _ = stage.shape
    n, ff, f = up_ref.shape[ZERO], down_ref.shape[ZERO], qkv_ref.shape[ZERO]
    kept = sums_ref.shape[ZERO] - (up_ref.shape[ONE] + out_ref.shape[ONE]) // WIDTH * n - qkv_ref.shape[ONE] // WIDTH * f
    todo = [(kept + i * rows_each) for i in range((down_ref.shape[ONE] // WIDTH * ff - kept) // rows_each)]

    def load(i):
        copy(a_hbm.at[pl.ds(todo[i], rows_each)], stage.at[i % slots], in_sem.at[i % slots])

    for i in range(slots):
        load(i)
    at = ZERO
    for ref, size in ((up_ref, n), (out_ref, n), (qkv_ref, f), (down_ref, ff)):
        for i in range(ref.shape[ONE] // WIDTH):
            if at < sums_ref.shape[ZERO]:
                copy(sums_ref.at[pl.ds(at, size)], ref.at[:, cols(i)], sem.at[ZERO])
            at += size
    for i, row in enumerate(todo):
        slot = i % slots
        drain(stage.at[slot], in_sem.at[slot])
        copy(stage.at[slot], down_ref.at[pl.ds(row % ff, rows_each), cols(row // ff)], out_sem.at[slot])
        if i >= ONE and i - ONE + slots < len(todo):
            drain(stage.at[slot], out_sem.at[(i - ONE) % slots])
            load(i - ONE + slots)
    for i in range(max(len(todo) - slots, ZERO), len(todo)):
        drain(stage.at[ZERO], out_sem.at[i % slots])
    drain(sums_ref, sem.at[ZERO])


def unpack(a, sums, d, ff, f):
    slots = 4
    dma = pltpu.SemaphoreType.DMA
    return pl.pallas_call(
        unpack_kernel, out_shape=(sds((ff, d), F32), sds((d, ff), F32), sds((d, d), F32), sds((f, d), F32)),
        in_specs=[ANY, pl.BlockSpec(memory_space=pltpu.VMEM)], out_specs=(ANY,) * 4,
        scratch_shapes=[pltpu.VMEM((slots, TWO * TILE, WIDTH), F32), dma((ONE,)), dma((slots,)), dma((slots,))],
        compiler_params=vmem(8), name="unpack",
    )(a, pltpu.with_memory_space_constraint(sums, pltpu.VMEM))


def solution(mesh):
    axis = mesh.axis_names[ZERO]
    n_dev = mesh.shape[axis]

    def local_step(q_hidden, q_mask, p_hidden, p_mask, w_qkv, b_qkv, w_out, b_out, ln1_gain, ln1_shift,
                   w_up, b_up, w_down, b_down, ln2_gain, ln2_shift):
        nq, _, d = q_hidden.shape
        n_pass, p_len = nq * p_hidden.shape[ONE], p_hidden.shape[TWO]
        _, three, heads, head = w_qkv.shape
        xq, xp = q_hidden.reshape(-ONE, d), p_hidden.reshape(-ONE, d)
        p_mask = p_mask.reshape(n_pass, p_len)
        wqkv_t = w_qkv.transpose(ONE, TWO, THREE, ZERO).reshape(-ONE, d)
        wo = w_out.reshape(-ONE, d)
        vecs = [v.reshape(ONE, d) for v in (b_out, ln1_gain, ln1_shift, b_down, ln2_gain, ln2_shift)]

        qkv_q, qkv_p = qkv_project(xq, xp, wqkv_t, b_qkv.reshape(ONE, -ONE))
        probs_q, ctx_q = attention(qkv_q, q_mask, head)
        probs_p, ctx_p = attention(qkv_p, p_mask, head)
        h, r1, g, gp, r2, pooled = ffn_forward(
            xq, xp, ctx_q, ctx_p, wo, vecs, q_mask, p_mask, w_up, b_up.reshape(ONE, -ONE), w_down)
        everyone = gather_embeddings(pooled, axis, ONE)
        mean_loss, d_pooled = loss_and_grad(everyone, pooled, axis, nq * n_dev)
        dwd, dr2, dr2b, dvec2 = down_backward(d_pooled, r2, q_mask, p_mask, vecs[4], g)
        dwb, dbu, dr1_q, dr1_p, low_q, low_p, dvec1, piece_a, _ = up_backward(
            axis, dr2, dr2b, h, gp, w_down, w_up, r1, vecs[ONE], ctx_q, ctx_p, dwd.reshape(-ONE, WIDTH), TWO)
        dwq, dbq, dh_q, dh_p, piece_b, _, a = attn_qkv_backward(
            axis, low_q, low_p, wo, qkv_q, qkv_p, probs_q, probs_p, xq, xp, wqkv_t, dr1_q, dr1_p, dwb.reshape(-ONE, WIDTH), piece_a, head, THREE)
        sums, small = finish_sum(axis, UNITS_B, UNITS_C, piece_b, dwq.reshape(-ONE, WIDTH), a, THREE * w_down.shape[ZERO],
                                 dvec1, dvec2, dbq, dbu, 4)
        d_down, d_up, d_out, d_qkv = unpack(a, sums, d, w_down.shape[ZERO], three * d)
        vec, bias = small[:8], small[8:]
        return (mean_loss, dh_q.reshape(q_hidden.shape), dh_p.reshape(p_hidden.shape),
                d_qkv.reshape(three, heads, head, d).transpose(THREE, ZERO, ONE, TWO), bias[:three].reshape(b_qkv.shape),
                d_out.reshape(w_out.shape), vec[ZERO], vec[ONE], vec[TWO], d_up, bias[three:-ONE].reshape(-ONE),
                d_down, vec[THREE], vec[4], vec[5])

    in_specs = (P(axis),) * 4 + (P(),) * 12
    out_specs = (P(), P(axis), P(axis)) + (P(),) * 12
    return jax.shard_map(local_step, mesh=mesh, in_specs=in_specs, out_specs=out_specs, check_vma=False)
```
